512 devices in a mesh: member: 2 (over y), seq: 32 (over z), head: 4 (over x), rep: 2 (over core).
Axes of the slice: x: 4, y: 2, z: 32, core: 2. Of those that a mesh axis runs over, the one named last changes fastest.
The devices are a block of a 4x8x32 slice.
Arguments:
- x_raw: bfloat16 [4, 32768, 2560], P(('member', 'rep'), 'seq', 'head'), parts along dimension 0, may hold values from -6 to 6
- bc_raw: bfloat16 [4, 32768, 256], P(('member', 'rep'), 'seq'), parts along dimension 0, may hold values from -3 to 3
- gate_in: bfloat16 [4, 32768, 2560], P(('member', 'rep'), 'seq', 'head'), parts along dimension 0, may hold values from -570 to 570
- step_raw: float32 [4, 32768, 40], P(('member', 'rep'), 'seq', 'head'), parts along dimension 0, may hold values from -1.9 to 4.9
- conv_x_weight: bfloat16 [8, 2560], P('member', 'head'), parts along dimension 0, may hold values from -3 to 3
- conv_x_bias: bfloat16 [5120], P(('member', 'head')), parts along dimension 0, may hold values from -0.5 to 0.5
- conv_bc_weight: bfloat16 [8, 256], P('member'), parts along dimension 0, may hold values from -3 to 3
- conv_bc_bias: bfloat16 [512], P('member'), parts along dimension 0, may hold values from -0.5 to 0.5
- dt_bias: float32 [80], P(('member', 'head')), parts along dimension 0, may hold values from -3.5 to 0.55
- a_log: float32 [80], P(('member', 'head')), parts along dimension 0
- d_skip: float32 [80], P(('member', 'head')), parts along dimension 0, may hold values from 0.5 to 2
- norm_gain: float32 [5120], P(('member', 'head')), parts along dimension 0, may hold values from 0.5 to 1.5
Outputs:
- mixer_out: bfloat16 [4, 32768, 2560], P(('member', 'rep'), 'seq', 'head'), parts along dimension 0
The draws below stay inside these ranges and needn't reach their ends.
There are 2 independent parts, one for each index of `member`. The reference program is written for one: setup_inputs(seed, part) draws one part's arguments, and reference() takes and returns one part's arrays. A program takes and returns all parts, laid end to end along the dimension named above; each array names one. Nothing has to cross between parts.
All inputs are finite; a program needn't handle non-finite values.
Results may differ from the reference program's by a relative error of at most 0.0082.
Values may be sent and summed in bfloat16 or wider, within the bound.
A program may use at most 64 MiB of HBM per device.

```python
import math
import jax
import jax.numpy as jnp
from jax import lax

HEADS = 40
HEADDIM = 64
STATE = 128
GROUP = 256
CONV = 4
TOK_DEV = 1024
DI = 2560
LENGTH = 32768
SEQS = 2


def head_plan(key):
    slow_share = 0.5
    chooser = jax.random.uniform(jax.random.fold_in(key, 7001), (HEADS,))
    slow_heads = chooser < slow_share

    def spread_log(label, lowest, highest):
        unit_draw = jax.random.uniform(jax.random.fold_in(key, label), (HEADS,))
        return jnp.exp(math.log(lowest) + unit_draw * (math.log(highest) - math.log(lowest)))
    base_step = jnp.where(slow_heads, spread_log(7002, 0.03, 0.1), spread_log(7003, 0.3, 1.0))
    slow_rate = spread_log(7004, 0.2, 0.6) / LENGTH
    decay_rate = jnp.where(slow_heads, slow_rate, spread_log(7005, 0.02, 0.1))
    return (base_step, decay_rate / base_step)


def draw_dt_bias(key, part):
    base_step, head_rate = head_plan(key)
    return jnp.log(jnp.expm1(base_step)).astype(jnp.float32)


def draw_a_log(key, part):
    base_step, head_rate = head_plan(key)
    return jnp.log(head_rate).astype(jnp.float32)


def draw_step_raw(key, part):
    blocks = LENGTH // TOK_DEV
    offsets = jax.random.uniform(jax.random.fold_in(key, 1), (SEQS, blocks, 1, HEADS), minval=-0.7, maxval=0.7)
    offsets = jnp.broadcast_to(offsets, (SEQS, blocks, TOK_DEV, HEADS)).reshape(SEQS, LENGTH, HEADS)
    jitter = jnp.clip(0.3 * jax.random.normal(jax.random.fold_in(key, 2), (SEQS, LENGTH, HEADS)), -1.2, 1.2)
    run_length = max(LENGTH // 32, 1)
    starts = jax.random.randint(jax.random.fold_in(key, 3), (SEQS, 3), 0, LENGTH - run_length + 1)
    places = jnp.arange(LENGTH)
    inside = jnp.any((places[None, None, :] >= starts[:, :, None]) & (places[None, None, :] < starts[:, :, None] + run_length), axis=1)
    return (offsets + jitter + 3.0 * inside[:, :, None].astype(jnp.float32)).astype(jnp.float32)


def draw_gate_in(key, part):
    channel_ramp = jnp.arange(DI).astype(jnp.float32) / DI
    noise_cols = jax.random.uniform(jax.random.fold_in(key, 11), (DI,), minval=-0.35, maxval=0.35)
    noise_rows = jax.random.uniform(jax.random.fold_in(key, 12), (SEQS, LENGTH, 1))
    columns = jnp.exp(math.log(10.0) * channel_ramp + noise_cols)
    row_scale = jnp.exp(math.log(4.0) * noise_rows)
    values = jnp.clip(jax.random.normal(jax.random.fold_in(key, 13), (SEQS, LENGTH, DI)), -4.0, 4.0)
    return (values * columns * row_scale).astype(jnp.bfloat16)


def level_of(stream_key, extent, split, low, high):
    factor_of = 1.0
    for dim, shards_of in split:
        draws = jax.random.uniform(jax.random.fold_in(jax.random.fold_in(stream_key, 6), dim), (shards_of,), jnp.float32, low / len(split), high / len(split))
        factor_of = factor_of * jnp.repeat(jnp.exp(draws), extent[dim] // shards_of).reshape((-1,) + (1,) * (len(extent) - 1 - dim))
    return factor_of


def bell_draw(key, shape, deviation, limit, cuts=(), dtype=jnp.bfloat16):
    drawn = jax.random.normal(key, shape, jnp.float32) * deviation
    if len(cuts) > 0:
        drawn = level_of(key, shape, cuts, -0.22, 0.18) * drawn
    return jnp.clip(drawn, min=-limit, max=limit).astype(dtype)


def setup_inputs(seed: int = 0, part: int = 0) -> dict:
    arg_keys = jax.random.split(jax.random.key(seed), 13)
    own_keys = jax.random.split(jax.random.fold_in(arg_keys[12], part), 13)
    return {
        "x_raw": bell_draw(own_keys[0], (SEQS, LENGTH, DI), 1.0, 6.0, ((0, 2), (1, 32), (2, 4))),
        "bc_raw": bell_draw(own_keys[1], (SEQS, LENGTH, 2 * STATE), 0.5, 3.0, ((0, 2), (1, 32))),
        "gate_in": draw_gate_in(jax.random.fold_in(jax.random.fold_in(arg_keys[12], part), 71), part),
        "step_raw": draw_step_raw(jax.random.fold_in(jax.random.fold_in(arg_keys[12], part), 71), part),
        "conv_x_weight": bell_draw(own_keys[4], (CONV, DI), CONV ** -0.5, 3.0, ((1, 4),)),
        "conv_x_bias": jnp.clip(jax.random.uniform(own_keys[5], (DI,), jnp.float32, -0.5, 0.5) * level_of(own_keys[5], (DI,), ((0, 4),), -0.4, 0.0), -0.5, 0.5).astype(jnp.bfloat16),
        "conv_bc_weight": bell_draw(own_keys[6], (CONV, 2 * STATE), CONV ** -0.5, 3.0),
        "conv_bc_bias": jnp.clip(jax.random.uniform(own_keys[7], (2 * STATE,), jnp.float32, -0.5, 0.5), -0.5, 0.5).astype(jnp.bfloat16),
        "dt_bias": draw_dt_bias(jax.random.fold_in(jax.random.fold_in(arg_keys[12], part), 71), part),
        "a_log": draw_a_log(jax.random.fold_in(jax.random.fold_in(arg_keys[12], part), 71), part),
        "d_skip": jnp.clip(0.5 + 1.5 * jax.random.uniform(own_keys[10], (HEADS,), jnp.float32) ** level_of(own_keys[10], (HEADS,), ((0, 4),), -0.2, 0.2), 0.5, 2.0),
        "norm_gain": jnp.clip(1.0 + 0.1 * jax.random.normal(own_keys[11], (DI,), jnp.float32), 0.5, 1.5),
    }


norm_eps = 1e-05

def causal_conv(raw_rows, conv_weight, conv_bias):
    row_count = raw_rows.shape[0]
    padded = jnp.pad(raw_rows, ((CONV - 1, 0), (0, 0))).astype(jnp.float32)
    summed = jnp.zeros(raw_rows.shape, jnp.float32) + conv_bias.astype(jnp.float32)
    for tap_index in range(CONV):
        summed = summed + conv_weight[tap_index].astype(jnp.float32) * padded[tap_index:tap_index + row_count]
    return jax.nn.silu(summed).astype(jnp.bfloat16)

def group_step(state_in, group_data):
    x_group, b_group, c_group, step_group, rate_group = group_data
    log_decay = jnp.cumsum(rate_group, axis=0)
    intersection = jnp.dot(c_group, b_group.T, preferred_element_type=jnp.float32)
    lower_mask = jnp.arange(GROUP)[:, None] >= jnp.arange(GROUP)[None, :]
    head_decay = log_decay.T
    spread = head_decay[:, :, None] - head_decay[:, None, :]
    kernel = jnp.where(lower_mask[None], jnp.exp(jnp.where(lower_mask[None], spread, 0.0)), 0.0)
    mixing = (intersection[None] * kernel * step_group.T[:, None, :]).astype(jnp.bfloat16)
    intra_out = jnp.einsum('hts,shp->thp', mixing.astype(jnp.float32), x_group.astype(jnp.float32))
    carried = jnp.einsum('tn,hpn->thp', c_group.astype(jnp.float32), state_in, precision=lax.Precision.HIGHEST)
    outputs = intra_out + jnp.exp(log_decay)[:, :, None] * carried
    tail_weight = jnp.exp(log_decay[-1][None, :] - log_decay) * step_group
    weighted = (tail_weight[:, :, None] * x_group.astype(jnp.float32)).astype(jnp.bfloat16)
    fresh_state = jnp.einsum('shp,sn->hpn', weighted.astype(jnp.float32), b_group.astype(jnp.float32))
    state_out = jnp.exp(log_decay[-1])[:, None, None] * state_in + fresh_state
    return (state_out, outputs)

def reference(x_raw, bc_raw, gate_in, step_raw, conv_x_weight, conv_x_bias, conv_bc_weight, conv_bc_bias, dt_bias, a_log, d_skip, norm_gain):
    groups = LENGTH // GROUP

    def one_sequence(sequence_data):
        x_rows, bc_rows, gate_rows, step_rows = sequence_data
        x_conv = causal_conv(x_rows, conv_x_weight, conv_x_bias)
        bc_conv = causal_conv(bc_rows, conv_bc_weight, conv_bc_bias)
        step_size = jax.nn.softplus(step_rows + dt_bias)
        log_rate = -jnp.exp(a_log) * step_size
        x_heads = x_conv.reshape(groups, GROUP, HEADS, HEADDIM)
        b_rows = bc_conv[:, :STATE].reshape(groups, GROUP, STATE)
        c_rows = bc_conv[:, STATE:].reshape(groups, GROUP, STATE)
        zero_state = jnp.zeros((HEADS, HEADDIM, STATE), jnp.float32)
        last_state, outputs = lax.scan(group_step, zero_state, (x_heads, b_rows, c_rows, step_size.reshape(groups, GROUP, HEADS), log_rate.reshape(groups, GROUP, HEADS)))
        mixed_rows = outputs.reshape(LENGTH, HEADS, HEADDIM) + d_skip[None, :, None] * x_conv.reshape(LENGTH, HEADS, HEADDIM).astype(jnp.float32)
        gated_rows = mixed_rows.reshape(LENGTH, DI) * jax.nn.silu(gate_rows.astype(jnp.float32))
        mean_square = lax.optimization_barrier(jnp.sum(gated_rows * gated_rows, axis=1, keepdims=True)) / DI
        return (gated_rows * lax.rsqrt(mean_square + norm_eps) * norm_gain).astype(jnp.bfloat16)
    return lax.map(one_sequence, (x_raw, bc_raw, gate_in, step_raw))
```

```python
import functools

import jax
import jax.numpy as jnp
from jax import lax
from jax.experimental import pallas as pl
from jax.experimental.pallas import tpu as pltpu
from jax.sharding import PartitionSpec as P

HEADDIM = 64
STATE = 128
GROUP = 256
CONV = 4
LANES = 128
HALO = 16
ROWS = 64
SEG = 8
LOG2E = 1.4426950408889634
norm_eps = 1e-05

F32 = jnp.float32
BF16 = jnp.bfloat16
MESH = pl.DeviceIdType.MESH


def silu(v):
    half = 0.5 * v
    return half + half * jnp.tanh(half)


def two_parts(v):
    high = v.astype(BF16)
    return high, (v - high.astype(F32)).astype(BF16)


def three_parts(v):
    high = v.astype(BF16)
    rest = v - high.astype(F32)
    mid = rest.astype(BF16)
    return high, mid, (rest - mid.astype(F32)).astype(BF16)


def dot(a, b, dims=((1,), (0,))):
    return lax.dot_general(a, b, (dims, ((), ())), preferred_element_type=F32)


def kernel(sizes, *refs):
    n_seq, n_head, seg_len, length, feat, heads = sizes
    (
        x_hbm, bc_hbm, gate_hbm, step_ref, cxw_ref, cxb_ref, cbw_ref, cbb_ref,
        dt_ref, alog_ref, skip_ref, gain_ref, out_ref,
        xext, bcext, gbuf, xconv, bconv, stepb, ldb, ldt, stept, par, cw, expand_m, tri_m,
        tail_e, weighted, fresh, entry, base, scale, dec,
        s_send, a_recv, ld_mine, ld_recv, loc, t_send, b_recv, lt_mine, lt_recv, c_send, inc,
        ss_mine, ss_recv,
        loc_sem, halo_s, halo_r, a_s, a_r, al_s, al_r, b_s, b_r, bl_s, bl_r, c_s, c_r, x_s, x_r,
    ) = refs
    groups = length // GROUP
    tiles = feat // LANES
    piece = STATE // seg_len
    segs = n_seq // seg_len
    di = feat * n_head

    me = lax.axis_index("seq")
    mine_h = lax.axis_index("head")
    seg = me // seg_len
    pos = lax.rem(me, seg_len)

    loads = [
        pltpu.make_async_copy(x_hbm, xext.at[pl.ds(HALO, length)], loc_sem.at[0]),
        pltpu.make_async_copy(bc_hbm, bcext.at[pl.ds(HALO, length)], loc_sem.at[1]),
        pltpu.make_async_copy(gate_hbm, gbuf, loc_sem.at[2]),
    ]
    for load in loads:
        load.start()

    b_recv[...] = jnp.zeros_like(b_recv)
    lt_recv[...] = jnp.zeros_like(lt_recv)
    barrier = pltpu.get_barrier_semaphore()
    following = lax.rem(me + 1, n_seq)
    partners = [{"seq": following}, {"seq": lax.rem(me + n_seq - 1, n_seq)}]
    for d in range(1, seg_len):
        partners.append({"seq": seg * seg_len + lax.rem(pos + d, seg_len)})
    for k in range(1, segs):
        partners.append({"seq": lax.rem(me + k * seg_len, n_seq)})
    for d in range(1, n_head):
        partners.append({"head": lax.rem(mine_h + d, n_head)})
    for partner in partners:
        pl.semaphore_signal(barrier, inc=1, device_id=partner, device_id_type=MESH)

    row_i = lax.broadcasted_iota(jnp.int32, (GROUP, GROUP), 0)
    col_i = lax.broadcasted_iota(jnp.int32, (GROUP, GROUP), 1)
    tri_m[...] = jnp.where(row_i >= col_i, 1.0, 0.0).astype(BF16)
    head_i = lax.broadcasted_iota(jnp.int32, (LANES, feat), 0)
    feat_i = lax.broadcasted_iota(jnp.int32, (LANES, feat), 1)
    expand_m[...] = jnp.where((feat_i >> 6) == head_i, 1.0, 0.0).astype(BF16)
    par[...] = jnp.zeros_like(par)
    par[0:1, 0:heads] = dt_ref[...]
    par[1:2, 0:heads] = alog_ref[...]
    par[2:3, 0:heads] = skip_ref[...]
    cw[0:CONV, 0:feat] = cxw_ref[...].astype(F32)
    cw[CONV : CONV + 1, 0:feat] = cxb_ref[...].astype(F32)
    cw[0:CONV, feat:] = cbw_ref[...].astype(F32)
    cw[CONV : CONV + 1, feat:] = cbb_ref[...].astype(F32)

    def widen3(v):
        total = None
        for part in three_parts(v):
            term = dot(part, expand_m[...])
            total = term if total is None else total + term
        return total

    def widen2(v):
        high, low = two_parts(v)
        return dot(high, expand_m[...]) + dot(low, expand_m[...])

    stepb[...] = jnp.zeros_like(stepb)
    stepb[:, 0:heads] = step_ref[...]
    rate = -LOG2E * jnp.exp(par[1:2, :])

    def decays(g, carry):
        r0 = pl.multiple_of(g * GROUP, GROUP)
        raw = stepb[pl.ds(r0, GROUP), :] + par[0:1, :]
        step = jnp.maximum(raw, 0.0) + jnp.log1p(jnp.exp(-jnp.abs(raw)))
        stepb[pl.ds(r0, GROUP), :] = step
        total = None
        for part in three_parts(rate * step):
            term = dot(tri_m[...], part)
            total = term if total is None else total + term
        ldb[pl.ds(r0, GROUP), :] = total
        dec[pl.ds(g, 1), :] = total[GROUP - 1 : GROUP, :]
        return carry

    dec[...] = jnp.zeros_like(dec)
    lax.fori_loop(0, groups, decays, 0)
    ld_total = dec[0:1, :]
    for g in range(1, groups):
        ld_total = ld_total + dec[g : g + 1, :]
    ld_mine[...] = ld_total[None]

    def conv(ext, r, c0, width, tile, w_off):
        block = ext[pl.ds(r, ROWS + HALO), c0 : c0 + width].astype(F32)
        lo = w_off + c0
        acc = cw[CONV : CONV + 1, lo : lo + width]
        for k in range(CONV):
            shift = CONV - 1 - k
            moved = block if shift == 0 else pltpu.roll(block, shift, 0)
            acc = acc + cw[k : k + 1, lo : lo + width] * moved[HALO:]
        return silu(acc)

    def states(g, carry):
        r0 = pl.multiple_of(g * GROUP, GROUP)
        ld = ldb[pl.ds(r0, GROUP), :]
        tail = jnp.exp2(ld[GROUP - 1 : GROUP, :] - ld) * stepb[pl.ds(r0, GROUP), :]
        tail_e[...] = widen2(tail)

        def chunk(i, inner):
            q0 = pl.multiple_of(i * ROWS, ROWS)
            r = pl.multiple_of(r0 + q0, ROWS)
            for j in range(2 * STATE // LANES):
                bconv[pl.ds(r, ROWS), j * LANES : (j + 1) * LANES] = conv(
                    bcext, r, j * LANES, LANES, j, feat
                ).astype(BF16)
            for j in range(tiles):
                c0 = j * LANES
                value = conv(xext, r, c0, LANES, j, 0).astype(BF16)
                xconv[pl.ds(r, ROWS), c0 : c0 + LANES] = value
                weighted[pl.ds(q0, ROWS), c0 : c0 + LANES] = (
                    tail_e[pl.ds(q0, ROWS), c0 : c0 + LANES] * value.astype(F32)
                ).astype(BF16)
            return inner

        lax.fori_loop(0, GROUP // ROWS, chunk, 0)
        fresh[pl.ds(g, 1)] = dot(
            bconv[pl.ds(r0, GROUP), 0:STATE], weighted[...], ((0,), (0,))
        )[None]
        return carry

    for load in loads[:2]:
        load.wait()
    lax.fori_loop(1, groups, states, 0)

    pl.semaphore_wait(barrier, len(partners))

    def remote(src, dst, send, recv, where):
        return pltpu.make_async_remote_copy(
            src_ref=src, dst_ref=dst, send_sem=send, recv_sem=recv,
            device_id=where, device_id_type=MESH,
        )

    halos = [
        remote(xext.at[pl.ds(length, HALO)], xext.at[pl.ds(0, HALO)], halo_s.at[0], halo_r.at[0], {"seq": following}),
        remote(bcext.at[pl.ds(length, HALO)], bcext.at[pl.ds(0, HALO)], halo_s.at[1], halo_r.at[1], {"seq": following}),
    ]
    for copy in halos:
        copy.start()

    def seg_peer(d):
        return {"seq": seg * seg_len + lax.rem(pos + d, seg_len)}

    ld_copies = []
    for d in range(1, seg_len):
        ld_copies.append(
            remote(ld_mine, ld_recv.at[pl.ds(pos, 1)], al_s.at[d - 1], al_r.at[d - 1], seg_peer(d))
        )
    for copy in ld_copies:
        copy.start()
    ld_recv[pl.ds(pos, 1)] = ld_mine[...]

    for copy in halos:
        copy.wait()
    xext[0:HALO, :] = jnp.where(me == 0, jnp.zeros((HALO, feat), BF16), xext[0:HALO, :])
    bcext[0:HALO, :] = jnp.where(me == 0, jnp.zeros((HALO, 2 * STATE), BF16), bcext[0:HALO, :])
    states(0, 0)

    group_decay = jnp.exp2(widen3(dec[...]))
    run = fresh[0]
    entry[0] = jnp.zeros((STATE, feat), F32)
    entry[1] = run
    for g in range(1, groups):
        run = group_decay[g : g + 1, :] * run + fresh[g]
        if g + 1 < groups:
            entry[g + 1] = run
    s_send[...] = run.astype(BF16).reshape(seg_len, piece, feat)

    a_copies = []
    for d in range(1, seg_len):
        to = lax.rem(pos + d, seg_len)
        a_copies.append(
            remote(s_send.at[pl.ds(to, 1)], a_recv.at[pl.ds(pos, 1)], a_s.at[d - 1], a_r.at[d - 1], seg_peer(d))
        )
    for copy in reversed(a_copies):
        copy.start()
    a_recv[pl.ds(pos, 1)] = s_send[pl.ds(pos, 1)]

    def transposes(g, carry):
        r0 = pl.multiple_of(g * GROUP, GROUP)
        ldt[pl.ds(g, 1)] = ldb[pl.ds(r0, GROUP), :].T[None, 0:16]
        stept[pl.ds(g, 1)] = stepb[pl.ds(r0, GROUP), :].T[None, 0:16]
        return carry

    skip_e = widen3(par[...])[2:3, :]

    def inside(g, carry):
        r0 = pl.multiple_of(g * GROUP, GROUP)
        scale[pl.ds(r0, GROUP), :] = widen2(jnp.exp2(ldb[pl.ds(r0, GROUP), :]))
        lane = lax.broadcasted_iota(jnp.int32, (ROWS, LANES), 1)
        for tb in range(GROUP // ROWS):
            cols = -(-(tb + 1) * ROWS // LANES) * LANES
            rt = pl.multiple_of(r0 + tb * ROWS, ROWS)
            inter = dot(
                bconv[pl.ds(rt, ROWS), STATE:], bconv[pl.ds(r0, cols), 0:STATE], ((1,), (1,))
            )
            t_i = tb * ROWS + lax.broadcasted_iota(jnp.int32, (ROWS, cols), 0)
            s_i = lax.broadcasted_iota(jnp.int32, (ROWS, cols), 1)
            keep = t_i >= s_i
            for j in range(tiles):
                c0 = j * LANES
                xs = xconv[pl.ds(r0, cols), c0 : c0 + LANES]
                halves = []
                for h in (2 * j, 2 * j + 1):
                    diff = ldb[pl.ds(rt, ROWS), h : h + 1] - ldt[g, h : h + 1, 0:cols]
                    kern = jnp.exp2(jnp.where(keep, diff, -jnp.inf))
                    mix = (inter * kern * stept[g, h : h + 1, 0:cols]).astype(BF16)
                    halves.append(dot(mix, xs))
                intra = jnp.where(lane < HEADDIM, halves[0], halves[1])
                x_t = xconv[pl.ds(rt, ROWS), c0 : c0 + LANES].astype(F32)
                gate = silu(gbuf[pl.ds(rt, ROWS), c0 : c0 + LANES].astype(F32))
                base[pl.ds(rt, ROWS), c0 : c0 + LANES] = (intra + skip_e[:, c0 : c0 + LANES] * x_t) * gate
                scale[pl.ds(rt, ROWS), c0 : c0 + LANES] = scale[pl.ds(rt, ROWS), c0 : c0 + LANES] * gate
        return carry

    lax.fori_loop(0, groups, transposes, 0)
    loads[2].wait()
    half_groups = groups // 2
    lax.fori_loop(0, half_groups, inside, 0)

    for copy in ld_copies:
        copy.wait()
    for copy in a_copies:
        copy.wait()
    lds = jnp.concatenate([ld_recv[q] for q in range(seg_len)], axis=0)
    dec_e = jnp.exp2(widen3(lds))
    run = jnp.zeros((piece, feat), F32)
    run_d = jnp.ones((1, feat), F32)
    seg_ld = ld_recv[0]
    before = []
    for q in range(seg_len):
        loc[q] = run
        before.append(run_d)
        run = dec_e[q : q + 1, :] * run + a_recv[q].astype(F32)
        run_d = run_d * dec_e[q : q + 1, :]
        if q > 0:
            seg_ld = seg_ld + ld_recv[q]
    t_send[...] = run[None]
    lt_mine[...] = seg_ld[None]

    def later_copies(k):
        where = {"seq": lax.rem(me + k * seg_len, n_seq)}
        return [
            remote(t_send, b_recv.at[pl.ds(k - 1, 1)], b_s.at[k - 1], b_r.at[k - 1], where),
            remote(lt_mine, lt_recv.at[pl.ds(k - 1, 1)], bl_s.at[k - 1], bl_r.at[k - 1], where),
        ]

    for k in range(segs - 1, 0, -1):

        @pl.when(seg + k < segs)
        def _():
            for copy in later_copies(k):
                copy.start()

    lax.fori_loop(half_groups, groups, inside, 0)

    for k in range(1, segs):

        @pl.when(seg + k < segs)
        def _():
            for copy in later_copies(k):
                copy.wait_send()

        @pl.when(seg >= k)
        def _():
            for copy in later_copies(k):
                copy.wait_recv()

    lts = jnp.concatenate([lt_recv[k] for k in range(segs - 1)] + [jnp.zeros((8 - segs + 1, LANES), F32)], axis=0)
    far_e = jnp.exp2(widen3(lts))
    carry = jnp.zeros((piece, feat), F32)
    for k in range(segs - 1, 0, -1):
        carry = far_e[k - 1 : k, :] * carry + b_recv[k - 1]
    for q in range(seg_len):
        c_send[q] = loc[q] + before[q] * carry

    c_copies = []
    for d in range(1, seg_len):
        to = lax.rem(pos + d, seg_len)
        c_copies.append(
            remote(c_send.at[pl.ds(to, 1)], inc.at[pl.ds(pos, 1)], c_s.at[d - 1], c_r.at[d - 1], seg_peer(d))
        )
    for copy in reversed(c_copies):
        copy.start()
    inc[pl.ds(pos, 1)] = c_send[pl.ds(pos, 1)]
    for copy in c_copies:
        copy.wait()

    run_d = jnp.ones((1, feat), F32)
    ss = jnp.zeros((8, LANES), F32)
    blocks = GROUP // 8
    lane8 = lax.broadcasted_iota(jnp.int32, (blocks, 8, LANES), 2)
    block_i = lax.broadcasted_iota(jnp.int32, (blocks, 8, LANES), 0)
    for g in range(groups):
        r0 = g * GROUP
        state = entry[g] + run_d * inc[...].reshape(STATE, feat)
        high, low = two_parts(state)
        c_rows = bconv[r0 : r0 + GROUP, STATE:]
        squares = jnp.zeros((GROUP, LANES), F32)
        for j in range(tiles):
            c0 = j * LANES
            carried = dot(c_rows, high[:, c0 : c0 + LANES]) + dot(c_rows, low[:, c0 : c0 + LANES])
            gated = base[r0 : r0 + GROUP, c0 : c0 + LANES] + scale[r0 : r0 + GROUP, c0 : c0 + LANES] * carried
            base[r0 : r0 + GROUP, c0 : c0 + LANES] = gated
            squares = squares + gated * gated
        total = jnp.broadcast_to(jnp.sum(squares, axis=1, keepdims=True), (GROUP, LANES))
        total = total.reshape(blocks, 8, LANES)
        ss = ss + jnp.sum(jnp.where(lane8 == block_i + g * blocks, total, 0.0), axis=0)
        run_d = run_d * group_decay[g : g + 1, :]
    ss_mine[...] = ss[None]

    x_copies = []
    for d in range(1, n_head):
        x_copies.append(
            remote(ss_mine, ss_recv.at[pl.ds(mine_h, 1)], x_s.at[d - 1], x_r.at[d - 1], {"head": lax.rem(mine_h + d, n_head)})
        )
    for copy in x_copies:
        copy.start()
    ss_recv[pl.ds(mine_h, 1)] = ss_mine[...]
    for copy in x_copies:
        copy.wait()
    ss = ss_recv[0]
    for h in range(1, n_head):
        ss = ss + ss_recv[h]
    inv = lax.rsqrt(ss * (1.0 / di) + norm_eps)
    for g in range(groups):
        spread = jnp.where(lane8 == block_i + g * blocks, jnp.broadcast_to(inv[None], (blocks, 8, LANES)), 0.0)
        row_inv = jnp.sum(spread.reshape(GROUP, LANES), axis=1, keepdims=True)
        r0 = g * GROUP
        for j in range(tiles):
            c0 = j * LANES
            out_ref[r0 : r0 + GROUP, c0 : c0 + LANES] = (
                base[r0 : r0 + GROUP, c0 : c0 + LANES] * row_inv * gain_ref[:, c0 : c0 + LANES]
            ).astype(BF16)


def on_device(n_seq, n_head, *args):
    (x_raw, bc_raw, gate_in, step_raw, cxw, cxb, cbw, cbb, dt_bias, a_log, d_skip, gain) = args
    length, feat = x_raw.shape[1], x_raw.shape[2]
    heads = dt_bias.shape[0]
    seg_len = SEG if n_seq % SEG == 0 else n_seq
    segs = n_seq // seg_len
    piece = STATE // seg_len
    groups = length // GROUP
    far = max(segs - 1, 1)
    vmem = pl.BlockSpec(memory_space=pltpu.VMEM)
    hbm = pl.BlockSpec(memory_space=pl.ANY)
    dma = pltpu.SemaphoreType.DMA
    scratch = [
        pltpu.VMEM((HALO + length, feat), BF16),
        pltpu.VMEM((HALO + length, 2 * STATE), BF16),
        pltpu.VMEM((length, feat), BF16),
        pltpu.VMEM((length, feat), BF16),
        pltpu.VMEM((length, 2 * STATE), BF16),
        pltpu.VMEM((length, LANES), F32),
        pltpu.VMEM((length, LANES), F32),
        pltpu.VMEM((groups, 16, GROUP), F32),
        pltpu.VMEM((groups, 16, GROUP), F32),
        pltpu.VMEM((8, LANES), F32),
        pltpu.VMEM((8, feat + 2 * STATE), F32),
        pltpu.VMEM((LANES, feat), BF16),
        pltpu.VMEM((GROUP, GROUP), BF16),
        pltpu.VMEM((GROUP, feat), F32),
        pltpu.VMEM((GROUP, feat), BF16),
        pltpu.VMEM((groups, STATE, feat), F32),
        pltpu.VMEM((groups, STATE, feat), F32),
        pltpu.VMEM((length, feat), F32),
        pltpu.VMEM((length, feat), F32),
        pltpu.VMEM((8, LANES), F32),
        pltpu.VMEM((seg_len, piece, feat), BF16),
        pltpu.VMEM((seg_len, piece, feat), BF16),
        pltpu.VMEM((1, 1, LANES), F32),
        pltpu.VMEM((seg_len, 1, LANES), F32),
        pltpu.VMEM((seg_len, piece, feat), F32),
        pltpu.VMEM((1, piece, feat), F32),
        pltpu.VMEM((far, piece, feat), F32),
        pltpu.VMEM((1, 1, LANES), F32),
        pltpu.VMEM((far, 1, LANES), F32),
        pltpu.VMEM((seg_len, piece, feat), F32),
        pltpu.VMEM((seg_len, piece, feat), F32),
        pltpu.VMEM((1, 8, LANES), F32),
        pltpu.VMEM((n_head, 8, LANES), F32),
        dma((3,)),
        dma((2,)), dma((2,)),
        dma((seg_len,)), dma((seg_len,)),
        dma((seg_len,)), dma((seg_len,)),
        dma((far,)), dma((far,)),
        dma((far,)), dma((far,)),
        dma((seg_len,)), dma((seg_len,)),
        dma((n_head,)), dma((n_head,)),
    ]
    sizes = (n_seq, n_head, seg_len, length, feat, heads)
    out = pl.pallas_call(
        functools.partial(kernel, sizes),
        out_shape=jax.ShapeDtypeStruct((length, feat), BF16),
        in_specs=[hbm, hbm, hbm] + [vmem] * 9,
        out_specs=vmem,
        scratch_shapes=scratch,
        compiler_params=pltpu.CompilerParams(
            collective_id=0, has_side_effects=True, vmem_limit_bytes=60 * 1024 * 1024
        ),
        name="ssd_layer",
    )(
        x_raw[0], bc_raw[0], gate_in[0], step_raw[0], cxw, cxb[None], cbw, cbb[None],
        dt_bias[None], a_log[None], d_skip[None], gain[None],
    )
    return out[None]


def solution(mesh):
    in_specs = (
        P(("member", "rep"), "seq", "head"),
        P(("member", "rep"), "seq", None),
        P(("member", "rep"), "seq", "head"),
        P(("member", "rep"), "seq", "head"),
        P("member", "head"),
        P(("member", "head")),
        P("member", None),
        P("member"),
        P(("member", "head")),
        P(("member", "head")),
        P(("member", "head")),
        P(("member", "head")),
    )
    out_specs = P(("member", "rep"), "seq", "head")
    return jax.shard_map(
        functools.partial(on_device, mesh.shape["seq"], mesh.shape["head"]),
        mesh=mesh, in_specs=in_specs, out_specs=out_specs, check_vma=False,
    )
```

```python
import functools

import jax
import jax.numpy as jnp
from jax import lax
from jax.experimental import pallas as pl
from jax.experimental.pallas import tpu as pltpu
from jax.sharding import PartitionSpec as P

HEADDIM = 64
STATE = 128
GROUP = 256
CONV = 4
LANES = 128
HALO = 16
ROWS = 64
SEG = 4
VMEM_LIMIT = 30 * 1024 * 1024
LOG2E = 1.4426950408889634
norm_eps = 1e-05

F32 = jnp.float32
BF16 = jnp.bfloat16
MESH = pl.DeviceIdType.MESH


def silu(v):
    half = 0.5 * v
    return half + half * jnp.tanh(half)


def two_parts(v):
    high = v.astype(BF16)
    return high, (v - high.astype(F32)).astype(BF16)


def three_parts(v):
    high = v.astype(BF16)
    rest = v - high.astype(F32)
    mid = rest.astype(BF16)
    return high, mid, (rest - mid.astype(F32)).astype(BF16)


def dot(a, b, dims=((1,), (0,))):
    return lax.dot_general(a, b, (dims, ((), ())), preferred_element_type=F32)


def kernel(sizes, *refs):
    n_seq, n_head, seg_len, length, feat, heads = sizes
    (
        x_hbm, bc_hbm, gate_hbm, step_hbm, cxw_hbm, cxb_hbm, cbw_hbm, cbb_hbm,
        dt_hbm, alog_hbm, skip_hbm, base,
        step_ref, cxw_ref, cxb_ref, cbw_ref, cbb_ref, dt_ref, alog_ref, skip_ref,
        xext, bcext, gbuf, xconv, bconv, raw_t, stepb, ldb, ldt, stept, par, cw, expand_m, tri_m,
        tail_e, weighted, fresh, entry, scale, dec,
        s_send, a_recv, ld_mine, ld_recv, loc, t_send, b_recv, lt_mine, lt_recv, c_send, inc,
        ss_mine, ss_recv, ready_h, ready_a, ready_b,
        loc_sem, halo_s, halo_r, a_s, a_r, al_s, al_r, b_s, b_r, bl_s, bl_r, c_s, c_r, x_s, x_r,
    ) = refs
    groups = length // GROUP
    tiles = feat // LANES
    piece = STATE // seg_len
    segs = n_seq // seg_len
    di = feat * n_head

    me = lax.axis_index("seq")
    mine_h = lax.axis_index("head")
    seg = me // seg_len
    pos = lax.rem(me, seg_len)

    loads = [
        pltpu.make_async_copy(x_hbm, xext.at[pl.ds(HALO, length)], loc_sem.at[0]),
        pltpu.make_async_copy(bc_hbm, bcext.at[pl.ds(HALO, length)], loc_sem.at[1]),
        pltpu.make_async_copy(gate_hbm, gbuf, loc_sem.at[2]),
        pltpu.make_async_copy(step_hbm, step_ref, loc_sem.at[3]),
        pltpu.make_async_copy(cxw_hbm, cxw_ref, loc_sem.at[4]),
        pltpu.make_async_copy(cxb_hbm, cxb_ref, loc_sem.at[5]),
        pltpu.make_async_copy(cbw_hbm, cbw_ref, loc_sem.at[6]),
        pltpu.make_async_copy(cbb_hbm, cbb_ref, loc_sem.at[7]),
        pltpu.make_async_copy(dt_hbm, dt_ref, loc_sem.at[8]),
        pltpu.make_async_copy(alog_hbm, alog_ref, loc_sem.at[9]),
        pltpu.make_async_copy(skip_hbm, skip_ref, loc_sem.at[10]),
    ]
    for load in loads[3:] + loads[:3]:
        load.start()

    b_recv[...] = jnp.zeros_like(b_recv)
    lt_recv[...] = jnp.zeros_like(lt_recv)
    inc[...] = jnp.zeros_like(inc)
    barrier = pltpu.get_barrier_semaphore()

    def greet(where):
        pl.semaphore_signal(barrier, inc=1, device_id=where, device_id_type=MESH)

    @pl.when(me + 1 < n_seq)
    def _():
        greet({"seq": me + 1})

    for d in range(1, seg_len):

        @pl.when(pos + d < seg_len)
        def _():
            greet({"seq": me + d})

    for k in range(1, segs):

        @pl.when(seg + k < segs)
        def _():
            greet({"seq": me + k * seg_len})

    for d in range(1, n_head):
        greet({"head": lax.rem(mine_h + d, n_head)})

    row_i = lax.broadcasted_iota(jnp.int32, (GROUP, GROUP), 0)
    col_i = lax.broadcasted_iota(jnp.int32, (GROUP, GROUP), 1)
    tri_m[...] = jnp.where(row_i >= col_i, 1.0, 0.0).astype(BF16)
    head_i = lax.broadcasted_iota(jnp.int32, (LANES, feat), 0)
    feat_i = lax.broadcasted_iota(jnp.int32, (LANES, feat), 1)
    expand_m[...] = jnp.where((feat_i >> 6) == head_i, 1.0, 0.0).astype(BF16)
    for load in loads[3:]:
        load.wait()
    par[...] = jnp.zeros_like(par)
    par[0:1, 0:heads] = dt_ref[...]
    par[1:2, 0:heads] = alog_ref[...]
    par[2:3, 0:heads] = skip_ref[...]
    cw[0:CONV, 0:feat] = cxw_ref[...].astype(F32)
    cw[CONV : CONV + 1, 0:feat] = cxb_ref[...].astype(F32).reshape(1, feat)
    cw[0:CONV, feat:] = cbw_ref[...].astype(F32)
    cw[CONV : CONV + 1, feat:] = cbb_ref[...].astype(F32).reshape(1, 2 * STATE)

    def widen3(v):
        total = None
        for part in three_parts(v):
            term = dot(part, expand_m[...])
            total = term if total is None else total + term
        return total

    def widen2(v):
        high, low = two_parts(v)
        return dot(high, expand_m[...]) + dot(low, expand_m[...])

    raw_t[...] = jnp.zeros_like(raw_t)
    for h in range(heads):
        raw_t[h : h + 1, :] = step_ref[h]
    rate = -LOG2E * jnp.exp(par[1:2, :])

    def decays(g, carry):
        r0 = pl.multiple_of(g * GROUP, GROUP)
        raw = raw_t[:, pl.ds(r0, GROUP)].T + par[0:1, :]
        step = jnp.maximum(raw, 0.0) + jnp.log1p(jnp.exp(-jnp.abs(raw)))
        stepb[pl.ds(r0, GROUP), :] = step
        total = None
        for part in three_parts(rate * step):
            term = dot(tri_m[...], part)
            total = term if total is None else total + term
        ldb[pl.ds(r0, GROUP), :] = total
        dec[pl.ds(g, 1), :] = total[GROUP - 1 : GROUP, :]
        return carry

    dec[...] = jnp.zeros_like(dec)
    lax.fori_loop(0, groups, decays, 0)
    ld_total = dec[0:1, :]
    for g in range(1, groups):
        ld_total = ld_total + dec[g : g + 1, :]
    ld_mine[...] = ld_total[None]

    def conv(ext, r, c0, width, tile, w_off):
        block = ext[pl.ds(r, ROWS + HALO), c0 : c0 + width].astype(F32)
        lo = w_off + c0
        acc = cw[CONV : CONV + 1, lo : lo + width]
        for k in range(CONV):
            shift = CONV - 1 - k
            moved = block if shift == 0 else pltpu.roll(block, shift, 0)
            acc = acc + cw[k : k + 1, lo : lo + width] * moved[HALO:]
        return silu(acc)

    def states(g, carry):
        r0 = pl.multiple_of(g * GROUP, GROUP)
        ld = ldb[pl.ds(r0, GROUP), :]
        tail = jnp.exp2(ld[GROUP - 1 : GROUP, :] - ld) * stepb[pl.ds(r0, GROUP), :]
        tail_e[...] = widen2(tail)

        def chunk(i, inner):
            q0 = pl.multiple_of(i * ROWS, ROWS)
            r = pl.multiple_of(r0 + q0, ROWS)
            for j in range(2 * STATE // LANES):
                bconv[pl.ds(r, ROWS), j * LANES : (j + 1) * LANES] = conv(
                    bcext, r, j * LANES, LANES, j, feat
                ).astype(BF16)
            for j in range(tiles):
                c0 = j * LANES
                value = conv(xext, r, c0, LANES, j, 0).astype(BF16)
                xconv[pl.ds(r, ROWS), c0 : c0 + LANES] = value
                weighted[pl.ds(q0, ROWS), c0 : c0 + LANES] = (
                    tail_e[pl.ds(q0, ROWS), c0 : c0 + LANES] * value.astype(F32)
                ).astype(BF16)
            return inner

        lax.fori_loop(0, GROUP // ROWS, chunk, 0)
        fresh[pl.ds(g, 1)] = dot(
            bconv[pl.ds(r0, GROUP), 0:STATE], weighted[...], ((0,), (0,))
        )[None]
        return carry

    for load in loads[:2]:
        load.wait()
    lax.fori_loop(1, groups, states, 0)

    @pl.when(me > 0)
    def _():
        pl.semaphore_wait(barrier, 1 + pos + seg + n_head - 1)
        pl.semaphore_signal(ready_h, inc=1, device_id={"seq": me - 1}, device_id_type=MESH)

    for d in range(1, seg_len):

        @pl.when(pos >= d)
        def _():
            pl.semaphore_signal(ready_a.at[d - 1], inc=1, device_id={"seq": me - d}, device_id_type=MESH)

    for k in range(1, segs):

        @pl.when(seg >= k)
        def _():
            pl.semaphore_signal(ready_b.at[k - 1], inc=1, device_id={"seq": me - k * seg_len}, device_id_type=MESH)

    def remote(src, dst, send, recv, where):
        return pltpu.make_async_remote_copy(
            src_ref=src, dst_ref=dst, send_sem=send, recv_sem=recv,
            device_id=where, device_id_type=MESH,
        )

    halos = [
        remote(xext.at[pl.ds(length, HALO)], xext.at[pl.ds(0, HALO)], halo_s.at[0], halo_r.at[0], {"seq": lax.rem(me + 1, n_seq)}),
        remote(bcext.at[pl.ds(length, HALO)], bcext.at[pl.ds(0, HALO)], halo_s.at[1], halo_r.at[1], {"seq": lax.rem(me + 1, n_seq)}),
    ]

    @pl.when(me + 1 < n_seq)
    def _():
        pl.semaphore_wait(ready_h, 1)
        for copy in halos:
            copy.start()

    def seg_peer(d):
        return {"seq": seg * seg_len + lax.rem(pos + d, seg_len)}

    for d in range(1, seg_len):

        @pl.when(pos + d < seg_len)
        def _():
            pl.semaphore_wait(ready_a.at[d - 1], 1)

    ld_copies = []
    for d in range(1, seg_len):
        ld_copies.append(
            remote(ld_mine, ld_recv.at[pl.ds(pos, 1)], al_s.at[d - 1], al_r.at[d - 1], seg_peer(d))
        )
    for copy in ld_copies:
        copy.start()
    ld_recv[pl.ds(pos, 1)] = ld_mine[...]

    @pl.when(me > 0)
    def _():
        for copy in halos:
            copy.wait_recv()

    @pl.when(me == 0)
    def _():
        xext[0:HALO, :] = jnp.zeros((HALO, feat), BF16)
        bcext[0:HALO, :] = jnp.zeros((HALO, 2 * STATE), BF16)

    states(0, 0)

    group_decay = jnp.exp2(widen3(dec[...]))
    run = fresh[0]
    entry[0] = jnp.zeros((STATE, feat), F32)
    entry[1] = run
    for g in range(1, groups):
        run = group_decay[g : g + 1, :] * run + fresh[g]
        if g + 1 < groups:
            entry[g + 1] = run
    s_send[...] = run.astype(BF16).reshape(seg_len, piece, feat)

    a_copies = []
    for d in range(1, seg_len):
        to = lax.rem(pos + d, seg_len)
        a_copies.append(
            remote(s_send.at[pl.ds(to, 1)], a_recv.at[pl.ds(pos, 1)], a_s.at[d - 1], a_r.at[d - 1], seg_peer(d))
        )
    for copy in reversed(a_copies):
        copy.start()
    a_recv[pl.ds(pos, 1)] = s_send[pl.ds(pos, 1)]

    def transposes(g, carry):
        r0 = pl.multiple_of(g * GROUP, GROUP)
        ldt[pl.ds(g, 1)] = ldb[pl.ds(r0, GROUP), :].T[None, 0:16]
        stept[pl.ds(g, 1)] = stepb[pl.ds(r0, GROUP), :].T[None, 0:16]
        return carry

    skip_e = widen3(par[...])[2:3, :]

    def inside(g, carry):
        r0 = pl.multiple_of(g * GROUP, GROUP)
        scale[pl.ds(r0, GROUP), :] = widen2(jnp.exp2(ldb[pl.ds(r0, GROUP), :]))
        lane = lax.broadcasted_iota(jnp.int32, (ROWS, LANES), 1)
        for tb in range(GROUP // ROWS):
            cols = -(-(tb + 1) * ROWS // LANES) * LANES
            rt = pl.multiple_of(r0 + tb * ROWS, ROWS)
            inter = dot(
                bconv[pl.ds(rt, ROWS), STATE:], bconv[pl.ds(r0, cols), 0:STATE], ((1,), (1,))
            )
            t_i = tb * ROWS + lax.broadcasted_iota(jnp.int32, (ROWS, cols), 0)
            s_i = lax.broadcasted_iota(jnp.int32, (ROWS, cols), 1)
            keep = t_i >= s_i
            for j in range(tiles):
                c0 = j * LANES
                xs = xconv[pl.ds(r0, cols), c0 : c0 + LANES]
                halves = []
                for h in (2 * j, 2 * j + 1):
                    diff = ldb[pl.ds(rt, ROWS), h : h + 1] - ldt[g, h : h + 1, 0:cols]
                    kern = jnp.exp2(jnp.where(keep, diff, -jnp.inf))
                    mix = (inter * kern * stept[g, h : h + 1, 0:cols]).astype(BF16)
                    halves.append(dot(mix, xs))
                intra = jnp.where(lane < HEADDIM, halves[0], halves[1])
                x_t = xconv[pl.ds(rt, ROWS), c0 : c0 + LANES].astype(F32)
                gate = silu(gbuf[pl.ds(rt, ROWS), c0 : c0 + LANES].astype(F32))
                base[pl.ds(rt, ROWS), c0 : c0 + LANES] = (intra + skip_e[:, c0 : c0 + LANES] * x_t) * gate
                scale[pl.ds(rt, ROWS), c0 : c0 + LANES] = scale[pl.ds(rt, ROWS), c0 : c0 + LANES] * gate
        return carry

    lax.fori_loop(0, groups, transposes, 0)
    loads[2].wait()
    lax.fori_loop(0, jnp.where(me == 0, 0, groups), inside, 0)

    for copy in ld_copies:
        copy.wait()
    for copy in a_copies:
        copy.wait()
    lds = jnp.concatenate([ld_recv[q] for q in range(seg_len)], axis=0)
    dec_e = jnp.exp2(widen3(lds))
    run = jnp.zeros((piece, feat), F32)
    run_d = jnp.ones((1, feat), F32)
    seg_ld = ld_recv[0]
    before = []
    for q in range(seg_len):
        loc[q] = run
        before.append(run_d)
        run = dec_e[q : q + 1, :] * run + a_recv[q].astype(F32)
        run_d = run_d * dec_e[q : q + 1, :]
        if q > 0:
            seg_ld = seg_ld + ld_recv[q]
    t_send[...] = run[None]
    lt_mine[...] = seg_ld[None]

    def later_copies(k):
        where = {"seq": lax.rem(me + k * seg_len, n_seq)}
        return [
            remote(t_send, b_recv.at[pl.ds(k - 1, 1)], b_s.at[k - 1], b_r.at[k - 1], where),
            remote(lt_mine, lt_recv.at[pl.ds(k - 1, 1)], bl_s.at[k - 1], bl_r.at[k - 1], where),
        ]

    for k in range(1, segs):

        @pl.when(seg + k < segs)
        def _():
            pl.semaphore_wait(ready_b.at[k - 1], 1)
            for copy in later_copies(k):
                copy.start()

    for k in range(1, segs):

        @pl.when(seg >= k)
        def _():
            for copy in later_copies(k):
                copy.wait_recv()

    lts = jnp.concatenate([lt_recv[k] for k in range(segs - 1)] + [jnp.zeros((8 - segs + 1, LANES), F32)], axis=0)
    far_e = jnp.exp2(widen3(lts))
    carry = jnp.zeros((piece, feat), F32)
    for k in range(segs - 1, 0, -1):
        carry = far_e[k - 1 : k, :] * carry + b_recv[k - 1]
    for q in range(seg_len):
        c_send[q] = loc[q] + before[q] * carry

    c_copies = []
    for d in range(1, seg_len):
        to = lax.rem(pos + d, seg_len)
        copy = remote(c_send.at[pl.ds(to, 1)], inc.at[pl.ds(pos, 1)], c_s.at[d - 1], c_r.at[d - 1], seg_peer(d))
        c_copies.append((seg + to > 0, copy))
    for wanted, copy in c_copies:

        @pl.when(wanted)
        def _():
            copy.start()

    inc[pl.ds(pos, 1)] = c_send[pl.ds(pos, 1)]
    lax.fori_loop(0, jnp.where(me == 0, groups, 0), inside, 0)

    @pl.when(me > 0)
    def _():
        for _, copy in c_copies:
            copy.wait_recv()

    run_d = jnp.ones((1, feat), F32)
    ss = jnp.zeros((8, LANES), F32)
    blocks = GROUP // 8
    lane8 = lax.broadcasted_iota(jnp.int32, (blocks, 8, LANES), 2)
    block_i = lax.broadcasted_iota(jnp.int32, (blocks, 8, LANES), 0)
    for g in range(groups):
        r0 = g * GROUP
        state = entry[g] + run_d * inc[...].reshape(STATE, feat)
        high, low = two_parts(state)
        c_rows = bconv[r0 : r0 + GROUP, STATE:]
        squares = jnp.zeros((GROUP, LANES), F32)
        for j in range(tiles):
            c0 = j * LANES
            carried = dot(c_rows, high[:, c0 : c0 + LANES]) + dot(c_rows, low[:, c0 : c0 + LANES])
            gated = base[r0 : r0 + GROUP, c0 : c0 + LANES] + scale[r0 : r0 + GROUP, c0 : c0 + LANES] * carried
            base[r0 : r0 + GROUP, c0 : c0 + LANES] = gated
            squares = squares + gated * gated
        total = jnp.broadcast_to(jnp.sum(squares, axis=1, keepdims=True), (GROUP, LANES))
        total = total.reshape(blocks, 8, LANES)
        ss = ss + jnp.sum(jnp.where(lane8 == block_i + g * blocks, total, 0.0), axis=0)
        run_d = run_d * group_decay[g : g + 1, :]
    ss_mine[...] = ss[None]

    @pl.when(me == 0)
    def _():
        pl.semaphore_wait(barrier, n_head - 1)

    x_copies = []
    for d in range(1, n_head):
        x_copies.append(
            remote(ss_mine, ss_recv.at[pl.ds(mine_h, 1)], x_s.at[d - 1], x_r.at[d - 1], {"head": lax.rem(mine_h + d, n_head)})
        )
    for copy in x_copies:
        copy.start()
    ss_recv[pl.ds(mine_h, 1)] = ss_mine[...]
    for copy in x_copies:
        copy.wait()
    ss = ss_recv[0]
    for h in range(1, n_head):
        ss = ss + ss_recv[h]
    inv = lax.rsqrt(ss * (1.0 / di) + norm_eps)
    for g in range(groups):
        spread = jnp.where(lane8 == block_i + g * blocks, jnp.broadcast_to(inv[None], (blocks, 8, LANES)), 0.0)
        row_inv = jnp.sum(spread.reshape(GROUP, LANES), axis=1, keepdims=True)
        r0 = g * GROUP
        for j in range(tiles):
            c0 = j * LANES
            base[r0 : r0 + GROUP, c0 : c0 + LANES] = base[r0 : r0 + GROUP, c0 : c0 + LANES] * row_inv

    @pl.when(me + 1 < n_seq)
    def _():
        for copy in halos:
            copy.wait_send()

    for k in range(1, segs):

        @pl.when(seg + k < segs)
        def _():
            for copy in later_copies(k):
                copy.wait_send()

    for wanted, copy in c_copies:

        @pl.when(wanted)
        def _():
            copy.wait_send()


def on_device(n_seq, n_head, *args):
    (x_raw, bc_raw, gate_in, step_raw, cxw, cxb, cbw, cbb, dt_bias, a_log, d_skip, gain) = args
    length, feat = x_raw.shape[1], x_raw.shape[2]
    heads = dt_bias.shape[0]
    seg_len = SEG if n_seq % SEG == 0 else n_seq
    segs = n_seq // seg_len
    piece = STATE // seg_len
    groups = length // GROUP
    far = max(segs - 1, 1)
    vmem = pl.BlockSpec(memory_space=pltpu.VMEM)
    hbm = pl.BlockSpec(memory_space=pltpu.HBM)
    dma = pltpu.SemaphoreType.DMA
    regular = pltpu.SemaphoreType.REGULAR
    scratch = [
        pltpu.VMEM((heads, 1, length), F32),
        pltpu.VMEM((CONV, feat), BF16),
        pltpu.VMEM((feat,), BF16),
        pltpu.VMEM((CONV, 2 * STATE), BF16),
        pltpu.VMEM((2 * STATE,), BF16),
        pltpu.VMEM((1, heads), F32),
        pltpu.VMEM((1, heads), F32),
        pltpu.VMEM((1, heads), F32),
        pltpu.VMEM((HALO + length, feat), BF16),
        pltpu.VMEM((HALO + length, 2 * STATE), BF16),
        pltpu.VMEM((length, feat), BF16),
        pltpu.VMEM((length, feat), BF16),
        pltpu.VMEM((length, 2 * STATE), BF16),
        pltpu.VMEM((LANES, length), F32),
        pltpu.VMEM((length, LANES), F32),
        pltpu.VMEM((length, LANES), F32),
        pltpu.VMEM((groups, 16, GROUP), F32),
        pltpu.VMEM((groups, 16, GROUP), F32),
        pltpu.VMEM((8, LANES), F32),
        pltpu.VMEM((8, feat + 2 * STATE), F32),
        pltpu.VMEM((LANES, feat), BF16),
        pltpu.VMEM((GROUP, GROUP), BF16),
        pltpu.VMEM((GROUP, feat), F32),
        pltpu.VMEM((GROUP, feat), BF16),
        pltpu.VMEM((groups, STATE, feat), F32),
        pltpu.VMEM((groups, STATE, feat), F32),
        pltpu.VMEM((length, feat), F32),
        pltpu.VMEM((8, LANES), F32),
        pltpu.VMEM((seg_len, piece, feat), BF16),
        pltpu.VMEM((seg_len, piece, feat), BF16),
        pltpu.VMEM((1, 1, LANES), F32),
        pltpu.VMEM((seg_len, 1, LANES), F32),
        pltpu.VMEM((seg_len, piece, feat), F32),
        pltpu.VMEM((1, piece, feat), F32),
        pltpu.VMEM((far, piece, feat), F32),
        pltpu.VMEM((1, 1, LANES), F32),
        pltpu.VMEM((far, 1, LANES), F32),
        pltpu.VMEM((seg_len, piece, feat), F32),
        pltpu.VMEM((seg_len, piece, feat), F32),
        pltpu.VMEM((1, 8, LANES), F32),
        pltpu.VMEM((n_head, 8, LANES), F32),
        regular, regular((seg_len,)), regular((far,)),
        dma((11,)),
        dma((2,)), dma((2,)),
        dma((seg_len,)), dma((seg_len,)),
        dma((seg_len,)), dma((seg_len,)),
        dma((far,)), dma((far,)),
        dma((far,)), dma((far,)),
        dma((seg_len,)), dma((seg_len,)),
        dma((n_head,)), dma((n_head,)),
    ]
    sizes = (n_seq, n_head, seg_len, length, feat, heads)
    out = pl.pallas_call(
        functools.partial(kernel, sizes),
        out_shape=jax.ShapeDtypeStruct((length, feat), F32),
        in_specs=[hbm] * 11,
        out_specs=vmem,
        scratch_shapes=scratch,
        compiler_params=pltpu.CompilerParams(
            collective_id=0, has_side_effects=True, vmem_limit_bytes=VMEM_LIMIT
        ),
        name="ssd_layer",
    )(
        x_raw[0], bc_raw[0], gate_in[0], jnp.transpose(step_raw, (2, 0, 1)), cxw, cxb, cbw, cbb,
        dt_bias[None], a_log[None], d_skip[None],
    )
    return (out * gain).astype(BF16)[None]


def solution(mesh):
    in_specs = (
        P(("member", "rep"), "seq", "head"),
        P(("member", "rep"), "seq", None),
        P(("member", "rep"), "seq", "head"),
        P(("member", "rep"), "seq", "head"),
        P("member", "head"),
        P(("member", "head")),
        P("member", None),
        P("member"),
        P(("member", "head")),
        P(("member", "head")),
        P(("member", "head")),
        P(("member", "head")),
    )
    out_specs = P(("member", "rep"), "seq", "head")
    return jax.shard_map(
        functools.partial(on_device, mesh.shape["seq"], mesh.shape["head"]),
        mesh=mesh, in_specs=in_specs, out_specs=out_specs, check_vma=False,
    )
```

```python
import functools

import jax
import jax.numpy as jnp
from jax import lax
from jax.experimental import pallas as pl
from jax.experimental.pallas import tpu as pltpu
from jax.sharding import PartitionSpec as P

HEADDIM = 64
STATE = 128
GROUP = 256
CONV = 4
LANES = 128
HALO = 16
ROWS = 64
SEG = 4
VMEM_LIMIT = 30 * 1024 * 1024
LOG2E = 1.4426950408889634
norm_eps = 1e-05

F32 = jnp.float32
BF16 = jnp.bfloat16
MESH = pl.DeviceIdType.MESH


def silu(v):
    half = 0.5 * v
    return half + half * jnp.tanh(half)


def two_parts(v):
    high = v.astype(BF16)
    return high, (v - high.astype(F32)).astype(BF16)


def three_parts(v):
    high = v.astype(BF16)
    rest = v - high.astype(F32)
    mid = rest.astype(BF16)
    return high, mid, (rest - mid.astype(F32)).astype(BF16)


def dot(a, b, dims=((1,), (0,))):
    return lax.dot_general(a, b, (dims, ((), ())), preferred_element_type=F32)


def kernel(sizes, *refs):
    n_seq, n_head, seg_len, length, feat, heads = sizes
    (
        x_hbm, bc_hbm, gate_hbm, step_hbm, cxw_hbm, cxb_hbm, cbw_hbm, cbb_hbm,
        dt_hbm, alog_hbm, skip_hbm, base,
        step_ref, cxw_ref, cxb_ref, cbw_ref, cbb_ref, dt_ref, alog_ref, skip_ref,
        xext, bcext, gbuf, xconv, bconv, raw_t, stepb, ldb, ldt, stept, par, cw, expand_m, tri_m,
        tail_e, weighted, fresh, entry, scale, dec,
        s_send, a_recv, ld_mine, ld_recv, loc, t_send, b_recv, c_send, inc,
        ss_mine, ss_recv, ready_h, ready_a, ready_b,
        loc_sem, halo_s, halo_r, a_s, a_r, al_s, al_r, b_s, b_r, c_s, c_r, x_s, x_r,
    ) = refs
    groups = length // GROUP
    tiles = feat // LANES
    piece = STATE // seg_len
    segs = n_seq // seg_len
    di = feat * n_head

    me = lax.axis_index("seq")
    mine_h = lax.axis_index("head")
    seg = me // seg_len
    pos = lax.rem(me, seg_len)

    loads = [
        pltpu.make_async_copy(x_hbm, xext.at[pl.ds(HALO, length)], loc_sem.at[0]),
        pltpu.make_async_copy(bc_hbm, bcext.at[pl.ds(HALO, length)], loc_sem.at[1]),
        pltpu.make_async_copy(gate_hbm, gbuf, loc_sem.at[2]),
        pltpu.make_async_copy(step_hbm, step_ref, loc_sem.at[3]),
        pltpu.make_async_copy(cxw_hbm, cxw_ref, loc_sem.at[4]),
        pltpu.make_async_copy(cxb_hbm, cxb_ref, loc_sem.at[5]),
        pltpu.make_async_copy(cbw_hbm, cbw_ref, loc_sem.at[6]),
        pltpu.make_async_copy(cbb_hbm, cbb_ref, loc_sem.at[7]),
        pltpu.make_async_copy(dt_hbm, dt_ref, loc_sem.at[8]),
        pltpu.make_async_copy(alog_hbm, alog_ref, loc_sem.at[9]),
        pltpu.make_async_copy(skip_hbm, skip_ref, loc_sem.at[10]),
    ]
    for load in loads[3:] + loads[:3]:
        load.start()

    b_recv[...] = jnp.zeros_like(b_recv)
    inc[...] = jnp.zeros_like(inc)
    barrier = pltpu.get_barrier_semaphore()

    def greet(where):
        pl.semaphore_signal(barrier, inc=1, device_id=where, device_id_type=MESH)

    @pl.when(me + 1 < n_seq)
    def _():
        greet({"seq": me + 1})

    for d in range(1, seg_len):

        @pl.when(pos + d < seg_len)
        def _():
            greet({"seq": me + d})

    @pl.when(seg + 1 < segs)
    def _():
        greet({"seq": me + seg_len})

    for d in range(1, n_head):
        greet({"head": lax.rem(mine_h + d, n_head)})

    row_i = lax.broadcasted_iota(jnp.int32, (GROUP, GROUP), 0)
    col_i = lax.broadcasted_iota(jnp.int32, (GROUP, GROUP), 1)
    tri_m[...] = jnp.where(row_i >= col_i, 1.0, 0.0).astype(BF16)
    head_i = lax.broadcasted_iota(jnp.int32, (LANES, feat), 0)
    feat_i = lax.broadcasted_iota(jnp.int32, (LANES, feat), 1)
    expand_m[...] = jnp.where((feat_i >> 6) == head_i, 1.0, 0.0).astype(BF16)
    for load in loads[3:]:
        load.wait()
    par[...] = jnp.zeros_like(par)
    par[0:1, 0:heads] = dt_ref[...]
    par[1:2, 0:heads] = alog_ref[...]
    par[2:3, 0:heads] = skip_ref[...]
    cw[0:CONV, 0:feat] = cxw_ref[...].astype(F32)
    cw[CONV : CONV + 1, 0:feat] = cxb_ref[...].astype(F32).reshape(1, feat)
    cw[0:CONV, feat:] = cbw_ref[...].astype(F32)
    cw[CONV : CONV + 1, feat:] = cbb_ref[...].astype(F32).reshape(1, 2 * STATE)

    def widen3(v):
        total = None
        for part in three_parts(v):
            term = dot(part, expand_m[...])
            total = term if total is None else total + term
        return total

    def widen2(v):
        high, low = two_parts(v)
        return dot(high, expand_m[...]) + dot(low, expand_m[...])

    raw_t[...] = jnp.zeros_like(raw_t)
    for h in range(heads):
        raw_t[h : h + 1, :] = step_ref[h]
    rate = -LOG2E * jnp.exp(par[1:2, :])

    def decays(g, carry):
        r0 = pl.multiple_of(g * GROUP, GROUP)
        raw = raw_t[:, pl.ds(r0, GROUP)].T + par[0:1, :]
        step = jnp.maximum(raw, 0.0) + jnp.log1p(jnp.exp(-jnp.abs(raw)))
        stepb[pl.ds(r0, GROUP), :] = step
        total = None
        for part in three_parts(rate * step):
            term = dot(tri_m[...], part)
            total = term if total is None else total + term
        ldb[pl.ds(r0, GROUP), :] = total
        dec[pl.ds(g, 1), :] = total[GROUP - 1 : GROUP, :]
        return carry

    dec[...] = jnp.zeros_like(dec)
    lax.fori_loop(0, groups, decays, 0)
    ld_total = dec[0:1, :]
    for g in range(1, groups):
        ld_total = ld_total + dec[g : g + 1, :]
    ld_mine[...] = ld_total[None]

    def conv(ext, r, c0, width, tile, w_off):
        block = ext[pl.ds(r, ROWS + HALO), c0 : c0 + width].astype(F32)
        lo = w_off + c0
        acc = cw[CONV : CONV + 1, lo : lo + width]
        for k in range(CONV):
            shift = CONV - 1 - k
            moved = block if shift == 0 else pltpu.roll(block, shift, 0)
            acc = acc + cw[k : k + 1, lo : lo + width] * moved[HALO:]
        return silu(acc)

    def states(g, carry):
        r0 = pl.multiple_of(g * GROUP, GROUP)
        ld = ldb[pl.ds(r0, GROUP), :]
        tail = jnp.exp2(ld[GROUP - 1 : GROUP, :] - ld) * stepb[pl.ds(r0, GROUP), :]
        tail_e[...] = widen2(tail)

        def chunk(i, inner):
            q0 = pl.multiple_of(i * ROWS, ROWS)
            r = pl.multiple_of(r0 + q0, ROWS)
            for j in range(2 * STATE // LANES):
                bconv[pl.ds(r, ROWS), j * LANES : (j + 1) * LANES] = conv(
                    bcext, r, j * LANES, LANES, j, feat
                ).astype(BF16)
            for j in range(tiles):
                c0 = j * LANES
                value = conv(xext, r, c0, LANES, j, 0).astype(BF16)
                xconv[pl.ds(r, ROWS), c0 : c0 + LANES] = value
                weighted[pl.ds(q0, ROWS), c0 : c0 + LANES] = (
                    tail_e[pl.ds(q0, ROWS), c0 : c0 + LANES] * value.astype(F32)
                ).astype(BF16)
            return inner

        lax.fori_loop(0, GROUP // ROWS, chunk, 0)
        fresh[pl.ds(g, 1)] = dot(
            bconv[pl.ds(r0, GROUP), 0:STATE], weighted[...], ((0,), (0,))
        )[None]
        return carry

    for load in loads[:2]:
        load.wait()
    lax.fori_loop(1, groups, states, 0)

    @pl.when(me > 0)
    def _():
        pl.semaphore_wait(barrier, 1 + pos + jnp.where(seg > 0, 1, 0) + n_head - 1)
        pl.semaphore_signal(ready_h, inc=1, device_id={"seq": me - 1}, device_id_type=MESH)

    for d in range(1, seg_len):

        @pl.when(pos >= d)
        def _():
            pl.semaphore_signal(ready_a.at[d - 1], inc=1, device_id={"seq": me - d}, device_id_type=MESH)

    @pl.when(seg > 0)
    def _():
        pl.semaphore_signal(ready_b, inc=1, device_id={"seq": me - seg_len}, device_id_type=MESH)

    def remote(src, dst, send, recv, where):
        return pltpu.make_async_remote_copy(
            src_ref=src, dst_ref=dst, send_sem=send, recv_sem=recv,
            device_id=where, device_id_type=MESH,
        )

    halos = [
        remote(xext.at[pl.ds(length, HALO)], xext.at[pl.ds(0, HALO)], halo_s.at[0], halo_r.at[0], {"seq": lax.rem(me + 1, n_seq)}),
        remote(bcext.at[pl.ds(length, HALO)], bcext.at[pl.ds(0, HALO)], halo_s.at[1], halo_r.at[1], {"seq": lax.rem(me + 1, n_seq)}),
    ]

    @pl.when(me + 1 < n_seq)
    def _():
        pl.semaphore_wait(ready_h, 1)
        for copy in halos:
            copy.start()

    def seg_peer(d):
        return {"seq": seg * seg_len + lax.rem(pos + d, seg_len)}

    for d in range(1, seg_len):

        @pl.when(pos + d < seg_len)
        def _():
            pl.semaphore_wait(ready_a.at[d - 1], 1)

    ld_copies = []
    for d in range(1, seg_len):
        ld_copies.append(
            remote(ld_mine, ld_recv.at[pl.ds(pos, 1)], al_s.at[d - 1], al_r.at[d - 1], seg_peer(d))
        )
    for copy in ld_copies:
        copy.start()
    ld_recv[pl.ds(pos, 1)] = ld_mine[...]

    @pl.when(me > 0)
    def _():
        for copy in halos:
            copy.wait_recv()

    @pl.when(me == 0)
    def _():
        xext[0:HALO, :] = jnp.zeros((HALO, feat), BF16)
        bcext[0:HALO, :] = jnp.zeros((HALO, 2 * STATE), BF16)

    states(0, 0)

    group_decay = jnp.exp2(widen3(dec[...]))
    run = fresh[0]
    entry[0] = jnp.zeros((STATE, feat), F32)
    entry[1] = run
    for g in range(1, groups):
        run = group_decay[g : g + 1, :] * run + fresh[g]
        if g + 1 < groups:
            entry[g + 1] = run
    s_send[...] = run.astype(BF16).reshape(seg_len, piece, feat)

    a_copies = []
    for d in range(1, seg_len):
        to = lax.rem(pos + d, seg_len)
        a_copies.append(
            remote(s_send.at[pl.ds(to, 1)], a_recv.at[pl.ds(pos, 1)], a_s.at[d - 1], a_r.at[d - 1], seg_peer(d))
        )
    for copy in reversed(a_copies):
        copy.start()
    a_recv[pl.ds(pos, 1)] = s_send[pl.ds(pos, 1)]

    def transposes(g, carry):
        r0 = pl.multiple_of(g * GROUP, GROUP)
        ldt[pl.ds(g, 1)] = ldb[pl.ds(r0, GROUP), :].T[None, 0:16]
        stept[pl.ds(g, 1)] = stepb[pl.ds(r0, GROUP), :].T[None, 0:16]
        return carry

    skip_e = widen3(par[...])[2:3, :]

    def inside(g, carry):
        r0 = pl.multiple_of(g * GROUP, GROUP)
        scale[pl.ds(r0, GROUP), :] = widen2(jnp.exp2(ldb[pl.ds(r0, GROUP), :]))
        lane = lax.broadcasted_iota(jnp.int32, (ROWS, LANES), 1)
        for tb in range(GROUP // ROWS):
            cols = -(-(tb + 1) * ROWS // LANES) * LANES
            rt = pl.multiple_of(r0 + tb * ROWS, ROWS)
            inter = dot(
                bconv[pl.ds(rt, ROWS), STATE:], bconv[pl.ds(r0, cols), 0:STATE], ((1,), (1,))
            )
            t_i = tb * ROWS + lax.broadcasted_iota(jnp.int32, (ROWS, cols), 0)
            s_i = lax.broadcasted_iota(jnp.int32, (ROWS, cols), 1)
            keep = t_i >= s_i
            for j in range(tiles):
                c0 = j * LANES
                xs = xconv[pl.ds(r0, cols), c0 : c0 + LANES]
                halves = []
                for h in (2 * j, 2 * j + 1):
                    diff = ldb[pl.ds(rt, ROWS), h : h + 1] - ldt[g, h : h + 1, 0:cols]
                    kern = jnp.exp2(jnp.where(keep, diff, -jnp.inf))
                    mix = (inter * kern * stept[g, h : h + 1, 0:cols]).astype(BF16)
                    halves.append(dot(mix, xs))
                intra = jnp.where(lane < HEADDIM, halves[0], halves[1])
                x_t = xconv[pl.ds(rt, ROWS), c0 : c0 + LANES].astype(F32)
                gate = silu(gbuf[pl.ds(rt, ROWS), c0 : c0 + LANES].astype(F32))
                base[pl.ds(rt, ROWS), c0 : c0 + LANES] = (intra + skip_e[:, c0 : c0 + LANES] * x_t) * gate
                scale[pl.ds(rt, ROWS), c0 : c0 + LANES] = scale[pl.ds(rt, ROWS), c0 : c0 + LANES] * gate
        return carry

    lax.fori_loop(0, groups, transposes, 0)
    loads[2].wait()
    lax.fori_loop(0, jnp.where(me == 0, 0, groups), inside, 0)

    for copy in ld_copies:
        copy.wait()
    for copy in a_copies:
        copy.wait()
    lds = jnp.concatenate([ld_recv[q] for q in range(seg_len)], axis=0)
    dec_e = jnp.exp2(widen3(lds))
    run = jnp.zeros((piece, feat), F32)
    run_d = jnp.ones((1, feat), F32)
    before = []
    for q in range(seg_len):
        loc[q] = run
        before.append(run_d)
        run = dec_e[q : q + 1, :] * run + a_recv[q].astype(F32)
        run_d = run_d * dec_e[q : q + 1, :]

    onward = remote(t_send, b_recv, b_s, b_r, {"seq": lax.rem(me + seg_len, n_seq)})

    @pl.when(seg > 0)
    def _():
        onward.wait_recv()

    carry = b_recv[0]
    t_send[...] = (run + run_d * carry)[None]

    @pl.when(seg + 1 < segs)
    def _():
        pl.semaphore_wait(ready_b, 1)
        onward.start()

    for q in range(seg_len):
        c_send[q] = loc[q] + before[q] * carry

    c_copies = []
    for d in range(1, seg_len):
        to = lax.rem(pos + d, seg_len)
        copy = remote(c_send.at[pl.ds(to, 1)], inc.at[pl.ds(pos, 1)], c_s.at[d - 1], c_r.at[d - 1], seg_peer(d))
        c_copies.append((seg + to > 0, copy))
    for wanted, copy in c_copies:

        @pl.when(wanted)
        def _():
            copy.start()

    inc[pl.ds(pos, 1)] = c_send[pl.ds(pos, 1)]
    lax.fori_loop(0, jnp.where(me == 0, groups, 0), inside, 0)

    @pl.when(me > 0)
    def _():
        for _, copy in c_copies:
            copy.wait_recv()

    run_d = jnp.ones((1, feat), F32)
    ss = jnp.zeros((8, LANES), F32)
    blocks = GROUP // 8
    lane8 = lax.broadcasted_iota(jnp.int32, (blocks, 8, LANES), 2)
    block_i = lax.broadcasted_iota(jnp.int32, (blocks, 8, LANES), 0)
    for g in range(groups):
        r0 = g * GROUP
        state = entry[g] + run_d * inc[...].reshape(STATE, feat)
        high, low = two_parts(state)
        c_rows = bconv[r0 : r0 + GROUP, STATE:]
        squares = jnp.zeros((GROUP, LANES), F32)
        for j in range(tiles):
            c0 = j * LANES
            carried = dot(c_rows, high[:, c0 : c0 + LANES]) + dot(c_rows, low[:, c0 : c0 + LANES])
            gated = base[r0 : r0 + GROUP, c0 : c0 + LANES] + scale[r0 : r0 + GROUP, c0 : c0 + LANES] * carried
            base[r0 : r0 + GROUP, c0 : c0 + LANES] = gated
            squares = squares + gated * gated
        total = jnp.broadcast_to(jnp.sum(squares, axis=1, keepdims=True), (GROUP, LANES))
        total = total.reshape(blocks, 8, LANES)
        ss = ss + jnp.sum(jnp.where(lane8 == block_i + g * blocks, total, 0.0), axis=0)
        run_d = run_d * group_decay[g : g + 1, :]
    ss_mine[...] = ss[None]

    @pl.when(me == 0)
    def _():
        pl.semaphore_wait(barrier, n_head - 1)

    x_copies = []
    for d in range(1, n_head):
        x_copies.append(
            remote(ss_mine, ss_recv.at[pl.ds(mine_h, 1)], x_s.at[d - 1], x_r.at[d - 1], {"head": lax.rem(mine_h + d, n_head)})
        )
    for copy in x_copies:
        copy.start()
    ss_recv[pl.ds(mine_h, 1)] = ss_mine[...]
    for copy in x_copies:
        copy.wait()
    ss = ss_recv[0]
    for h in range(1, n_head):
        ss = ss + ss_recv[h]
    inv = lax.rsqrt(ss * (1.0 / di) + norm_eps)
    for g in range(groups):
        spread = jnp.where(lane8 == block_i + g * blocks, jnp.broadcast_to(inv[None], (blocks, 8, LANES)), 0.0)
        row_inv = jnp.sum(spread.reshape(GROUP, LANES), axis=1, keepdims=True)
        r0 = g * GROUP
        for j in range(tiles):
            c0 = j * LANES
            base[r0 : r0 + GROUP, c0 : c0 + LANES] = base[r0 : r0 + GROUP, c0 : c0 + LANES] * row_inv

    @pl.when(me + 1 < n_seq)
    def _():
        for copy in halos:
            copy.wait_send()

    @pl.when(seg + 1 < segs)
    def _():
        onward.wait_send()

    for wanted, copy in c_copies:

        @pl.when(wanted)
        def _():
            copy.wait_send()


def on_device(n_seq, n_head, *args):
    (x_raw, bc_raw, gate_in, step_raw, cxw, cxb, cbw, cbb, dt_bias, a_log, d_skip, gain) = args
    length, feat = x_raw.shape[1], x_raw.shape[2]
    heads = dt_bias.shape[0]
    seg_len = SEG if n_seq % SEG == 0 else n_seq
    piece = STATE // seg_len
    groups = length // GROUP
    vmem = pl.BlockSpec(memory_space=pltpu.VMEM)
    hbm = pl.BlockSpec(memory_space=pltpu.HBM)
    dma = pltpu.SemaphoreType.DMA
    regular = pltpu.SemaphoreType.REGULAR
    scratch = [
        pltpu.VMEM((heads, 1, length), F32),
        pltpu.VMEM((CONV, feat), BF16),
        pltpu.VMEM((feat,), BF16),
        pltpu.VMEM((CONV, 2 * STATE), BF16),
        pltpu.VMEM((2 * STATE,), BF16),
        pltpu.VMEM((1, heads), F32),
        pltpu.VMEM((1, heads), F32),
        pltpu.VMEM((1, heads), F32),
        pltpu.VMEM((HALO + length, feat), BF16),
        pltpu.VMEM((HALO + length, 2 * STATE), BF16),
        pltpu.VMEM((length, feat), BF16),
        pltpu.VMEM((length, feat), BF16),
        pltpu.VMEM((length, 2 * STATE), BF16),
        pltpu.VMEM((LANES, length), F32),
        pltpu.VMEM((length, LANES), F32),
        pltpu.VMEM((length, LANES), F32),
        pltpu.VMEM((groups, 16, GROUP), F32),
        pltpu.VMEM((groups, 16, GROUP), F32),
        pltpu.VMEM((8, LANES), F32),
        pltpu.VMEM((8, feat + 2 * STATE), F32),
        pltpu.VMEM((LANES, feat), BF16),
        pltpu.VMEM((GROUP, GROUP), BF16),
        pltpu.VMEM((GROUP, feat), F32),
        pltpu.VMEM((GROUP, feat), BF16),
        pltpu.VMEM((groups, STATE, feat), F32),
        pltpu.VMEM((groups, STATE, feat), F32),
        pltpu.VMEM((length, feat), F32),
        pltpu.VMEM((8, LANES), F32),
        pltpu.VMEM((seg_len, piece, feat), BF16),
        pltpu.VMEM((seg_len, piece, feat), BF16),
        pltpu.VMEM((1, 1, LANES), F32),
        pltpu.VMEM((seg_len, 1, LANES), F32),
        pltpu.VMEM((seg_len, piece, feat), F32),
        pltpu.VMEM((1, piece, feat), F32),
        pltpu.VMEM((1, piece, feat), F32),
        pltpu.VMEM((seg_len, piece, feat), F32),
        pltpu.VMEM((seg_len, piece, feat), F32),
        pltpu.VMEM((1, 8, LANES), F32),
        pltpu.VMEM((n_head, 8, LANES), F32),
        regular, regular((seg_len,)), regular,
        dma((11,)),
        dma((2,)), dma((2,)),
        dma((seg_len,)), dma((seg_len,)),
        dma((seg_len,)), dma((seg_len,)),
        dma, dma,
        dma((seg_len,)), dma((seg_len,)),
        dma((n_head,)), dma((n_head,)),
    ]
    sizes = (n_seq, n_head, seg_len, length, feat, heads)
    keep = lambda v: pltpu.with_memory_space_constraint(v, pltpu.HBM)
    out = pl.pallas_call(
        functools.partial(kernel, sizes),
        out_shape=jax.ShapeDtypeStruct((length, feat), F32),
        in_specs=[hbm] * 11,
        out_specs=vmem,
        scratch_shapes=scratch,
        compiler_params=pltpu.CompilerParams(
            collective_id=0, has_side_effects=True, vmem_limit_bytes=VMEM_LIMIT
        ),
        name="ssd_layer",
    )(
        *map(keep, (
            x_raw[0], bc_raw[0], gate_in[0], jnp.transpose(step_raw, (2, 0, 1)), cxw, cxb, cbw, cbb,
            dt_bias[None], a_log[None], d_skip[None],
        ))
    )
    return (out * gain).astype(BF16)[None]


def solution(mesh):
    in_specs = (
        P(("member", "rep"), "seq", "head"),
        P(("member", "rep"), "seq", None),
        P(("member", "rep"), "seq", "head"),
        P(("member", "rep"), "seq", "head"),
        P("member", "head"),
        P(("member", "head")),
        P("member", None),
        P("member"),
        P(("member", "head")),
        P(("member", "head")),
        P(("member", "head")),
        P(("member", "head")),
    )
    out_specs = P(("member", "rep"), "seq", "head")
    return jax.shard_map(
        functools.partial(on_device, mesh.shape["seq"], mesh.shape["head"]),
        mesh=mesh, in_specs=in_specs, out_specs=out_specs, check_vma=False,
    )
```

```python
import functools

import jax
import jax.numpy as jnp
from jax import lax
from jax.experimental import pallas as pl
from jax.experimental.pallas import tpu as pltpu
from jax.sharding import PartitionSpec as P

HEADDIM = 64
STATE = 128
GROUP = 256
CONV = 4
LANES = 128
HALO = 16
ROWS = 64
SEG = 4
VMEM_LIMIT = 30 * 1024 * 1024
LOG2E = 1.4426950408889634
norm_eps = 1e-05

F32 = jnp.float32
BF16 = jnp.bfloat16
MESH = pl.DeviceIdType.MESH


def silu_of_half(half):
    return half + half * jnp.tanh(half)


def two_parts(v):
    high = v.astype(BF16)
    return high, (v - high.astype(F32)).astype(BF16)


def three_parts(v):
    high = v.astype(BF16)
    rest = v - high.astype(F32)
    mid = rest.astype(BF16)
    return high, mid, (rest - mid.astype(F32)).astype(BF16)


def dot(a, b, dims=((1,), (0,))):
    return lax.dot_general(a, b, (dims, ((), ())), preferred_element_type=F32)


def kernel(sizes, *refs):
    n_seq, n_head, seg_len, length, feat, heads = sizes
    (
        x_hbm, bc_hbm, gate_hbm, step_hbm, cxw_hbm, cxb_hbm, cbw_hbm, cbb_hbm,
        dt_hbm, alog_hbm, skip_hbm, base,
        step_ref, cxw_ref, cxb_ref, cbw_ref, cbb_ref, dt_ref, alog_ref, skip_ref,
        xext, bcext, gbuf, xconv, bconv, raw_t, shifts, stepb, ldb, ldt, stept, par, cw, expand_m, tri_m,
        tail_e, weighted, fresh, entry, scale, dec,
        s_send, a_recv, ld_mine, ld_recv, loc, t_send, b_recv, lx_mine, lx_recv, f_recv, c_send, inc,
        ss_mine, ss_recv, ready_h, ready_a, ready_b, ready_w,
        loc_sem, halo_s, halo_r, a_s, a_r, al_s, al_r, b_s, b_r, bl_s, bl_r, f_s, f_r, fw_s, c_s, c_r, x_s, x_r,
    ) = refs
    groups = length // GROUP
    tiles = feat // LANES
    piece = STATE // seg_len
    segs = n_seq // seg_len
    di = feat * n_head

    middle = segs // 2
    wrap = segs - 1 > middle
    me = lax.axis_index("seq")
    mine_h = lax.axis_index("head")
    seg = me // seg_len
    pos = lax.rem(me, seg_len)
    last_seg = jnp.where(seg == segs - 1, 1, 0) if wrap else 0

    loads = [
        pltpu.make_async_copy(x_hbm, xext.at[pl.ds(HALO, length)], loc_sem.at[0]),
        pltpu.make_async_copy(bc_hbm, bcext.at[pl.ds(HALO, length)], loc_sem.at[1]),
        pltpu.make_async_copy(gate_hbm, gbuf, loc_sem.at[2]),
        pltpu.make_async_copy(step_hbm, step_ref, loc_sem.at[3]),
        pltpu.make_async_copy(cxw_hbm, cxw_ref, loc_sem.at[4]),
        pltpu.make_async_copy(cxb_hbm, cxb_ref, loc_sem.at[5]),
        pltpu.make_async_copy(cbw_hbm, cbw_ref, loc_sem.at[6]),
        pltpu.make_async_copy(cbb_hbm, cbb_ref, loc_sem.at[7]),
        pltpu.make_async_copy(dt_hbm, dt_ref, loc_sem.at[8]),
        pltpu.make_async_copy(alog_hbm, alog_ref, loc_sem.at[9]),
        pltpu.make_async_copy(skip_hbm, skip_ref, loc_sem.at[10]),
    ]
    for load in loads[3:] + loads[:3]:
        load.start()

    b_recv[...] = jnp.zeros_like(b_recv)
    lx_recv[...] = jnp.zeros_like(lx_recv)
    inc[...] = jnp.zeros_like(inc)
    barrier = pltpu.get_barrier_semaphore()

    def greet(where):
        pl.semaphore_signal(barrier, inc=1, device_id=where, device_id_type=MESH)

    @pl.when(me + 1 < n_seq)
    def _():
        greet({"seq": me + 1})

    for d in range(1, seg_len):

        @pl.when(pos + d < seg_len)
        def _():
            greet({"seq": me + d})

    @pl.when(seg + 1 < segs)
    def _():
        greet({"seq": me + seg_len})

    if wrap:

        @pl.when(seg == 0)
        def _():
            greet({"seq": me + (segs - 1) * seg_len})

    for d in range(1, n_head):
        greet({"head": lax.rem(mine_h + d, n_head)})

    row_i = lax.broadcasted_iota(jnp.int32, (GROUP, GROUP), 0)
    col_i = lax.broadcasted_iota(jnp.int32, (GROUP, GROUP), 1)
    tri_m[...] = jnp.where(row_i <= col_i, 1.0, 0.0).astype(BF16)
    head_i = lax.broadcasted_iota(jnp.int32, (2 * LANES, feat), 0)
    feat_i = lax.broadcasted_iota(jnp.int32, (2 * LANES, feat), 1)
    expand_m[...] = jnp.where((feat_i >> 6) == (head_i & (LANES - 1)), 1.0, 0.0).astype(BF16)
    for load in loads[3:]:
        load.wait()
    par[...] = jnp.zeros_like(par)
    par[0:1, 0:heads] = dt_ref[...]
    par[1:2, 0:heads] = alog_ref[...]
    par[2:3, 0:heads] = skip_ref[...]
    cw[0:CONV, 0:feat] = 0.5 * cxw_ref[...].astype(F32)
    cw[CONV : CONV + 1, 0:feat] = 0.5 * cxb_ref[...].astype(F32).reshape(1, feat)
    cw[0:CONV, feat:] = 0.5 * cbw_ref[...].astype(F32)
    cw[CONV : CONV + 1, feat:] = 0.5 * cbb_ref[...].astype(F32).reshape(1, 2 * STATE)

    def widen3(v):
        total = None
        for part in three_parts(v):
            term = dot(part, expand_m[0:LANES, :])
            total = term if total is None else total + term
        return total

    def widen2(v):
        high, low = two_parts(v)
        return dot(jnp.concatenate([high, low], axis=1), expand_m[...])

    raw_t[...] = jnp.zeros_like(raw_t)
    for h in range(heads):
        raw_t[h : h + 1, :] = step_ref[h]
    par_t = par[...].T
    raw = raw_t[...] + par_t[0:16, 0:1]
    step = jnp.maximum(raw, 0.0) + jnp.log1p(jnp.exp(-jnp.abs(raw)))
    raw_t[...] = step
    rates = jnp.concatenate(three_parts(-LOG2E * jnp.exp(par_t[0:16, 1:2]) * step), axis=0)
    rest = jnp.zeros((LANES - 16, GROUP), F32)
    dec[...] = jnp.zeros_like(dec)
    for g in range(groups):
        r0 = g * GROUP
        sums = dot(rates[:, r0 : r0 + GROUP], tri_m[...])
        sums = sums[0:16] + sums[16:32] + sums[32:48]
        ldt[g] = sums
        stept[g] = raw_t[:, r0 : r0 + GROUP]
        ldb[r0 : r0 + GROUP, :] = jnp.concatenate([sums, rest], axis=0).T
        stepb[r0 : r0 + GROUP, :] = jnp.concatenate([stept[g], rest], axis=0).T
        dec[g : g + 1, :] = ldb[r0 + GROUP - 1 : r0 + GROUP, :]
    ld_total = dec[0:1, :]
    for g in range(1, groups):
        ld_total = ld_total + dec[g : g + 1, :]
    ld_mine[...] = ld_total[None]

    def conv(ext, r, j, w_off):
        slot = j + w_off // LANES
        shifts[slot] = ext[pl.ds(r, ROWS + HALO), j * LANES : (j + 1) * LANES].astype(F32)
        lo = w_off + j * LANES
        acc = cw[CONV : CONV + 1, lo : lo + LANES]
        for k in range(CONV):
            start = HALO - (CONV - 1 - k)
            acc = acc + cw[k : k + 1, lo : lo + LANES] * shifts[slot, start : start + ROWS, :]
        return silu_of_half(acc)

    def states(g, carry):
        r0 = pl.multiple_of(g * GROUP, GROUP)
        ld = ldb[pl.ds(r0, GROUP), :]
        tail = jnp.exp2(ld[GROUP - 1 : GROUP, :] - ld) * stepb[pl.ds(r0, GROUP), :]
        tail_e[...] = widen2(tail)

        def chunk(i, inner):
            q0 = pl.multiple_of(i * ROWS, ROWS)
            r = pl.multiple_of(r0 + q0, ROWS)
            for j in range(2 * STATE // LANES):
                bconv[pl.ds(r, ROWS), j * LANES : (j + 1) * LANES] = conv(bcext, r, j, feat).astype(BF16)
            for j in range(tiles):
                c0 = j * LANES
                value = conv(xext, r, j, 0).astype(BF16)
                xconv[pl.ds(r, ROWS), c0 : c0 + LANES] = value
                weighted[pl.ds(q0, ROWS), c0 : c0 + LANES] = (
                    tail_e[pl.ds(q0, ROWS), c0 : c0 + LANES] * value.astype(F32)
                ).astype(BF16)
            return inner

        lax.fori_loop(0, GROUP // ROWS, chunk, 0)
        fresh[pl.ds(g, 1)] = dot(
            bconv[pl.ds(r0, GROUP), 0:STATE], weighted[...], ((0,), (0,))
        )[None]
        return carry

    for load in loads[:2]:
        load.wait()
    lax.fori_loop(1, groups, states, 0)

    @pl.when(me > 0)
    def _():
        pl.semaphore_wait(barrier, 1 + pos + jnp.where(seg > 0, 1, 0) + n_head - 1 + last_seg)
        pl.semaphore_signal(ready_h, inc=1, device_id={"seq": me - 1}, device_id_type=MESH)

    for d in range(1, seg_len):

        @pl.when(pos >= d)
        def _():
            pl.semaphore_signal(ready_a.at[d - 1], inc=1, device_id={"seq": me - d}, device_id_type=MESH)

    @pl.when(seg > 0)
    def _():
        pl.semaphore_signal(ready_b, inc=1, device_id={"seq": me - seg_len}, device_id_type=MESH)

    if wrap:

        @pl.when(seg == segs - 1)
        def _():
            pl.semaphore_signal(ready_w, inc=1, device_id={"seq": me - (segs - 1) * seg_len}, device_id_type=MESH)

    def remote(src, dst, send, recv, where):
        return pltpu.make_async_remote_copy(
            src_ref=src, dst_ref=dst, send_sem=send, recv_sem=recv,
            device_id=where, device_id_type=MESH,
        )

    halos = [
        remote(xext.at[pl.ds(length, HALO)], xext.at[pl.ds(0, HALO)], halo_s.at[0], halo_r.at[0], {"seq": lax.rem(me + 1, n_seq)}),
        remote(bcext.at[pl.ds(length, HALO)], bcext.at[pl.ds(0, HALO)], halo_s.at[1], halo_r.at[1], {"seq": lax.rem(me + 1, n_seq)}),
    ]

    @pl.when(me + 1 < n_seq)
    def _():
        pl.semaphore_wait(ready_h, 1)
        for copy in halos:
            copy.start()

    def seg_peer(d):
        return {"seq": seg * seg_len + lax.rem(pos + d, seg_len)}

    for d in range(1, seg_len):

        @pl.when(pos + d < seg_len)
        def _():
            pl.semaphore_wait(ready_a.at[d - 1], 1)

    ld_copies = []
    for d in range(1, seg_len):
        ld_copies.append(
            remote(ld_mine, ld_recv.at[pl.ds(pos, 1)], al_s.at[d - 1], al_r.at[d - 1], seg_peer(d))
        )
    for copy in ld_copies:
        copy.start()
    ld_recv[pl.ds(pos, 1)] = ld_mine[...]

    @pl.when(me > 0)
    def _():
        for copy in halos:
            copy.wait_recv()

    @pl.when(me == 0)
    def _():
        xext[0:HALO, :] = jnp.zeros((HALO, feat), BF16)
        bcext[0:HALO, :] = jnp.zeros((HALO, 2 * STATE), BF16)

    states(0, 0)

    group_decay = jnp.exp2(widen3(dec[...]))
    run = fresh[0]
    entry[0] = jnp.zeros((STATE, feat), F32)
    entry[1] = run
    for g in range(1, groups):
        run = group_decay[g : g + 1, :] * run + fresh[g]
        if g + 1 < groups:
            entry[g + 1] = run
    s_send[...] = run.astype(BF16).reshape(seg_len, piece, feat)

    a_copies = []
    for d in range(1, seg_len):
        to = lax.rem(pos + d, seg_len)
        a_copies.append(
            remote(s_send.at[pl.ds(to, 1)], a_recv.at[pl.ds(pos, 1)], a_s.at[d - 1], a_r.at[d - 1], seg_peer(d))
        )
    for copy in reversed(a_copies):
        copy.start()
    a_recv[pl.ds(pos, 1)] = s_send[pl.ds(pos, 1)]

    skip_e = widen3(par[...])[2:3, :]

    def inside(g, carry):
        r0 = pl.multiple_of(g * GROUP, GROUP)
        scale[pl.ds(r0, GROUP), :] = widen2(jnp.exp2(ldb[pl.ds(r0, GROUP), :]))
        lane = lax.broadcasted_iota(jnp.int32, (ROWS, LANES), 1)
        for tb in range(GROUP // ROWS):
            cols = -(-(tb + 1) * ROWS // LANES) * LANES
            rt = pl.multiple_of(r0 + tb * ROWS, ROWS)
            inter = dot(
                bconv[pl.ds(rt, ROWS), STATE:], bconv[pl.ds(r0, cols), 0:STATE], ((1,), (1,))
            )
            t_i = tb * ROWS + lax.broadcasted_iota(jnp.int32, (ROWS, cols), 0)
            s_i = lax.broadcasted_iota(jnp.int32, (ROWS, cols), 1)
            keep = t_i >= s_i
            for j in range(tiles):
                c0 = j * LANES
                xs = xconv[pl.ds(r0, cols), c0 : c0 + LANES]
                halves = []
                for h in (2 * j, 2 * j + 1):
                    diff = ldb[pl.ds(rt, ROWS), h : h + 1] - ldt[g, h : h + 1, 0:cols]
                    kern = jnp.exp2(jnp.where(keep, diff, -jnp.inf))
                    mix = (inter * kern * stept[g, h : h + 1, 0:cols]).astype(BF16)
                    halves.append(dot(mix, xs))
                intra = jnp.where(lane < HEADDIM, halves[0], halves[1])
                x_t = xconv[pl.ds(rt, ROWS), c0 : c0 + LANES].astype(F32)
                gate = silu_of_half(0.5 * gbuf[pl.ds(rt, ROWS), c0 : c0 + LANES].astype(F32))
                base[pl.ds(rt, ROWS), c0 : c0 + LANES] = (intra + skip_e[:, c0 : c0 + LANES] * x_t) * gate
                scale[pl.ds(rt, ROWS), c0 : c0 + LANES] = scale[pl.ds(rt, ROWS), c0 : c0 + LANES] * gate
        return carry

    loads[2].wait()
    lax.fori_loop(0, jnp.where(me == 0, 0, groups), inside, 0)

    for copy in ld_copies:
        copy.wait()
    for copy in a_copies:
        copy.wait()
    lds = jnp.concatenate([ld_recv[q] for q in range(seg_len)], axis=0)
    dec_e = jnp.exp2(widen3(lds))
    run = jnp.zeros((piece, feat), F32)
    run_d = jnp.ones((1, feat), F32)
    before = []
    for q in range(seg_len):
        loc[q] = run
        before.append(run_d)
        run = dec_e[q : q + 1, :] * run + a_recv[q].astype(F32)
        run_d = run_d * dec_e[q : q + 1, :]

    seg_ld = ld_recv[0]
    for q in range(1, seg_len):
        seg_ld = seg_ld + ld_recv[q]
    after = {"seq": lax.rem(me + seg_len, n_seq)}
    onward = [
        remote(t_send, b_recv, b_s, b_r, after),
        remote(lx_mine, lx_recv, bl_s, bl_r, after),
    ]
    sends = (seg >= 1) & (seg + 1 < segs)

    @pl.when(seg >= 2)
    def _():
        for copy in onward:
            copy.wait_recv()

    t_send[...] = (run + run_d * b_recv[0])[None]
    lx_mine[...] = lx_recv[...] + seg_ld[None]

    @pl.when(seg + 1 < segs)
    def _():
        pl.semaphore_wait(ready_b, 1)

    @pl.when(sends)
    def _():
        for copy in onward:
            copy.start()

    first_up = remote(f_recv, f_recv, f_s, f_r, after)
    first_down = remote(f_recv, f_recv, f_s, f_r, {"seq": lax.rem(me + n_seq - seg_len, n_seq)})
    first_wrap = remote(f_recv, f_recv, fw_s, f_r, {"seq": lax.rem(me + (segs - 1) * seg_len, n_seq)})

    @pl.when(seg == 0)
    def _():
        f_recv[...] = run[None]

    @pl.when(seg >= 1)
    def _():
        first_up.wait_recv()

    @pl.when(seg < middle)
    def _():
        first_up.start()

    @pl.when(seg >= middle + 2)
    def _():
        first_down.start()

    carry = b_recv[0] + jnp.exp2(widen3(jnp.broadcast_to(lx_recv[0], (8, LANES))))[0:1, :] * f_recv[0]
    carry = jnp.where(seg == 0, jnp.zeros_like(carry), carry)
    for q in range(seg_len):
        c_send[q] = loc[q] + before[q] * carry

    c_copies = []
    for d in range(1, seg_len):
        to = lax.rem(pos + d, seg_len)
        copy = remote(c_send.at[pl.ds(to, 1)], inc.at[pl.ds(pos, 1)], c_s.at[d - 1], c_r.at[d - 1], seg_peer(d))
        c_copies.append((seg + to > 0, copy))
    for wanted, copy in c_copies:

        @pl.when(wanted)
        def _():
            copy.start()

    inc[pl.ds(pos, 1)] = c_send[pl.ds(pos, 1)]
    if wrap:

        @pl.when(seg == 0)
        def _():
            pl.semaphore_wait(ready_w, 1)
            first_wrap.start()

    lax.fori_loop(0, jnp.where(me == 0, groups, 0), inside, 0)

    @pl.when(me > 0)
    def _():
        for _, copy in c_copies:
            copy.wait_recv()

    run_d = jnp.ones((1, feat), F32)
    ss = jnp.zeros((8, LANES), F32)
    blocks = GROUP // 8
    lane8 = lax.broadcasted_iota(jnp.int32, (blocks, 8, LANES), 2)
    block_i = lax.broadcasted_iota(jnp.int32, (blocks, 8, LANES), 0)
    for g in range(groups):
        r0 = g * GROUP
        state = entry[g] + run_d * inc[...].reshape(STATE, feat)
        high, low = two_parts(state)
        c_rows = bconv[r0 : r0 + GROUP, STATE:]
        c_rows = jnp.concatenate([c_rows, c_rows], axis=1)
        both = jnp.concatenate([high, low], axis=0)
        squares = jnp.zeros((GROUP, LANES), F32)
        for j in range(tiles):
            c0 = j * LANES
            carried = dot(c_rows, both[:, c0 : c0 + LANES])
            gated = base[r0 : r0 + GROUP, c0 : c0 + LANES] + scale[r0 : r0 + GROUP, c0 : c0 + LANES] * carried
            base[r0 : r0 + GROUP, c0 : c0 + LANES] = gated
            squares = squares + gated * gated
        total = jnp.broadcast_to(jnp.sum(squares, axis=1, keepdims=True), (GROUP, LANES))
        total = total.reshape(blocks, 8, LANES)
        ss = ss + jnp.sum(jnp.where(lane8 == block_i + g * blocks, total, 0.0), axis=0)
        run_d = run_d * group_decay[g : g + 1, :]
    ss_mine[...] = ss[None]

    @pl.when(me == 0)
    def _():
        pl.semaphore_wait(barrier, n_head - 1)

    x_copies = []
    for d in range(1, n_head):
        x_copies.append(
            remote(ss_mine, ss_recv.at[pl.ds(mine_h, 1)], x_s.at[d - 1], x_r.at[d - 1], {"head": lax.rem(mine_h + d, n_head)})
        )
    for copy in x_copies:
        copy.start()
    ss_recv[pl.ds(mine_h, 1)] = ss_mine[...]
    for copy in x_copies:
        copy.wait()
    ss = ss_recv[0]
    for h in range(1, n_head):
        ss = ss + ss_recv[h]
    inv = lax.rsqrt(ss * (1.0 / di) + norm_eps)
    for g in range(groups):
        spread = jnp.where(lane8 == block_i + g * blocks, jnp.broadcast_to(inv[None], (blocks, 8, LANES)), 0.0)
        row_inv = jnp.sum(spread.reshape(GROUP, LANES), axis=1, keepdims=True)
        r0 = g * GROUP
        for j in range(tiles):
            c0 = j * LANES
            base[r0 : r0 + GROUP, c0 : c0 + LANES] = base[r0 : r0 + GROUP, c0 : c0 + LANES] * row_inv

    @pl.when(me + 1 < n_seq)
    def _():
        for copy in halos:
            copy.wait_send()

    @pl.when(sends)
    def _():
        for copy in onward:
            copy.wait_send()

    @pl.when(seg < middle)
    def _():
        first_up.wait_send()

    @pl.when(seg >= middle + 2)
    def _():
        first_down.wait_send()

    if wrap:

        @pl.when(seg == 0)
        def _():
            first_wrap.wait_send()

    for wanted, copy in c_copies:

        @pl.when(wanted)
        def _():
            copy.wait_send()


def on_device(n_seq, n_head, *args):
    (x_raw, bc_raw, gate_in, step_raw, cxw, cxb, cbw, cbb, dt_bias, a_log, d_skip, gain) = args
    length, feat = x_raw.shape[1], x_raw.shape[2]
    heads = dt_bias.shape[0]
    seg_len = SEG if n_seq % SEG == 0 else n_seq
    piece = STATE // seg_len
    groups = length // GROUP
    vmem = pl.BlockSpec(memory_space=pltpu.VMEM)
    hbm = pl.BlockSpec(memory_space=pltpu.HBM)
    dma = pltpu.SemaphoreType.DMA
    regular = pltpu.SemaphoreType.REGULAR
    scratch = [
        pltpu.VMEM((heads, 1, length), F32),
        pltpu.VMEM((CONV, feat), BF16),
        pltpu.VMEM((feat,), BF16),
        pltpu.VMEM((CONV, 2 * STATE), BF16),
        pltpu.VMEM((2 * STATE,), BF16),
        pltpu.VMEM((1, heads), F32),
        pltpu.VMEM((1, heads), F32),
        pltpu.VMEM((1, heads), F32),
        pltpu.VMEM((HALO + length, feat), BF16),
        pltpu.VMEM((HALO + length, 2 * STATE), BF16),
        pltpu.VMEM((length, feat), BF16),
        pltpu.VMEM((length, feat), BF16),
        pltpu.VMEM((length, 2 * STATE), BF16),
        pltpu.VMEM((16, length), F32),
        pltpu.VMEM((feat // LANES + 2, ROWS + HALO, LANES), F32),
        pltpu.VMEM((length, LANES), F32),
        pltpu.VMEM((length, LANES), F32),
        pltpu.VMEM((groups, 16, GROUP), F32),
        pltpu.VMEM((groups, 16, GROUP), F32),
        pltpu.VMEM((8, LANES), F32),
        pltpu.VMEM((8, feat + 2 * STATE), F32),
        pltpu.VMEM((2 * LANES, feat), BF16),
        pltpu.VMEM((GROUP, GROUP), BF16),
        pltpu.VMEM((GROUP, feat), F32),
        pltpu.VMEM((GROUP, feat), BF16),
        pltpu.VMEM((groups, STATE, feat), F32),
        pltpu.VMEM((groups, STATE, feat), F32),
        pltpu.VMEM((length, feat), F32),
        pltpu.VMEM((8, LANES), F32),
        pltpu.VMEM((seg_len, piece, feat), BF16),
        pltpu.VMEM((seg_len, piece, feat), BF16),
        pltpu.VMEM((1, 1, LANES), F32),
        pltpu.VMEM((seg_len, 1, LANES), F32),
        pltpu.VMEM((seg_len, piece, feat), F32),
        pltpu.VMEM((1, piece, feat), F32),
        pltpu.VMEM((1, piece, feat), F32),
        pltpu.VMEM((1, 1, LANES), F32),
        pltpu.VMEM((1, 1, LANES), F32),
        pltpu.VMEM((1, piece, feat), F32),
        pltpu.VMEM((seg_len, piece, feat), F32),
        pltpu.VMEM((seg_len, piece, feat), F32),
        pltpu.VMEM((1, 8, LANES), F32),
        pltpu.VMEM((n_head, 8, LANES), F32),
        regular, regular((seg_len,)), regular, regular,
        dma((11,)),
        dma((2,)), dma((2,)),
        dma((seg_len,)), dma((seg_len,)),
        dma((seg_len,)), dma((seg_len,)),
        dma, dma, dma, dma, dma, dma, dma,
        dma((seg_len,)), dma((seg_len,)),
        dma((n_head,)), dma((n_head,)),
    ]
    sizes = (n_seq, n_head, seg_len, length, feat, heads)
    keep = lambda v: pltpu.with_memory_space_constraint(v, pltpu.HBM)
    out = pl.pallas_call(
        functools.partial(kernel, sizes),
        out_shape=jax.ShapeDtypeStruct((length, feat), F32),
        in_specs=[hbm] * 11,
        out_specs=vmem,
        scratch_shapes=scratch,
        compiler_params=pltpu.CompilerParams(
            collective_id=0, has_side_effects=True, vmem_limit_bytes=VMEM_LIMIT
        ),
        name="ssd_layer",
    )(
        *map(keep, (
            x_raw[0], bc_raw[0], gate_in[0], jnp.transpose(step_raw, (2, 0, 1)), cxw, cxb, cbw, cbb,
            dt_bias[None], a_log[None], d_skip[None],
        ))
    )
    return (out * gain).astype(BF16)[None]


def solution(mesh):
    in_specs = (
        P(("member", "rep"), "seq", "head"),
        P(("member", "rep"), "seq", None),
        P(("member", "rep"), "seq", "head"),
        P(("member", "rep"), "seq", "head"),
        P("member", "head"),
        P(("member", "head")),
        P("member", None),
        P("member"),
        P(("member", "head")),
        P(("member", "head")),
        P(("member", "head")),
        P(("member", "head")),
    )
    out_specs = P(("member", "rep"), "seq", "head")
    return jax.shard_map(
        functools.partial(on_device, mesh.shape["seq"], mesh.shape["head"]),
        mesh=mesh, in_specs=in_specs, out_specs=out_specs, check_vma=False,
    )
```

```python
import functools

import jax
import jax.numpy as jnp
from jax import lax
from jax.experimental import pallas as pl
from jax.experimental.pallas import tpu as pltpu
from jax.sharding import PartitionSpec as P

HEADDIM = 64
STATE = 128
GROUP = 256
CONV = 4
LANES = 128
HALO = 16
ROWS = 64
SEG = 4
SUB = 4
VMEM_LIMIT = 30 * 1024 * 1024
LOG2E = 1.4426950408889634
norm_eps = 1e-05

F32 = jnp.float32
BF16 = jnp.bfloat16
MESH = pl.DeviceIdType.MESH


def silu_of_half(half):
    return half + half * jnp.tanh(half)


def two_parts(v):
    high = v.astype(BF16)
    return high, (v - high.astype(F32)).astype(BF16)


def three_parts(v):
    high = v.astype(BF16)
    rest = v - high.astype(F32)
    mid = rest.astype(BF16)
    return high, mid, (rest - mid.astype(F32)).astype(BF16)


def dot(a, b, dims=((1,), (0,))):
    return lax.dot_general(a, b, (dims, ((), ())), preferred_element_type=F32)


def kernel(sizes, *refs):
    n_seq, n_head, seg_len, length, feat, heads = sizes
    (
        x_hbm, bc_hbm, gate_hbm, step_hbm, cxw_hbm, cxb_hbm, cbw_hbm, cbb_hbm,
        dt_hbm, alog_hbm, skip_hbm, base,
        step_ref, cxw_ref, cxb_ref, cbw_ref, cbb_ref, dt_ref, alog_ref, skip_ref,
        xext, bcext, gbuf, xconv, bconv, raw_t, shifts, stepb, ldb, ldt, stept, par, cw, expand_m, tri_m,
        tail_e, weighted, fresh, entry, scale, dec,
        s_send, a_recv, ld_mine, ld_recv, loc, t_send, b_recv, c_send, inc,
        ss_mine, ss_recv, ready_h, ready_a, ready_b,
        loc_sem, halo_s, halo_r, a_s, a_r, al_s, al_r, b_s, b_r, c_s, c_r, x_s, x_r,
    ) = refs
    groups = length // GROUP
    tiles = feat // LANES
    piece = STATE // seg_len
    segs = n_seq // seg_len
    di = feat * n_head

    me = lax.axis_index("seq")
    mine_h = lax.axis_index("head")
    seg = me // seg_len
    pos = lax.rem(me, seg_len)

    loads = [
        pltpu.make_async_copy(x_hbm, xext.at[pl.ds(HALO, length)], loc_sem.at[0]),
        pltpu.make_async_copy(bc_hbm, bcext.at[pl.ds(HALO, length)], loc_sem.at[1]),
        pltpu.make_async_copy(gate_hbm, gbuf, loc_sem.at[2]),
        pltpu.make_async_copy(step_hbm, step_ref, loc_sem.at[3]),
        pltpu.make_async_copy(cxw_hbm, cxw_ref, loc_sem.at[4]),
        pltpu.make_async_copy(cxb_hbm, cxb_ref, loc_sem.at[5]),
        pltpu.make_async_copy(cbw_hbm, cbw_ref, loc_sem.at[6]),
        pltpu.make_async_copy(cbb_hbm, cbb_ref, loc_sem.at[7]),
        pltpu.make_async_copy(dt_hbm, dt_ref, loc_sem.at[8]),
        pltpu.make_async_copy(alog_hbm, alog_ref, loc_sem.at[9]),
        pltpu.make_async_copy(skip_hbm, skip_ref, loc_sem.at[10]),
    ]
    for load in loads[3:] + loads[:3]:
        load.start()

    b_recv[...] = jnp.zeros_like(b_recv)
    inc[...] = jnp.zeros_like(inc)
    barrier = pltpu.get_barrier_semaphore()

    def greet(where):
        pl.semaphore_signal(barrier, inc=1, device_id=where, device_id_type=MESH)

    @pl.when(me + 1 < n_seq)
    def _():
        greet({"seq": me + 1})

    for d in range(1, seg_len):

        @pl.when(pos + d < seg_len)
        def _():
            greet({"seq": me + d})

    @pl.when(seg + 1 < segs)
    def _():
        greet({"seq": me + seg_len})

    for d in range(1, n_head):
        greet({"head": lax.rem(mine_h + d, n_head)})

    row_i = lax.broadcasted_iota(jnp.int32, (GROUP, GROUP), 0)
    col_i = lax.broadcasted_iota(jnp.int32, (GROUP, GROUP), 1)
    tri_m[...] = jnp.where(row_i <= col_i, 1.0, 0.0).astype(BF16)
    head_i = lax.broadcasted_iota(jnp.int32, (2 * LANES, feat), 0)
    feat_i = lax.broadcasted_iota(jnp.int32, (2 * LANES, feat), 1)
    expand_m[...] = jnp.where((feat_i >> 6) == (head_i & (LANES - 1)), 1.0, 0.0).astype(BF16)
    for load in loads[3:]:
        load.wait()
    par[...] = jnp.zeros_like(par)
    par[0:1, 0:heads] = dt_ref[...]
    par[1:2, 0:heads] = alog_ref[...]
    par[2:3, 0:heads] = skip_ref[...]
    cw[0:CONV, 0:feat] = 0.5 * cxw_ref[...].astype(F32)
    cw[CONV : CONV + 1, 0:feat] = 0.5 * cxb_ref[...].astype(F32).reshape(1, feat)
    cw[0:CONV, feat:] = 0.5 * cbw_ref[...].astype(F32)
    cw[CONV : CONV + 1, feat:] = 0.5 * cbb_ref[...].astype(F32).reshape(1, 2 * STATE)

    def widen3(v):
        total = None
        for part in three_parts(v):
            term = dot(part, expand_m[0:LANES, :])
            total = term if total is None else total + term
        return total

    def widen2(v):
        high, low = two_parts(v)
        return dot(jnp.concatenate([high, low], axis=1), expand_m[...])

    raw_t[...] = jnp.zeros_like(raw_t)
    for h in range(heads):
        raw_t[h : h + 1, :] = step_ref[h]
    par_t = par[...].T
    raw = raw_t[...] + par_t[0:16, 0:1]
    step = jnp.maximum(raw, 0.0) + jnp.log1p(jnp.exp(-jnp.abs(raw)))
    raw_t[...] = step
    rates = jnp.concatenate(three_parts(-LOG2E * jnp.exp(par_t[0:16, 1:2]) * step), axis=0)
    rest = jnp.zeros((LANES - 16, GROUP), F32)
    dec[...] = jnp.zeros_like(dec)
    for g in range(groups):
        r0 = g * GROUP
        sums = dot(rates[:, r0 : r0 + GROUP], tri_m[...])
        sums = sums[0:16] + sums[16:32] + sums[32:48]
        ldt[g] = sums
        stept[g] = raw_t[:, r0 : r0 + GROUP]
        ldb[r0 : r0 + GROUP, :] = jnp.concatenate([sums, rest], axis=0).T
        stepb[r0 : r0 + GROUP, :] = jnp.concatenate([stept[g], rest], axis=0).T
        dec[g : g + 1, :] = ldb[r0 + GROUP - 1 : r0 + GROUP, :]
    ld_total = dec[0:1, :]
    for g in range(1, groups):
        ld_total = ld_total + dec[g : g + 1, :]
    ld_mine[...] = ld_total[None]

    def conv(ext, r, j, w_off):
        slot = j + w_off // LANES
        shifts[slot] = ext[pl.ds(r, ROWS + HALO), j * LANES : (j + 1) * LANES].astype(F32)
        lo = w_off + j * LANES
        acc = cw[CONV : CONV + 1, lo : lo + LANES]
        for k in range(CONV):
            start = HALO - (CONV - 1 - k)
            acc = acc + cw[k : k + 1, lo : lo + LANES] * shifts[slot, start : start + ROWS, :]
        return silu_of_half(acc)

    def states(g, carry):
        r0 = pl.multiple_of(g * GROUP, GROUP)
        ld = ldb[pl.ds(r0, GROUP), :]
        tail = jnp.exp2(ld[GROUP - 1 : GROUP, :] - ld) * stepb[pl.ds(r0, GROUP), :]
        tail_e[...] = widen2(tail)

        def chunk(i, inner):
            q0 = i * ROWS
            r = pl.multiple_of(r0 + q0, ROWS)
            for j in range(2 * STATE // LANES):
                bconv[pl.ds(r, ROWS), j * LANES : (j + 1) * LANES] = conv(bcext, r, j, feat).astype(BF16)
            for j in range(tiles):
                c0 = j * LANES
                value = conv(xext, r, j, 0).astype(BF16)
                xconv[pl.ds(r, ROWS), c0 : c0 + LANES] = value
                weighted[pl.ds(q0, ROWS), c0 : c0 + LANES] = (
                    tail_e[pl.ds(q0, ROWS), c0 : c0 + LANES] * value.astype(F32)
                ).astype(BF16)
            return inner

        for i in range(GROUP // ROWS):
            chunk(i, 0)
        fresh[pl.ds(g, 1)] = dot(
            bconv[pl.ds(r0, GROUP), 0:STATE], weighted[...], ((0,), (0,))
        )[None]
        return carry

    for load in loads[:2]:
        load.wait()
    lax.fori_loop(1, groups, states, 0)

    @pl.when(me > 0)
    def _():
        pl.semaphore_wait(barrier, 1 + pos + jnp.where(seg > 0, 1, 0) + n_head - 1)
        pl.semaphore_signal(ready_h, inc=1, device_id={"seq": me - 1}, device_id_type=MESH)

    for d in range(1, seg_len):

        @pl.when(pos >= d)
        def _():
            pl.semaphore_signal(ready_a.at[d - 1], inc=1, device_id={"seq": me - d}, device_id_type=MESH)

    @pl.when(seg > 0)
    def _():
        pl.semaphore_signal(ready_b, inc=1, device_id={"seq": me - seg_len}, device_id_type=MESH)

    def remote(src, dst, send, recv, where):
        return pltpu.make_async_remote_copy(
            src_ref=src, dst_ref=dst, send_sem=send, recv_sem=recv,
            device_id=where, device_id_type=MESH,
        )

    halos = [
        remote(xext.at[pl.ds(length, HALO)], xext.at[pl.ds(0, HALO)], halo_s.at[0], halo_r.at[0], {"seq": lax.rem(me + 1, n_seq)}),
        remote(bcext.at[pl.ds(length, HALO)], bcext.at[pl.ds(0, HALO)], halo_s.at[1], halo_r.at[1], {"seq": lax.rem(me + 1, n_seq)}),
    ]

    @pl.when(me + 1 < n_seq)
    def _():
        pl.semaphore_wait(ready_h, 1)
        for copy in halos:
            copy.start()

    def seg_peer(d):
        return {"seq": seg * seg_len + lax.rem(pos + d, seg_len)}

    for d in range(1, seg_len):

        @pl.when(pos + d < seg_len)
        def _():
            pl.semaphore_wait(ready_a.at[d - 1], 1)

    ld_copies = []
    for d in range(1, seg_len):
        ld_copies.append(
            remote(ld_mine, ld_recv.at[pl.ds(pos, 1)], al_s.at[d - 1], al_r.at[d - 1], seg_peer(d))
        )
    for copy in ld_copies:
        copy.start()
    ld_recv[pl.ds(pos, 1)] = ld_mine[...]

    @pl.when(me > 0)
    def _():
        for copy in halos:
            copy.wait_recv()

    @pl.when(me == 0)
    def _():
        xext[0:HALO, :] = jnp.zeros((HALO, feat), BF16)
        bcext[0:HALO, :] = jnp.zeros((HALO, 2 * STATE), BF16)

    states(0, 0)

    group_decay = jnp.exp2(widen3(dec[...]))
    run = fresh[0]
    entry[0] = jnp.zeros((STATE, feat), F32)
    entry[1] = run
    for g in range(1, groups):
        run = group_decay[g : g + 1, :] * run + fresh[g]
        if g + 1 < groups:
            entry[g + 1] = run
    s_send[...] = run.astype(BF16).reshape(seg_len, piece, feat)

    a_copies = []
    for d in range(1, seg_len):
        to = lax.rem(pos + d, seg_len)
        a_copies.append(
            remote(s_send.at[pl.ds(to, 1)], a_recv.at[pl.ds(pos, 1)], a_s.at[d - 1], a_r.at[d - 1], seg_peer(d))
        )
    for copy in reversed(a_copies):
        copy.start()
    a_recv[pl.ds(pos, 1)] = s_send[pl.ds(pos, 1)]

    skip_e = widen3(par[...])[2:3, :]

    def inside(g, carry):
        r0 = pl.multiple_of(g * GROUP, GROUP)
        scale[pl.ds(r0, GROUP), :] = widen2(jnp.exp2(ldb[pl.ds(r0, GROUP), :]))
        lane = lax.broadcasted_iota(jnp.int32, (ROWS, LANES), 1)
        for tb in range(GROUP // ROWS):
            cols = -(-(tb + 1) * ROWS // LANES) * LANES
            rt = pl.multiple_of(r0 + tb * ROWS, ROWS)
            inter = dot(
                bconv[pl.ds(rt, ROWS), STATE:], bconv[pl.ds(r0, cols), 0:STATE], ((1,), (1,))
            )
            t_i = tb * ROWS + lax.broadcasted_iota(jnp.int32, (ROWS, cols), 0)
            s_i = lax.broadcasted_iota(jnp.int32, (ROWS, cols), 1)
            keep = t_i >= s_i
            for j in range(tiles):
                c0 = j * LANES
                xs = xconv[pl.ds(r0, cols), c0 : c0 + LANES]
                halves = []
                for h in (2 * j, 2 * j + 1):
                    diff = ldb[pl.ds(rt, ROWS), h : h + 1] - ldt[g, h : h + 1, 0:cols]
                    kern = jnp.exp2(jnp.where(keep, diff, -jnp.inf))
                    mix = (inter * kern * stept[g, h : h + 1, 0:cols]).astype(BF16)
                    halves.append(dot(mix, xs))
                intra = jnp.where(lane < HEADDIM, halves[0], halves[1])
                x_t = xconv[pl.ds(rt, ROWS), c0 : c0 + LANES].astype(F32)
                gate = silu_of_half(0.5 * gbuf[pl.ds(rt, ROWS), c0 : c0 + LANES].astype(F32))
                base[pl.ds(rt, ROWS), c0 : c0 + LANES] = (intra + skip_e[:, c0 : c0 + LANES] * x_t) * gate
                scale[pl.ds(rt, ROWS), c0 : c0 + LANES] = scale[pl.ds(rt, ROWS), c0 : c0 + LANES] * gate
        return carry

    loads[2].wait()
    lax.fori_loop(0, jnp.where(me == 0, 0, groups), inside, 0)

    for copy in ld_copies:
        copy.wait()
    for copy in a_copies:
        copy.wait()
    lds = jnp.concatenate([ld_recv[q] for q in range(seg_len)], axis=0)
    dec_e = jnp.exp2(widen3(lds))
    run = jnp.zeros((piece, feat), F32)
    run_d = jnp.ones((1, feat), F32)
    before = []
    for q in range(seg_len):
        loc[q] = run
        before.append(run_d)
        run = dec_e[q : q + 1, :] * run + a_recv[q].astype(F32)
        run_d = run_d * dec_e[q : q + 1, :]

    after = {"seq": lax.rem(me + seg_len, n_seq)}
    rows = piece // SUB
    onward = [
        remote(t_send.at[pl.ds(u, 1)], b_recv.at[pl.ds(u, 1)], b_s.at[u], b_r.at[u], after)
        for u in range(SUB)
    ]

    @pl.when(seg + 1 < segs)
    def _():
        pl.semaphore_wait(ready_b, 1)

    for u in range(SUB):

        @pl.when(seg > 0)
        def _():
            onward[u].wait_recv()

        t_send[u] = run[u * rows : (u + 1) * rows] + run_d * b_recv[u]

        @pl.when(seg + 1 < segs)
        def _():
            onward[u].start()

    carry = b_recv[...].reshape(piece, feat)
    for q in range(seg_len):
        c_send[q] = loc[q] + before[q] * carry

    c_copies = []
    for d in range(1, seg_len):
        to = lax.rem(pos + d, seg_len)
        copy = remote(c_send.at[pl.ds(to, 1)], inc.at[pl.ds(pos, 1)], c_s.at[d - 1], c_r.at[d - 1], seg_peer(d))
        c_copies.append((seg + to > 0, copy))
    for wanted, copy in c_copies:

        @pl.when(wanted)
        def _():
            copy.start()

    inc[pl.ds(pos, 1)] = c_send[pl.ds(pos, 1)]
    lax.fori_loop(0, jnp.where(me == 0, groups, 0), inside, 0)

    @pl.when(me > 0)
    def _():
        for _, copy in c_copies:
            copy.wait_recv()

    run_d = jnp.ones((1, feat), F32)
    ss = jnp.zeros((8, LANES), F32)
    blocks = GROUP // 8
    lane8 = lax.broadcasted_iota(jnp.int32, (blocks, 8, LANES), 2)
    block_i = lax.broadcasted_iota(jnp.int32, (blocks, 8, LANES), 0)
    for g in range(groups):
        r0 = g * GROUP
        state = entry[g] + run_d * inc[...].reshape(STATE, feat)
        high, low = two_parts(state)
        c_rows = bconv[r0 : r0 + GROUP, STATE:]
        c_rows = jnp.concatenate([c_rows, c_rows], axis=1)
        both = jnp.concatenate([high, low], axis=0)
        squares = jnp.zeros((GROUP, LANES), F32)
        for j in range(tiles):
            c0 = j * LANES
            carried = dot(c_rows, both[:, c0 : c0 + LANES])
            gated = base[r0 : r0 + GROUP, c0 : c0 + LANES] + scale[r0 : r0 + GROUP, c0 : c0 + LANES] * carried
            base[r0 : r0 + GROUP, c0 : c0 + LANES] = gated
            squares = squares + gated * gated
        total = jnp.broadcast_to(jnp.sum(squares, axis=1, keepdims=True), (GROUP, LANES))
        total = total.reshape(blocks, 8, LANES)
        ss = ss + jnp.sum(jnp.where(lane8 == block_i + g * blocks, total, 0.0), axis=0)
        run_d = run_d * group_decay[g : g + 1, :]
    ss_mine[...] = ss[None]

    @pl.when(me == 0)
    def _():
        pl.semaphore_wait(barrier, n_head - 1)

    x_copies = []
    for d in range(1, n_head):
        x_copies.append(
            remote(ss_mine, ss_recv.at[pl.ds(mine_h, 1)], x_s.at[d - 1], x_r.at[d - 1], {"head": lax.rem(mine_h + d, n_head)})
        )
    for copy in x_copies:
        copy.start()
    ss_recv[pl.ds(mine_h, 1)] = ss_mine[...]
    for copy in x_copies:
        copy.wait()
    ss = ss_recv[0]
    for h in range(1, n_head):
        ss = ss + ss_recv[h]
    inv = lax.rsqrt(ss * (1.0 / di) + norm_eps)
    for g in range(groups):
        spread = jnp.where(lane8 == block_i + g * blocks, jnp.broadcast_to(inv[None], (blocks, 8, LANES)), 0.0)
        row_inv = jnp.sum(spread.reshape(GROUP, LANES), axis=1, keepdims=True)
        r0 = g * GROUP
        for j in range(tiles):
            c0 = j * LANES
            base[r0 : r0 + GROUP, c0 : c0 + LANES] = base[r0 : r0 + GROUP, c0 : c0 + LANES] * row_inv

    @pl.when(me + 1 < n_seq)
    def _():
        for copy in halos:
            copy.wait_send()

    @pl.when(seg + 1 < segs)
    def _():
        for copy in onward:
            copy.wait_send()

    for wanted, copy in c_copies:

        @pl.when(wanted)
        def _():
            copy.wait_send()


def on_device(n_seq, n_head, *args):
    (x_raw, bc_raw, gate_in, step_raw, cxw, cxb, cbw, cbb, dt_bias, a_log, d_skip, gain) = args
    length, feat = x_raw.shape[1], x_raw.shape[2]
    heads = dt_bias.shape[0]
    seg_len = SEG if n_seq % SEG == 0 else n_seq
    piece = STATE // seg_len
    groups = length // GROUP
    vmem = pl.BlockSpec(memory_space=pltpu.VMEM)
    hbm = pl.BlockSpec(memory_space=pltpu.HBM)
    dma = pltpu.SemaphoreType.DMA
    regular = pltpu.SemaphoreType.REGULAR
    scratch = [
        pltpu.VMEM((heads, 1, length), F32),
        pltpu.VMEM((CONV, feat), BF16),
        pltpu.VMEM((feat,), BF16),
        pltpu.VMEM((CONV, 2 * STATE), BF16),
        pltpu.VMEM((2 * STATE,), BF16),
        pltpu.VMEM((1, heads), F32),
        pltpu.VMEM((1, heads), F32),
        pltpu.VMEM((1, heads), F32),
        pltpu.VMEM((HALO + length, feat), BF16),
        pltpu.VMEM((HALO + length, 2 * STATE), BF16),
        pltpu.VMEM((length, feat), BF16),
        pltpu.VMEM((length, feat), BF16),
        pltpu.VMEM((length, 2 * STATE), BF16),
        pltpu.VMEM((16, length), F32),
        pltpu.VMEM((feat // LANES + 2, ROWS + HALO, LANES), F32),
        pltpu.VMEM((length, LANES), F32),
        pltpu.VMEM((length, LANES), F32),
        pltpu.VMEM((groups, 16, GROUP), F32),
        pltpu.VMEM((groups, 16, GROUP), F32),
        pltpu.VMEM((8, LANES), F32),
        pltpu.VMEM((8, feat + 2 * STATE), F32),
        pltpu.VMEM((2 * LANES, feat), BF16),
        pltpu.VMEM((GROUP, GROUP), BF16),
        pltpu.VMEM((GROUP, feat), F32),
        pltpu.VMEM((GROUP, feat), BF16),
        pltpu.VMEM((groups, STATE, feat), F32),
        pltpu.VMEM((groups, STATE, feat), F32),
        pltpu.VMEM((length, feat), F32),
        pltpu.VMEM((8, LANES), F32),
        pltpu.VMEM((seg_len, piece, feat), BF16),
        pltpu.VMEM((seg_len, piece, feat), BF16),
        pltpu.VMEM((1, 1, LANES), F32),
        pltpu.VMEM((seg_len, 1, LANES), F32),
        pltpu.VMEM((seg_len, piece, feat), F32),
        pltpu.VMEM((SUB, piece // SUB, feat), F32),
        pltpu.VMEM((SUB, piece // SUB, feat), F32),
        pltpu.VMEM((seg_len, piece, feat), F32),
        pltpu.VMEM((seg_len, piece, feat), F32),
        pltpu.VMEM((1, 8, LANES), F32),
        pltpu.VMEM((n_head, 8, LANES), F32),
        regular, regular((seg_len,)), regular,
        dma((11,)),
        dma((2,)), dma((2,)),
        dma((seg_len,)), dma((seg_len,)),
        dma((seg_len,)), dma((seg_len,)),
        dma((SUB,)), dma((SUB,)),
        dma((seg_len,)), dma((seg_len,)),
        dma((n_head,)), dma((n_head,)),
    ]
    sizes = (n_seq, n_head, seg_len, length, feat, heads)
    keep = lambda v: pltpu.with_memory_space_constraint(v, pltpu.HBM)
    out = pl.pallas_call(
        functools.partial(kernel, sizes),
        out_shape=jax.ShapeDtypeStruct((length, feat), F32),
        in_specs=[hbm] * 11,
        out_specs=vmem,
        scratch_shapes=scratch,
        compiler_params=pltpu.CompilerParams(
            collective_id=0, has_side_effects=True, vmem_limit_bytes=VMEM_LIMIT
        ),
        name="ssd_layer",
    )(
        *map(keep, (
            x_raw[0], bc_raw[0], gate_in[0], jnp.transpose(step_raw, (2, 0, 1)), cxw, cxb, cbw, cbb,
            dt_bias[None], a_log[None], d_skip[None],
        ))
    )
    return (out * gain).astype(BF16)[None]


def solution(mesh):
    in_specs = (
        P(("member", "rep"), "seq", "head"),
        P(("member", "rep"), "seq", None),
        P(("member", "rep"), "seq", "head"),
        P(("member", "rep"), "seq", "head"),
        P("member", "head"),
        P(("member", "head")),
        P("member", None),
        P("member"),
        P(("member", "head")),
        P(("member", "head")),
        P(("member", "head")),
        P(("member", "head")),
    )
    out_specs = P(("member", "rep"), "seq", "head")
    return jax.shard_map(
        functools.partial(on_device, mesh.shape["seq"], mesh.shape["head"]),
        mesh=mesh, in_specs=in_specs, out_specs=out_specs, check_vma=False,
    )
```

```python
import functools

import jax
import jax.numpy as jnp
from jax import lax
from jax.experimental import pallas as pl
from jax.experimental.pallas import tpu as pltpu
from jax.sharding import PartitionSpec as P

HEADDIM = 64
STATE = 128
GROUP = 256
CONV = 4
LANES = 128
HALO = 16
ROWS = 64
SEG = 4
SUB = 4
VMEM_LIMIT = 30 * 1024 * 1024
LOG2E = 1.4426950408889634
norm_eps = 1e-05

F32 = jnp.float32
BF16 = jnp.bfloat16
MESH = pl.DeviceIdType.MESH


def silu_of_half(half):
    return half + half * jnp.tanh(half)


def two_parts(v):
    high = v.astype(BF16)
    return high, (v - high.astype(F32)).astype(BF16)


def three_parts(v):
    high = v.astype(BF16)
    rest = v - high.astype(F32)
    mid = rest.astype(BF16)
    return high, mid, (rest - mid.astype(F32)).astype(BF16)


def dot(a, b, dims=((1,), (0,))):
    return lax.dot_general(a, b, (dims, ((), ())), preferred_element_type=F32)


def kernel(sizes, *refs):
    n_seq, n_head, seg_len, length, feat, heads = sizes
    (
        x_hbm, bc_hbm, gate_hbm, step_hbm, cxw_hbm, cxb_hbm, cbw_hbm, cbb_hbm,
        dt_hbm, alog_hbm, skip_hbm, base,
        step_ref, cxw_ref, cxb_ref, cbw_ref, cbb_ref, dt_ref, alog_ref, skip_ref,
        xext, bcext, gbuf, xconv, bconv, raw_t, shifts, stepb, ldb, ldt, stept, par, cw, expand_m, tri_m,
        tail_e, weighted, fresh, entry, scale, dec, gdec,
        s_send, a_recv, ld_mine, ld_recv, loc, t_send, b_recv, c_send, inc,
        ss_mine, ss_recv, ready_h, ready_a, ready_b,
        loc_sem, halo_s, halo_r, a_s, a_r, al_s, al_r, b_s, b_r, c_s, c_r, x_s, x_r,
    ) = refs
    groups = length // GROUP
    tiles = feat // LANES
    piece = STATE // seg_len
    segs = n_seq // seg_len
    di = feat * n_head

    me = lax.axis_index("seq")
    mine_h = lax.axis_index("head")
    seg = me // seg_len
    pos = lax.rem(me, seg_len)

    loads = [
        pltpu.make_async_copy(x_hbm, xext.at[pl.ds(HALO, length)], loc_sem.at[0]),
        pltpu.make_async_copy(bc_hbm, bcext.at[pl.ds(HALO, length)], loc_sem.at[1]),
        pltpu.make_async_copy(gate_hbm, gbuf, loc_sem.at[2]),
        pltpu.make_async_copy(step_hbm, step_ref, loc_sem.at[3]),
        pltpu.make_async_copy(cxw_hbm, cxw_ref, loc_sem.at[4]),
        pltpu.make_async_copy(cxb_hbm, cxb_ref, loc_sem.at[5]),
        pltpu.make_async_copy(cbw_hbm, cbw_ref, loc_sem.at[6]),
        pltpu.make_async_copy(cbb_hbm, cbb_ref, loc_sem.at[7]),
        pltpu.make_async_copy(dt_hbm, dt_ref, loc_sem.at[8]),
        pltpu.make_async_copy(alog_hbm, alog_ref, loc_sem.at[9]),
        pltpu.make_async_copy(skip_hbm, skip_ref, loc_sem.at[10]),
    ]
    for load in loads[3:] + loads[:3]:
        load.start()

    b_recv[...] = jnp.zeros_like(b_recv)
    inc[...] = jnp.zeros_like(inc)
    barrier = pltpu.get_barrier_semaphore()

    def greet(where):
        pl.semaphore_signal(barrier, inc=1, device_id=where, device_id_type=MESH)

    @pl.when(me + 1 < n_seq)
    def _():
        greet({"seq": me + 1})

    for d in range(1, seg_len):

        @pl.when(pos + d < seg_len)
        def _():
            greet({"seq": me + d})

    @pl.when(seg + 1 < segs)
    def _():
        greet({"seq": me + seg_len})

    for d in range(1, n_head):
        greet({"head": lax.rem(mine_h + d, n_head)})

    row_i = lax.broadcasted_iota(jnp.int32, (GROUP, GROUP), 0)
    col_i = lax.broadcasted_iota(jnp.int32, (GROUP, GROUP), 1)
    tri_m[...] = jnp.where(row_i <= col_i, 1.0, 0.0).astype(BF16)
    head_i = lax.broadcasted_iota(jnp.int32, (2 * LANES, feat), 0)
    feat_i = lax.broadcasted_iota(jnp.int32, (2 * LANES, feat), 1)
    expand_m[...] = jnp.where((feat_i >> 6) == (head_i & (LANES - 1)), 1.0, 0.0).astype(BF16)
    for load in loads[3:]:
        load.wait()
    par[...] = jnp.zeros_like(par)
    par[0:1, 0:heads] = dt_ref[...]
    par[1:2, 0:heads] = alog_ref[...]
    par[2:3, 0:heads] = skip_ref[...]
    cw[0:CONV, 0:feat] = 0.5 * cxw_ref[...].astype(F32)
    cw[CONV : CONV + 1, 0:feat] = 0.5 * cxb_ref[...].astype(F32).reshape(1, feat)
    cw[0:CONV, feat:] = 0.5 * cbw_ref[...].astype(F32)
    cw[CONV : CONV + 1, feat:] = 0.5 * cbb_ref[...].astype(F32).reshape(1, 2 * STATE)

    def widen3(v):
        total = None
        for part in three_parts(v):
            term = dot(part, expand_m[0:LANES, :])
            total = term if total is None else total + term
        return total

    def widen2(v):
        high, low = two_parts(v)
        return dot(jnp.concatenate([high, low], axis=1), expand_m[...])

    raw_t[...] = jnp.zeros_like(raw_t)
    for h in range(heads):
        raw_t[h : h + 1, :] = step_ref[h]
    par_t = par[...].T
    raw = raw_t[...] + par_t[0:16, 0:1]
    step = jnp.maximum(raw, 0.0) + jnp.log1p(jnp.exp(-jnp.abs(raw)))
    raw_t[...] = step
    rates = jnp.concatenate(three_parts(-LOG2E * jnp.exp(par_t[0:16, 1:2]) * step), axis=0)
    rest = jnp.zeros((LANES - 16, GROUP), F32)
    dec[...] = jnp.zeros_like(dec)
    for g in range(groups):
        r0 = g * GROUP
        sums = dot(rates[:, r0 : r0 + GROUP], tri_m[...])
        sums = sums[0:16] + sums[16:32] + sums[32:48]
        ldt[g] = sums
        stept[g] = raw_t[:, r0 : r0 + GROUP]
        ldb[r0 : r0 + GROUP, :] = jnp.concatenate([sums, rest], axis=0).T
        stepb[r0 : r0 + GROUP, :] = jnp.concatenate([stept[g], rest], axis=0).T
        dec[g : g + 1, :] = ldb[r0 + GROUP - 1 : r0 + GROUP, :]
    ld_total = dec[0:1, :]
    for g in range(1, groups):
        ld_total = ld_total + dec[g : g + 1, :]
    ld_mine[...] = ld_total[None]

    def conv(ext, r, j, w_off):
        slot = j + w_off // LANES
        shifts[slot] = ext[pl.ds(r, ROWS + HALO), j * LANES : (j + 1) * LANES].astype(F32)
        lo = w_off + j * LANES
        acc = cw[CONV : CONV + 1, lo : lo + LANES]
        for k in range(CONV):
            start = HALO - (CONV - 1 - k)
            acc = acc + cw[k : k + 1, lo : lo + LANES] * shifts[slot, start : start + ROWS, :]
        return silu_of_half(acc)

    def states(g, carry):
        r0 = pl.multiple_of(g * GROUP, GROUP)
        ld = ldb[pl.ds(r0, GROUP), :]
        tail = jnp.exp2(ld[GROUP - 1 : GROUP, :] - ld) * stepb[pl.ds(r0, GROUP), :]
        tail_e[...] = widen2(tail)

        def chunk(i, inner):
            q0 = i * ROWS
            r = pl.multiple_of(r0 + q0, ROWS)
            for j in range(2 * STATE // LANES):
                bconv[pl.ds(r, ROWS), j * LANES : (j + 1) * LANES] = conv(bcext, r, j, feat).astype(BF16)
            for j in range(tiles):
                c0 = j * LANES
                value = conv(xext, r, j, 0).astype(BF16)
                xconv[pl.ds(r, ROWS), c0 : c0 + LANES] = value
                weighted[pl.ds(q0, ROWS), c0 : c0 + LANES] = (
                    tail_e[pl.ds(q0, ROWS), c0 : c0 + LANES] * value.astype(F32)
                ).astype(BF16)
            return inner

        for i in range(GROUP // ROWS):
            chunk(i, 0)
        fresh[pl.ds(g, 1)] = dot(
            bconv[pl.ds(r0, GROUP), 0:STATE], weighted[...], ((0,), (0,))
        )[None]
        return carry

    for load in loads[:2]:
        load.wait()
    @pl.when(me > 0)
    def _():
        pl.semaphore_wait(barrier, 1 + pos + jnp.where(seg > 0, 1, 0) + n_head - 1)
        pl.semaphore_signal(ready_h, inc=1, device_id={"seq": me - 1}, device_id_type=MESH)

    for d in range(1, seg_len):

        @pl.when(pos >= d)
        def _():
            pl.semaphore_signal(ready_a.at[d - 1], inc=1, device_id={"seq": me - d}, device_id_type=MESH)

    @pl.when(seg > 0)
    def _():
        pl.semaphore_signal(ready_b, inc=1, device_id={"seq": me - seg_len}, device_id_type=MESH)

    def remote(src, dst, send, recv, where):
        return pltpu.make_async_remote_copy(
            src_ref=src, dst_ref=dst, send_sem=send, recv_sem=recv,
            device_id=where, device_id_type=MESH,
        )

    halos = [
        remote(xext.at[pl.ds(length, HALO)], xext.at[pl.ds(0, HALO)], halo_s.at[0], halo_r.at[0], {"seq": lax.rem(me + 1, n_seq)}),
        remote(bcext.at[pl.ds(length, HALO)], bcext.at[pl.ds(0, HALO)], halo_s.at[1], halo_r.at[1], {"seq": lax.rem(me + 1, n_seq)}),
    ]

    def states_and_halo(g, carry):
        @pl.when((g == min(2, groups - 1)) & (me + 1 < n_seq))
        def _():
            pl.semaphore_wait(ready_h, 1)
            for copy in halos:
                copy.start()

        return states(g, carry)

    lax.fori_loop(1, groups, states_and_halo, 0)

    def far_first(copies, wanted):
        for m in range(seg_len - 1, 0, -1):
            for inside_seg, to, d in ((pos + m < seg_len, pos + m, m), (pos >= m, pos - m, seg_len - m)):

                @pl.when(inside_seg & wanted(to))
                def _():
                    copies[d - 1].start()

    def seg_peer(d):
        return {"seq": seg * seg_len + lax.rem(pos + d, seg_len)}

    for d in range(1, seg_len):

        @pl.when(pos + d < seg_len)
        def _():
            pl.semaphore_wait(ready_a.at[d - 1], 1)

    ld_copies = []
    for d in range(1, seg_len):
        ld_copies.append(
            remote(ld_mine, ld_recv.at[pl.ds(pos, 1)], al_s.at[d - 1], al_r.at[d - 1], seg_peer(d))
        )
    for copy in ld_copies:
        copy.start()
    ld_recv[pl.ds(pos, 1)] = ld_mine[...]

    @pl.when(me > 0)
    def _():
        for copy in halos:
            copy.wait_recv()

    @pl.when(me == 0)
    def _():
        xext[0:HALO, :] = jnp.zeros((HALO, feat), BF16)
        bcext[0:HALO, :] = jnp.zeros((HALO, 2 * STATE), BF16)

    states(0, 0)

    group_decay = jnp.exp2(widen3(dec[...]))
    run = fresh[0]
    entry[0] = jnp.zeros((STATE, feat), F32)
    entry[1] = run
    for g in range(1, groups):
        run = group_decay[g : g + 1, :] * run + fresh[g]
        if g + 1 < groups:
            entry[g + 1] = run
    s_send[...] = run.astype(BF16).reshape(seg_len, piece, feat)

    a_copies = []
    for d in range(1, seg_len):
        to = lax.rem(pos + d, seg_len)
        a_copies.append(
            remote(s_send.at[pl.ds(to, 1)], a_recv.at[pl.ds(pos, 1)], a_s.at[d - 1], a_r.at[d - 1], seg_peer(d))
        )
    far_first(a_copies, lambda to: True)
    a_recv[pl.ds(pos, 1)] = s_send[pl.ds(pos, 1)]

    skip_e = widen3(par[...])[2:3, :]

    def inside(g, carry):
        r0 = pl.multiple_of(g * GROUP, GROUP)
        scale[pl.ds(r0, GROUP), :] = widen2(jnp.exp2(ldb[pl.ds(r0, GROUP), :]))
        lane = lax.broadcasted_iota(jnp.int32, (ROWS, LANES), 1)
        for tb in range(GROUP // ROWS):
            cols = -(-(tb + 1) * ROWS // LANES) * LANES
            rt = pl.multiple_of(r0 + tb * ROWS, ROWS)
            inter = dot(
                bconv[pl.ds(rt, ROWS), STATE:], bconv[pl.ds(r0, cols), 0:STATE], ((1,), (1,))
            )
            t_i = tb * ROWS + lax.broadcasted_iota(jnp.int32, (ROWS, cols), 0)
            s_i = lax.broadcasted_iota(jnp.int32, (ROWS, cols), 1)
            keep = t_i >= s_i
            for j in range(tiles):
                c0 = j * LANES
                xs = xconv[pl.ds(r0, cols), c0 : c0 + LANES]
                halves = []
                for h in (2 * j, 2 * j + 1):
                    diff = ldb[pl.ds(rt, ROWS), h : h + 1] - ldt[g, h : h + 1, 0:cols]
                    kern = jnp.exp2(jnp.where(keep, diff, -jnp.inf))
                    mix = (inter * kern * stept[g, h : h + 1, 0:cols]).astype(BF16)
                    halves.append(dot(mix, xs))
                intra = jnp.where(lane < HEADDIM, halves[0], halves[1])
                x_t = xconv[pl.ds(rt, ROWS), c0 : c0 + LANES].astype(F32)
                gate = silu_of_half(0.5 * gbuf[pl.ds(rt, ROWS), c0 : c0 + LANES].astype(F32))
                base[pl.ds(rt, ROWS), c0 : c0 + LANES] = (intra + skip_e[:, c0 : c0 + LANES] * x_t) * gate
                scale[pl.ds(rt, ROWS), c0 : c0 + LANES] = scale[pl.ds(rt, ROWS), c0 : c0 + LANES] * gate
        return carry

    loads[2].wait()
    lax.fori_loop(0, groups, inside, 0)

    blocks = GROUP // 8
    lane8 = lax.broadcasted_iota(jnp.int32, (blocks, 8, LANES), 2)
    block_i = lax.broadcasted_iota(jnp.int32, (blocks, 8, LANES), 0)
    gdec[0:groups, :] = group_decay[0:groups, :]

    def finish(g, so_far):
        run_d, ss = so_far
        r0 = pl.multiple_of(g * GROUP, GROUP)
        state = entry[g] + run_d * inc[...].reshape(STATE, feat)
        high, low = two_parts(state)
        c_rows = bconv[pl.ds(r0, GROUP), STATE:]
        c_rows = jnp.concatenate([c_rows, c_rows], axis=1)
        both = jnp.concatenate([high, low], axis=0)
        squares = jnp.zeros((GROUP, LANES), F32)
        for j in range(tiles):
            c0 = j * LANES
            carried = dot(c_rows, both[:, c0 : c0 + LANES])
            gated = base[pl.ds(r0, GROUP), c0 : c0 + LANES] + scale[pl.ds(r0, GROUP), c0 : c0 + LANES] * carried
            base[pl.ds(r0, GROUP), c0 : c0 + LANES] = gated
            squares = squares + gated * gated
        total = jnp.broadcast_to(jnp.sum(squares, axis=1, keepdims=True), (GROUP, LANES))
        total = total.reshape(blocks, 8, LANES)
        ss = ss + jnp.sum(jnp.where(lane8 == block_i + g * blocks, total, 0.0), axis=0)
        return run_d * gdec[pl.ds(g, 1), :], ss

    nothing = (jnp.ones((1, feat), F32), jnp.zeros((8, LANES), F32))
    _, ss_early = lax.fori_loop(0, jnp.where(me == 0, groups, 0), finish, nothing)

    for copy in ld_copies:
        copy.wait()
    for copy in a_copies:
        copy.wait()
    lds = jnp.concatenate([ld_recv[q] for q in range(seg_len)], axis=0)
    dec_e = jnp.exp2(widen3(lds))
    run = jnp.zeros((piece, feat), F32)
    run_d = jnp.ones((1, feat), F32)
    before = []
    for q in range(seg_len):
        loc[q] = run
        before.append(run_d)
        run = dec_e[q : q + 1, :] * run + a_recv[q].astype(F32)
        run_d = run_d * dec_e[q : q + 1, :]

    after = {"seq": lax.rem(me + seg_len, n_seq)}
    rows = piece // SUB
    onward = [
        remote(t_send.at[pl.ds(u, 1)], b_recv.at[pl.ds(u, 1)], b_s.at[u], b_r.at[u], after)
        for u in range(SUB)
    ]

    @pl.when(seg + 1 < segs)
    def _():
        pl.semaphore_wait(ready_b, 1)

    for u in range(SUB):

        @pl.when(seg > 0)
        def _():
            onward[u].wait_recv()

        t_send[u] = run[u * rows : (u + 1) * rows] + run_d * b_recv[u]

        @pl.when(seg + 1 < segs)
        def _():
            onward[u].start()

    carry = b_recv[...].reshape(piece, feat)
    for q in range(seg_len):
        c_send[q] = loc[q] + before[q] * carry

    c_copies = []
    for d in range(1, seg_len):
        to = lax.rem(pos + d, seg_len)
        copy = remote(c_send.at[pl.ds(to, 1)], inc.at[pl.ds(pos, 1)], c_s.at[d - 1], c_r.at[d - 1], seg_peer(d))
        c_copies.append((seg + to > 0, copy))
    far_first([copy for _, copy in c_copies], lambda to: seg + to > 0)
    inc[pl.ds(pos, 1)] = c_send[pl.ds(pos, 1)]

    @pl.when(me > 0)
    def _():
        for _, copy in c_copies:
            copy.wait_recv()

    _, ss_late = lax.fori_loop(0, jnp.where(me == 0, 0, groups), finish, nothing)
    ss = ss_early + ss_late
    ss_mine[...] = ss[None]

    @pl.when(me == 0)
    def _():
        pl.semaphore_wait(barrier, n_head - 1)

    x_copies = []
    for d in range(1, n_head):
        x_copies.append(
            remote(ss_mine, ss_recv.at[pl.ds(mine_h, 1)], x_s.at[d - 1], x_r.at[d - 1], {"head": lax.rem(mine_h + d, n_head)})
        )
    for copy in x_copies:
        copy.start()
    ss_recv[pl.ds(mine_h, 1)] = ss_mine[...]
    for copy in x_copies:
        copy.wait()
    ss = ss_recv[0]
    for h in range(1, n_head):
        ss = ss + ss_recv[h]
    inv = lax.rsqrt(ss * (1.0 / di) + norm_eps)
    for g in range(groups):
        spread = jnp.where(lane8 == block_i + g * blocks, jnp.broadcast_to(inv[None], (blocks, 8, LANES)), 0.0)
        row_inv = jnp.sum(spread.reshape(GROUP, LANES), axis=1, keepdims=True)
        r0 = g * GROUP
        for j in range(tiles):
            c0 = j * LANES
            base[r0 : r0 + GROUP, c0 : c0 + LANES] = base[r0 : r0 + GROUP, c0 : c0 + LANES] * row_inv

    @pl.when(me + 1 < n_seq)
    def _():
        for copy in halos:
            copy.wait_send()

    @pl.when(seg + 1 < segs)
    def _():
        for copy in onward:
            copy.wait_send()

    for wanted, copy in c_copies:

        @pl.when(wanted)
        def _():
            copy.wait_send()


def on_device(n_seq, n_head, *args):
    (x_raw, bc_raw, gate_in, step_raw, cxw, cxb, cbw, cbb, dt_bias, a_log, d_skip, gain) = args
    length, feat = x_raw.shape[1], x_raw.shape[2]
    heads = dt_bias.shape[0]
    seg_len = SEG if n_seq % SEG == 0 else n_seq
    piece = STATE // seg_len
    groups = length // GROUP
    vmem = pl.BlockSpec(memory_space=pltpu.VMEM)
    hbm = pl.BlockSpec(memory_space=pltpu.HBM)
    dma = pltpu.SemaphoreType.DMA
    regular = pltpu.SemaphoreType.REGULAR
    scratch = [
        pltpu.VMEM((heads, 1, length), F32),
        pltpu.VMEM((CONV, feat), BF16),
        pltpu.VMEM((feat,), BF16),
        pltpu.VMEM((CONV, 2 * STATE), BF16),
        pltpu.VMEM((2 * STATE,), BF16),
        pltpu.VMEM((1, heads), F32),
        pltpu.VMEM((1, heads), F32),
        pltpu.VMEM((1, heads), F32),
        pltpu.VMEM((HALO + length, feat), BF16),
        pltpu.VMEM((HALO + length, 2 * STATE), BF16),
        pltpu.VMEM((length, feat), BF16),
        pltpu.VMEM((length, feat), BF16),
        pltpu.VMEM((length, 2 * STATE), BF16),
        pltpu.VMEM((16, length), F32),
        pltpu.VMEM((feat // LANES + 2, ROWS + HALO, LANES), F32),
        pltpu.VMEM((length, LANES), F32),
        pltpu.VMEM((length, LANES), F32),
        pltpu.VMEM((groups, 16, GROUP), F32),
        pltpu.VMEM((groups, 16, GROUP), F32),
        pltpu.VMEM((8, LANES), F32),
        pltpu.VMEM((8, feat + 2 * STATE), F32),
        pltpu.VMEM((2 * LANES, feat), BF16),
        pltpu.VMEM((GROUP, GROUP), BF16),
        pltpu.VMEM((GROUP, feat), F32),
        pltpu.VMEM((GROUP, feat), BF16),
        pltpu.VMEM((groups, STATE, feat), F32),
        pltpu.VMEM((groups, STATE, feat), F32),
        pltpu.VMEM((length, feat), F32),
        pltpu.VMEM((8, LANES), F32),
        pltpu.VMEM((8, feat), F32),
        pltpu.VMEM((seg_len, piece, feat), BF16),
        pltpu.VMEM((seg_len, piece, feat), BF16),
        pltpu.VMEM((1, 1, LANES), F32),
        pltpu.VMEM((seg_len, 1, LANES), F32),
        pltpu.VMEM((seg_len, piece, feat), F32),
        pltpu.VMEM((SUB, piece // SUB, feat), F32),
        pltpu.VMEM((SUB, piece // SUB, feat), F32),
        pltpu.VMEM((seg_len, piece, feat), F32),
        pltpu.VMEM((seg_len, piece, feat), F32),
        pltpu.VMEM((1, 8, LANES), F32),
        pltpu.VMEM((n_head, 8, LANES), F32),
        regular, regular((seg_len,)), regular,
        dma((11,)),
        dma((2,)), dma((2,)),
        dma((seg_len,)), dma((seg_len,)),
        dma((seg_len,)), dma((seg_len,)),
        dma((SUB,)), dma((SUB,)),
        dma((seg_len,)), dma((seg_len,)),
        dma((n_head,)), dma((n_head,)),
    ]
    sizes = (n_seq, n_head, seg_len, length, feat, heads)
    keep = lambda v: pltpu.with_memory_space_constraint(v, pltpu.HBM)
    out = pl.pallas_call(
        functools.partial(kernel, sizes),
        out_shape=jax.ShapeDtypeStruct((length, feat), F32),
        in_specs=[hbm] * 11,
        out_specs=vmem,
        scratch_shapes=scratch,
        compiler_params=pltpu.CompilerParams(
            collective_id=0, has_side_effects=True, vmem_limit_bytes=VMEM_LIMIT
        ),
        name="ssd_layer",
    )(
        *map(keep, (
            x_raw[0], bc_raw[0], gate_in[0], jnp.transpose(step_raw, (2, 0, 1)), cxw, cxb, cbw, cbb,
            dt_bias[None], a_log[None], d_skip[None],
        ))
    )
    return (out * gain).astype(BF16)[None]


def solution(mesh):
    in_specs = (
        P(("member", "rep"), "seq", "head"),
        P(("member", "rep"), "seq", None),
        P(("member", "rep"), "seq", "head"),
        P(("member", "rep"), "seq", "head"),
        P("member", "head"),
        P(("member", "head")),
        P("member", None),
        P("member"),
        P(("member", "head")),
        P(("member", "head")),
        P(("member", "head")),
        P(("member", "head")),
    )
    out_specs = P(("member", "rep"), "seq", "head")
    return jax.shard_map(
        functools.partial(on_device, mesh.shape["seq"], mesh.shape["head"]),
        mesh=mesh, in_specs=in_specs, out_specs=out_specs, check_vma=False,
    )
```

```python
import functools

import jax
import jax.numpy as jnp
from jax import lax
from jax.experimental import pallas as pl
from jax.experimental.pallas import tpu as pltpu
from jax.sharding import PartitionSpec as P

HEADDIM = 64
STATE = 128
GROUP = 256
CONV = 4
LANES = 128
HALO = 16
ROWS = 64
SEG = 4
SUB = 4
VMEM_LIMIT = 30 * 1024 * 1024
LOG2E = 1.4426950408889634
norm_eps = 1e-05

F32 = jnp.float32
BF16 = jnp.bfloat16
MESH = pl.DeviceIdType.MESH


def silu_of_half(half):
    return half + half * jnp.tanh(half)


def two_parts(v):
    high = v.astype(BF16)
    return high, (v - high.astype(F32)).astype(BF16)


def three_parts(v):
    high = v.astype(BF16)
    rest = v - high.astype(F32)
    mid = rest.astype(BF16)
    return high, mid, (rest - mid.astype(F32)).astype(BF16)


def dot(a, b, dims=((1,), (0,))):
    return lax.dot_general(a, b, (dims, ((), ())), preferred_element_type=F32)


def kernel(sizes, *refs):
    n_seq, n_head, seg_len, length, feat, heads = sizes
    (
        x_hbm, bc_hbm, gate_hbm, step_hbm, cxw_hbm, cxb_hbm, cbw_hbm, cbb_hbm,
        dt_hbm, alog_hbm, skip_hbm, base,
        step_ref, cxw_ref, cxb_ref, cbw_ref, cbb_ref, dt_ref, alog_ref, skip_ref,
        xext, bcext, gbuf, xconv, bconv, raw_t, shifts, stepb, ldb, ldt, stept, par, cw, expand_m, tri_m,
        tail_e, weighted, fresh, entry, scale, dec, gdec,
        s_send, a_recv, ld_mine, ld_recv, loc, t_send, b_recv, c_send, inc,
        ss_mine, ss_recv, ready_h, ready_a, ready_b,
        loc_sem, halo_s, halo_r, a_s, a_r, al_s, al_r, b_s, b_r, c_s, c_r, x_s, x_r,
    ) = refs
    groups = length // GROUP
    tiles = feat // LANES
    piece = STATE // seg_len
    segs = n_seq // seg_len
    di = feat * n_head

    me = lax.axis_index("seq")
    mine_h = lax.axis_index("head")
    seg = me // seg_len
    pos = lax.rem(me, seg_len)

    loads = [
        pltpu.make_async_copy(x_hbm, xext.at[pl.ds(HALO, length)], loc_sem.at[0]),
        pltpu.make_async_copy(bc_hbm, bcext.at[pl.ds(HALO, length)], loc_sem.at[1]),
        pltpu.make_async_copy(gate_hbm, gbuf, loc_sem.at[2]),
        pltpu.make_async_copy(step_hbm, step_ref, loc_sem.at[3]),
        pltpu.make_async_copy(cxw_hbm, cxw_ref, loc_sem.at[4]),
        pltpu.make_async_copy(cxb_hbm, cxb_ref, loc_sem.at[5]),
        pltpu.make_async_copy(cbw_hbm, cbw_ref, loc_sem.at[6]),
        pltpu.make_async_copy(cbb_hbm, cbb_ref, loc_sem.at[7]),
        pltpu.make_async_copy(dt_hbm, dt_ref, loc_sem.at[8]),
        pltpu.make_async_copy(alog_hbm, alog_ref, loc_sem.at[9]),
        pltpu.make_async_copy(skip_hbm, skip_ref, loc_sem.at[10]),
    ]
    for load in loads[3:] + loads[:3]:
        load.start()

    b_recv[...] = jnp.zeros_like(b_recv)
    inc[...] = jnp.zeros_like(inc)
    barrier = pltpu.get_barrier_semaphore()

    def greet(where):
        pl.semaphore_signal(barrier, inc=1, device_id=where, device_id_type=MESH)

    @pl.when(me + 1 < n_seq)
    def _():
        greet({"seq": me + 1})

    for d in range(1, seg_len):

        @pl.when(pos + d < seg_len)
        def _():
            greet({"seq": me + d})

    @pl.when(seg + 1 < segs)
    def _():
        greet({"seq": me + seg_len})

    for d in range(1, n_head):
        greet({"head": lax.rem(mine_h + d, n_head)})

    row_i = lax.broadcasted_iota(jnp.int32, (GROUP, GROUP), 0)
    col_i = lax.broadcasted_iota(jnp.int32, (GROUP, GROUP), 1)
    tri_m[...] = jnp.where(row_i <= col_i, 1.0, 0.0).astype(BF16)
    head_i = lax.broadcasted_iota(jnp.int32, (2 * LANES, feat), 0)
    feat_i = lax.broadcasted_iota(jnp.int32, (2 * LANES, feat), 1)
    expand_m[...] = jnp.where((feat_i >> 6) == (head_i & (LANES - 1)), 1.0, 0.0).astype(BF16)
    for load in loads[3:]:
        load.wait()
    par[...] = jnp.zeros_like(par)
    par[0:1, 0:heads] = dt_ref[...]
    par[1:2, 0:heads] = alog_ref[...]
    par[2:3, 0:heads] = skip_ref[...]
    cw[0:CONV, 0:feat] = 0.5 * cxw_ref[...].astype(F32)
    cw[CONV : CONV + 1, 0:feat] = 0.5 * cxb_ref[...].astype(F32).reshape(1, feat)
    cw[0:CONV, feat:] = 0.5 * cbw_ref[...].astype(F32)
    cw[CONV : CONV + 1, feat:] = 0.5 * cbb_ref[...].astype(F32).reshape(1, 2 * STATE)

    def widen3(v):
        total = None
        for part in three_parts(v):
            term = dot(part, expand_m[0:LANES, :])
            total = term if total is None else total + term
        return total

    def widen2(v):
        high, low = two_parts(v)
        return dot(jnp.concatenate([high, low], axis=1), expand_m[...])

    raw_t[...] = jnp.zeros_like(raw_t)
    for h in range(heads):
        raw_t[h : h + 1, :] = step_ref[h]
    par_t = par[...].T
    raw = raw_t[...] + par_t[0:16, 0:1]
    step = jnp.maximum(raw, 0.0) + jnp.log1p(jnp.exp(-jnp.abs(raw)))
    raw_t[...] = step
    rates = jnp.concatenate(three_parts(-LOG2E * jnp.exp(par_t[0:16, 1:2]) * step), axis=0)
    rest = jnp.zeros((LANES - 16, GROUP), F32)
    dec[...] = jnp.zeros_like(dec)
    for g in range(groups):
        r0 = g * GROUP
        sums = dot(rates[:, r0 : r0 + GROUP], tri_m[...])
        sums = sums[0:16] + sums[16:32] + sums[32:48]
        ldt[g] = sums
        stept[g] = raw_t[:, r0 : r0 + GROUP]
        ldb[r0 : r0 + GROUP, :] = jnp.concatenate([sums, rest], axis=0).T
        stepb[r0 : r0 + GROUP, :] = jnp.concatenate([stept[g], rest], axis=0).T
        dec[g : g + 1, :] = ldb[r0 + GROUP - 1 : r0 + GROUP, :]
    ld_total = dec[0:1, :]
    for g in range(1, groups):
        ld_total = ld_total + dec[g : g + 1, :]
    ld_mine[...] = ld_total[None]

    def conv(ext, r, j, w_off):
        slot = j + w_off // LANES
        shifts[slot] = ext[pl.ds(r, ROWS + HALO), j * LANES : (j + 1) * LANES].astype(F32)
        lo = w_off + j * LANES
        acc = cw[CONV : CONV + 1, lo : lo + LANES]
        for k in range(CONV):
            start = HALO - (CONV - 1 - k)
            acc = acc + cw[k : k + 1, lo : lo + LANES] * shifts[slot, start : start + ROWS, :]
        return silu_of_half(acc)

    def states(g, carry):
        r0 = pl.multiple_of(g * GROUP, GROUP)
        ld = ldb[pl.ds(r0, GROUP), :]
        tail = jnp.exp2(ld[GROUP - 1 : GROUP, :] - ld) * stepb[pl.ds(r0, GROUP), :]
        tail_e[...] = widen2(tail)

        def chunk(i, inner):
            q0 = i * ROWS
            r = pl.multiple_of(r0 + q0, ROWS)
            for j in range(2 * STATE // LANES):
                bconv[pl.ds(r, ROWS), j * LANES : (j + 1) * LANES] = conv(bcext, r, j, feat).astype(BF16)
            for j in range(tiles):
                c0 = j * LANES
                value = conv(xext, r, j, 0).astype(BF16)
                xconv[pl.ds(r, ROWS), c0 : c0 + LANES] = value
                weighted[pl.ds(q0, ROWS), c0 : c0 + LANES] = (
                    tail_e[pl.ds(q0, ROWS), c0 : c0 + LANES] * value.astype(F32)
                ).astype(BF16)
            return inner

        for i in range(GROUP // ROWS):
            chunk(i, 0)
        fresh[pl.ds(g, 1)] = dot(
            bconv[pl.ds(r0, GROUP), 0:STATE], weighted[...], ((0,), (0,))
        )[None]
        return carry

    for load in loads[:2]:
        load.wait()
    @pl.when(me > 0)
    def _():
        pl.semaphore_wait(barrier, 1 + pos + jnp.where(seg > 0, 1, 0) + n_head - 1)
        pl.semaphore_signal(ready_h, inc=1, device_id={"seq": me - 1}, device_id_type=MESH)

    for d in range(1, seg_len):

        @pl.when(pos >= d)
        def _():
            pl.semaphore_signal(ready_a.at[d - 1], inc=1, device_id={"seq": me - d}, device_id_type=MESH)

    @pl.when(seg > 0)
    def _():
        pl.semaphore_signal(ready_b, inc=1, device_id={"seq": me - seg_len}, device_id_type=MESH)

    def remote(src, dst, send, recv, where):
        return pltpu.make_async_remote_copy(
            src_ref=src, dst_ref=dst, send_sem=send, recv_sem=recv,
            device_id=where, device_id_type=MESH,
        )

    halos = [
        remote(xext.at[pl.ds(length, HALO)], xext.at[pl.ds(0, HALO)], halo_s.at[0], halo_r.at[0], {"seq": lax.rem(me + 1, n_seq)}),
        remote(bcext.at[pl.ds(length, HALO)], bcext.at[pl.ds(0, HALO)], halo_s.at[1], halo_r.at[1], {"seq": lax.rem(me + 1, n_seq)}),
    ]

    def states_and_halo(g, carry):
        @pl.when((g == min(2, groups - 1)) & (me + 1 < n_seq))
        def _():
            pl.semaphore_wait(ready_h, 1)
            for copy in halos:
                copy.start()

        return states(g, carry)

    lax.fori_loop(1, groups, states_and_halo, 0)

    def far_first(copies, wanted):
        for m in range(seg_len - 1, 0, -1):
            for inside_seg, to, d in ((pos + m < seg_len, pos + m, m), (pos >= m, pos - m, seg_len - m)):

                @pl.when(inside_seg & wanted(to))
                def _():
                    copies[d - 1].start()

    def seg_peer(d):
        return {"seq": seg * seg_len + lax.rem(pos + d, seg_len)}

    for d in range(1, seg_len):

        @pl.when(pos + d < seg_len)
        def _():
            pl.semaphore_wait(ready_a.at[d - 1], 1)

    ld_copies = []
    for d in range(1, seg_len):
        ld_copies.append(
            remote(ld_mine, ld_recv.at[pl.ds(pos, 1)], al_s.at[d - 1], al_r.at[d - 1], seg_peer(d))
        )
    for copy in ld_copies:
        copy.start()
    ld_recv[pl.ds(pos, 1)] = ld_mine[...]

    @pl.when(me > 0)
    def _():
        for copy in halos:
            copy.wait_recv()

    @pl.when(me == 0)
    def _():
        xext[0:HALO, :] = jnp.zeros((HALO, feat), BF16)
        bcext[0:HALO, :] = jnp.zeros((HALO, 2 * STATE), BF16)

    states(0, 0)

    group_decay = jnp.exp2(widen3(dec[...]))
    run = fresh[0]
    entry[0] = jnp.zeros((STATE, feat), F32)
    entry[1] = run
    for g in range(1, groups):
        run = group_decay[g : g + 1, :] * run + fresh[g]
        if g + 1 < groups:
            entry[g + 1] = run
    s_send[...] = run.astype(BF16).reshape(seg_len, piece, feat)

    a_copies = []
    for d in range(1, seg_len):
        to = lax.rem(pos + d, seg_len)
        a_copies.append(
            remote(s_send.at[pl.ds(to, 1)], a_recv.at[pl.ds(pos, 1)], a_s.at[d - 1], a_r.at[d - 1], seg_peer(d))
        )
    far_first(a_copies, lambda to: True)
    a_recv[pl.ds(pos, 1)] = s_send[pl.ds(pos, 1)]

    skip_e = widen3(par[...])[2:3, :]

    def inside(g, carry):
        r0 = pl.multiple_of(g * GROUP, GROUP)
        scale[pl.ds(r0, GROUP), :] = widen2(jnp.exp2(ldb[pl.ds(r0, GROUP), :]))
        lane = lax.broadcasted_iota(jnp.int32, (ROWS, LANES), 1)
        for tb in range(GROUP // ROWS):
            cols = -(-(tb + 1) * ROWS // LANES) * LANES
            rt = pl.multiple_of(r0 + tb * ROWS, ROWS)
            inter = dot(
                bconv[pl.ds(rt, ROWS), STATE:], bconv[pl.ds(r0, cols), 0:STATE], ((1,), (1,))
            )
            t_i = tb * ROWS + lax.broadcasted_iota(jnp.int32, (ROWS, cols), 0)
            s_i = lax.broadcasted_iota(jnp.int32, (ROWS, cols), 1)
            keep = t_i >= s_i
            for j in range(tiles):
                c0 = j * LANES
                xs = xconv[pl.ds(r0, cols), c0 : c0 + LANES]
                halves = []
                for h in (2 * j, 2 * j + 1):
                    diff = ldb[pl.ds(rt, ROWS), h : h + 1] - ldt[g, h : h + 1, 0:cols]
                    kern = jnp.exp2(jnp.where(keep, diff, -jnp.inf))
                    mix = (inter * kern * stept[g, h : h + 1, 0:cols]).astype(BF16)
                    halves.append(dot(mix, xs))
                intra = jnp.where(lane < HEADDIM, halves[0], halves[1])
                x_t = xconv[pl.ds(rt, ROWS), c0 : c0 + LANES].astype(F32)
                gate = silu_of_half(0.5 * gbuf[pl.ds(rt, ROWS), c0 : c0 + LANES].astype(F32))
                base[pl.ds(rt, ROWS), c0 : c0 + LANES] = (intra + skip_e[:, c0 : c0 + LANES] * x_t) * gate
                scale[pl.ds(rt, ROWS), c0 : c0 + LANES] = scale[pl.ds(rt, ROWS), c0 : c0 + LANES] * gate
        return carry

    loads[2].wait()
    first_part = jnp.where(seg == 0, groups // 2, groups)
    lax.fori_loop(0, first_part, inside, 0)

    blocks = GROUP // 8
    lane8 = lax.broadcasted_iota(jnp.int32, (blocks, 8, LANES), 2)
    block_i = lax.broadcasted_iota(jnp.int32, (blocks, 8, LANES), 0)
    gdec[0:groups, :] = group_decay[0:groups, :]

    def finish(g, so_far):
        run_d, ss = so_far
        r0 = pl.multiple_of(g * GROUP, GROUP)
        state = entry[g] + run_d * inc[...].reshape(STATE, feat)
        high, low = two_parts(state)
        c_rows = bconv[pl.ds(r0, GROUP), STATE:]
        c_rows = jnp.concatenate([c_rows, c_rows], axis=1)
        both = jnp.concatenate([high, low], axis=0)
        squares = jnp.zeros((GROUP, LANES), F32)
        for j in range(tiles):
            c0 = j * LANES
            carried = dot(c_rows, both[:, c0 : c0 + LANES])
            gated = base[pl.ds(r0, GROUP), c0 : c0 + LANES] + scale[pl.ds(r0, GROUP), c0 : c0 + LANES] * carried
            base[pl.ds(r0, GROUP), c0 : c0 + LANES] = gated
            squares = squares + gated * gated
        total = jnp.broadcast_to(jnp.sum(squares, axis=1, keepdims=True), (GROUP, LANES))
        total = total.reshape(blocks, 8, LANES)
        ss = ss + jnp.sum(jnp.where(lane8 == block_i + g * blocks, total, 0.0), axis=0)
        return run_d * gdec[pl.ds(g, 1), :], ss

    nothing = (jnp.ones((1, feat), F32), jnp.zeros((8, LANES), F32))

    for copy in ld_copies:
        copy.wait()
    for copy in a_copies:
        copy.wait()
    lds = jnp.concatenate([ld_recv[q] for q in range(seg_len)], axis=0)
    dec_e = jnp.exp2(widen3(lds))
    run = jnp.zeros((piece, feat), F32)
    run_d = jnp.ones((1, feat), F32)
    before = []
    for q in range(seg_len):
        loc[q] = run
        before.append(run_d)
        run = dec_e[q : q + 1, :] * run + a_recv[q].astype(F32)
        run_d = run_d * dec_e[q : q + 1, :]

    after = {"seq": lax.rem(me + seg_len, n_seq)}
    rows = piece // SUB
    onward = [
        remote(t_send.at[pl.ds(u, 1)], b_recv.at[pl.ds(u, 1)], b_s.at[u], b_r.at[u], after)
        for u in range(SUB)
    ]

    @pl.when(seg + 1 < segs)
    def _():
        pl.semaphore_wait(ready_b, 1)

    for u in range(SUB):

        @pl.when(seg > 0)
        def _():
            onward[u].wait_recv()

        t_send[u] = run[u * rows : (u + 1) * rows] + run_d * b_recv[u]

        @pl.when(seg + 1 < segs)
        def _():
            onward[u].start()

    carry = b_recv[...].reshape(piece, feat)
    for q in range(seg_len):
        c_send[q] = loc[q] + before[q] * carry

    c_copies = []
    for d in range(1, seg_len):
        to = lax.rem(pos + d, seg_len)
        copy = remote(c_send.at[pl.ds(to, 1)], inc.at[pl.ds(pos, 1)], c_s.at[d - 1], c_r.at[d - 1], seg_peer(d))
        c_copies.append((seg + to > 0, copy))
    far_first([copy for _, copy in c_copies], lambda to: seg + to > 0)
    inc[pl.ds(pos, 1)] = c_send[pl.ds(pos, 1)]
    lax.fori_loop(first_part, groups, inside, 0)

    @pl.when(me > 0)
    def _():
        for _, copy in c_copies:
            copy.wait_recv()

    _, ss = lax.fori_loop(0, groups, finish, nothing)
    ss_mine[...] = ss[None]

    @pl.when(me == 0)
    def _():
        pl.semaphore_wait(barrier, n_head - 1)

    x_copies = []
    for d in range(1, n_head):
        x_copies.append(
            remote(ss_mine, ss_recv.at[pl.ds(mine_h, 1)], x_s.at[d - 1], x_r.at[d - 1], {"head": lax.rem(mine_h + d, n_head)})
        )
    for copy in x_copies:
        copy.start()
    ss_recv[pl.ds(mine_h, 1)] = ss_mine[...]
    for copy in x_copies:
        copy.wait()
    ss = ss_recv[0]
    for h in range(1, n_head):
        ss = ss + ss_recv[h]
    inv = lax.rsqrt(ss * (1.0 / di) + norm_eps)
    for g in range(groups):
        spread = jnp.where(lane8 == block_i + g * blocks, jnp.broadcast_to(inv[None], (blocks, 8, LANES)), 0.0)
        row_inv = jnp.sum(spread.reshape(GROUP, LANES), axis=1, keepdims=True)
        r0 = g * GROUP
        for j in range(tiles):
            c0 = j * LANES
            base[r0 : r0 + GROUP, c0 : c0 + LANES] = base[r0 : r0 + GROUP, c0 : c0 + LANES] * row_inv

    @pl.when(me + 1 < n_seq)
    def _():
        for copy in halos:
            copy.wait_send()

    @pl.when(seg + 1 < segs)
    def _():
        for copy in onward:
            copy.wait_send()

    for wanted, copy in c_copies:

        @pl.when(wanted)
        def _():
            copy.wait_send()


def on_device(n_seq, n_head, *args):
    (x_raw, bc_raw, gate_in, step_raw, cxw, cxb, cbw, cbb, dt_bias, a_log, d_skip, gain) = args
    length, feat = x_raw.shape[1], x_raw.shape[2]
    heads = dt_bias.shape[0]
    seg_len = SEG if n_seq % SEG == 0 else n_seq
    piece = STATE // seg_len
    groups = length // GROUP
    vmem = pl.BlockSpec(memory_space=pltpu.VMEM)
    hbm = pl.BlockSpec(memory_space=pltpu.HBM)
    dma = pltpu.SemaphoreType.DMA
    regular = pltpu.SemaphoreType.REGULAR
    scratch = [
        pltpu.VMEM((heads, 1, length), F32),
        pltpu.VMEM((CONV, feat), BF16),
        pltpu.VMEM((feat,), BF16),
        pltpu.VMEM((CONV, 2 * STATE), BF16),
        pltpu.VMEM((2 * STATE,), BF16),
        pltpu.VMEM((1, heads), F32),
        pltpu.VMEM((1, heads), F32),
        pltpu.VMEM((1, heads), F32),
        pltpu.VMEM((HALO + length, feat), BF16),
        pltpu.VMEM((HALO + length, 2 * STATE), BF16),
        pltpu.VMEM((length, feat), BF16),
        pltpu.VMEM((length, feat), BF16),
        pltpu.VMEM((length, 2 * STATE), BF16),
        pltpu.VMEM((16, length), F32),
        pltpu.VMEM((feat // LANES + 2, ROWS + HALO, LANES), F32),
        pltpu.VMEM((length, LANES), F32),
        pltpu.VMEM((length, LANES), F32),
        pltpu.VMEM((groups, 16, GROUP), F32),
        pltpu.VMEM((groups, 16, GROUP), F32),
        pltpu.VMEM((8, LANES), F32),
        pltpu.VMEM((8, feat + 2 * STATE), F32),
        pltpu.VMEM((2 * LANES, feat), BF16),
        pltpu.VMEM((GROUP, GROUP), BF16),
        pltpu.VMEM((GROUP, feat), F32),
        pltpu.VMEM((GROUP, feat), BF16),
        pltpu.VMEM((groups, STATE, feat), F32),
        pltpu.VMEM((groups, STATE, feat), F32),
        pltpu.VMEM((length, feat), F32),
        pltpu.VMEM((8, LANES), F32),
        pltpu.VMEM((8, feat), F32),
        pltpu.VMEM((seg_len, piece, feat), BF16),
        pltpu.VMEM((seg_len, piece, feat), BF16),
        pltpu.VMEM((1, 1, LANES), F32),
        pltpu.VMEM((seg_len, 1, LANES), F32),
        pltpu.VMEM((seg_len, piece, feat), F32),
        pltpu.VMEM((SUB, piece // SUB, feat), F32),
        pltpu.VMEM((SUB, piece // SUB, feat), F32),
        pltpu.VMEM((seg_len, piece, feat), F32),
        pltpu.VMEM((seg_len, piece, feat), F32),
        pltpu.VMEM((1, 8, LANES), F32),
        pltpu.VMEM((n_head, 8, LANES), F32),
        regular, regular((seg_len,)), regular,
        dma((11,)),
        dma((2,)), dma((2,)),
        dma((seg_len,)), dma((seg_len,)),
        dma((seg_len,)), dma((seg_len,)),
        dma((SUB,)), dma((SUB,)),
        dma((seg_len,)), dma((seg_len,)),
        dma((n_head,)), dma((n_head,)),
    ]
    sizes = (n_seq, n_head, seg_len, length, feat, heads)
    keep = lambda v: pltpu.with_memory_space_constraint(v, pltpu.HBM)
    out = pl.pallas_call(
        functools.partial(kernel, sizes),
        out_shape=jax.ShapeDtypeStruct((length, feat), F32),
        in_specs=[hbm] * 11,
        out_specs=vmem,
        scratch_shapes=scratch,
        compiler_params=pltpu.CompilerParams(
            collective_id=0, has_side_effects=True, vmem_limit_bytes=VMEM_LIMIT
        ),
        name="ssd_layer",
    )(
        *map(keep, (
            x_raw[0], bc_raw[0], gate_in[0], jnp.transpose(step_raw, (2, 0, 1)), cxw, cxb, cbw, cbb,
            dt_bias[None], a_log[None], d_skip[None],
        ))
    )
    return (out * gain).astype(BF16)[None]


def solution(mesh):
    in_specs = (
        P(("member", "rep"), "seq", "head"),
        P(("member", "rep"), "seq", None),
        P(("member", "rep"), "seq", "head"),
        P(("member", "rep"), "seq", "head"),
        P("member", "head"),
        P(("member", "head")),
        P("member", None),
        P("member"),
        P(("member", "head")),
        P(("member", "head")),
        P(("member", "head")),
        P(("member", "head")),
    )
    out_specs = P(("member", "rep"), "seq", "head")
    return jax.shard_map(
        functools.partial(on_device, mesh.shape["seq"], mesh.shape["head"]),
        mesh=mesh, in_specs=in_specs, out_specs=out_specs, check_vma=False,
    )
```

```python
import functools

import jax
import jax.numpy as jnp
from jax import lax
from jax.experimental import pallas as pl
from jax.experimental.pallas import tpu as pltpu
from jax.sharding import PartitionSpec as P

HEADDIM = 64
STATE = 128
GROUP = 256
CONV = 4
LANES = 128
HALO = 16
ROWS = 64
SEG = 4
SUB = 4
VMEM_LIMIT = 30 * 1024 * 1024
LOG2E = 1.4426950408889634
norm_eps = 1e-05

F32 = jnp.float32
BF16 = jnp.bfloat16
MESH = pl.DeviceIdType.MESH


def silu_of_half(half):
    return half + half * jnp.tanh(half)


def two_parts(v):
    high = v.astype(BF16)
    return high, (v - high.astype(F32)).astype(BF16)


def three_parts(v):
    high = v.astype(BF16)
    rest = v - high.astype(F32)
    mid = rest.astype(BF16)
    return high, mid, (rest - mid.astype(F32)).astype(BF16)


def dot(a, b, dims=((1,), (0,))):
    return lax.dot_general(a, b, (dims, ((), ())), preferred_element_type=F32)


def kernel(sizes, *refs):
    n_seq, n_head, seg_len, length, feat, heads = sizes
    (
        x_hbm, bc_hbm, gate_hbm, step_hbm, cxw_hbm, cxb_hbm, cbw_hbm, cbb_hbm,
        dt_hbm, alog_hbm, skip_hbm, base,
        step_ref, cxw_ref, cxb_ref, cbw_ref, cbb_ref, dt_ref, alog_ref, skip_ref,
        xext, bcext, gbuf, xconv, bconv, raw_t, shifts, stepb, ldb, ldt, stept, par, cw, expand_m, tri_m,
        tail_e, weighted, fresh, entry, scale, dec, gdec,
        s_send, a_recv, ld_mine, ld_recv, loc, t_send, b_recv, c_send, inc,
        ss_mine, ss_recv, ready_h, ready_a, ready_b,
        loc_sem, halo_s, halo_r, a_s, a_r, al_s, al_r, b_s, b_r, c_s, c_r, x_s, x_r,
    ) = refs
    groups = length // GROUP
    tiles = feat // LANES
    piece = STATE // seg_len
    segs = n_seq // seg_len
    di = feat * n_head

    me = lax.axis_index("seq")
    mine_h = lax.axis_index("head")
    seg = me // seg_len
    pos = lax.rem(me, seg_len)

    loads = [
        pltpu.make_async_copy(x_hbm, xext.at[pl.ds(HALO, length)], loc_sem.at[0]),
        pltpu.make_async_copy(bc_hbm, bcext.at[pl.ds(HALO, length)], loc_sem.at[1]),
        pltpu.make_async_copy(gate_hbm, gbuf, loc_sem.at[2]),
        pltpu.make_async_copy(step_hbm, step_ref, loc_sem.at[3]),
        pltpu.make_async_copy(cxw_hbm, cxw_ref, loc_sem.at[4]),
        pltpu.make_async_copy(cxb_hbm, cxb_ref, loc_sem.at[5]),
        pltpu.make_async_copy(cbw_hbm, cbw_ref, loc_sem.at[6]),
        pltpu.make_async_copy(cbb_hbm, cbb_ref, loc_sem.at[7]),
        pltpu.make_async_copy(dt_hbm, dt_ref, loc_sem.at[8]),
        pltpu.make_async_copy(alog_hbm, alog_ref, loc_sem.at[9]),
        pltpu.make_async_copy(skip_hbm, skip_ref, loc_sem.at[10]),
    ]
    for load in loads[3:] + loads[:3]:
        load.start()

    b_recv[...] = jnp.zeros_like(b_recv)
    inc[...] = jnp.zeros_like(inc)
    barrier = pltpu.get_barrier_semaphore()

    def greet(where):
        pl.semaphore_signal(barrier, inc=1, device_id=where, device_id_type=MESH)

    @pl.when(me + 1 < n_seq)
    def _():
        greet({"seq": me + 1})

    for d in range(1, seg_len):

        @pl.when(pos + d < seg_len)
        def _():
            greet({"seq": me + d})

    @pl.when(seg + 1 < segs)
    def _():
        greet({"seq": me + seg_len})

    for d in range(1, n_head):
        greet({"head": lax.rem(mine_h + d, n_head)})

    row_i = lax.broadcasted_iota(jnp.int32, (GROUP, GROUP), 0)
    col_i = lax.broadcasted_iota(jnp.int32, (GROUP, GROUP), 1)
    tri_m[...] = jnp.where(row_i <= col_i, 1.0, 0.0).astype(BF16)
    head_i = lax.broadcasted_iota(jnp.int32, (2 * LANES, feat), 0)
    feat_i = lax.broadcasted_iota(jnp.int32, (2 * LANES, feat), 1)
    expand_m[...] = jnp.where((feat_i >> 6) == (head_i & (LANES - 1)), 1.0, 0.0).astype(BF16)
    for load in loads[3:]:
        load.wait()
    par[...] = jnp.zeros_like(par)
    par[0:1, 0:heads] = dt_ref[...]
    par[1:2, 0:heads] = alog_ref[...]
    par[2:3, 0:heads] = skip_ref[...]
    cw[0:CONV, 0:feat] = 0.5 * cxw_ref[...].astype(F32)
    cw[CONV : CONV + 1, 0:feat] = 0.5 * cxb_ref[...].astype(F32).reshape(1, feat)
    cw[0:CONV, feat:] = 0.5 * cbw_ref[...].astype(F32)
    cw[CONV : CONV + 1, feat:] = 0.5 * cbb_ref[...].astype(F32).reshape(1, 2 * STATE)

    def widen3(v):
        total = None
        for part in three_parts(v):
            term = dot(part, expand_m[0:LANES, :])
            total = term if total is None else total + term
        return total

    def widen2(v):
        high, low = two_parts(v)
        return dot(jnp.concatenate([high, low], axis=1), expand_m[...])

    raw_t[...] = jnp.zeros_like(raw_t)
    for h in range(heads):
        raw_t[h : h + 1, :] = step_ref[h]
    par_t = par[...].T
    raw = raw_t[...] + par_t[0:16, 0:1]
    step = jnp.maximum(raw, 0.0) + jnp.log1p(jnp.exp(-jnp.abs(raw)))
    raw_t[...] = step
    rates = jnp.concatenate(three_parts(-LOG2E * jnp.exp(par_t[0:16, 1:2]) * step), axis=0)
    rest = jnp.zeros((LANES - 16, GROUP), F32)
    dec[...] = jnp.zeros_like(dec)
    for g in range(groups):
        r0 = g * GROUP
        sums = dot(rates[:, r0 : r0 + GROUP], tri_m[...])
        sums = sums[0:16] + sums[16:32] + sums[32:48]
        ldt[g] = sums
        stept[g] = raw_t[:, r0 : r0 + GROUP]
        ldb[r0 : r0 + GROUP, :] = jnp.concatenate([sums, rest], axis=0).T
        stepb[r0 : r0 + GROUP, :] = jnp.concatenate([stept[g], rest], axis=0).T
        dec[g : g + 1, :] = ldb[r0 + GROUP - 1 : r0 + GROUP, :]
    ld_total = dec[0:1, :]
    for g in range(1, groups):
        ld_total = ld_total + dec[g : g + 1, :]
    ld_mine[...] = ld_total[None]

    def conv(ext, r, j, w_off):
        slot = j + w_off // LANES
        shifts[slot] = ext[pl.ds(r, ROWS + HALO), j * LANES : (j + 1) * LANES].astype(F32)
        lo = w_off + j * LANES
        acc = cw[CONV : CONV + 1, lo : lo + LANES]
        for k in range(CONV):
            start = HALO - (CONV - 1 - k)
            acc = acc + cw[k : k + 1, lo : lo + LANES] * shifts[slot, start : start + ROWS, :]
        return silu_of_half(acc)

    def states(g, carry):
        r0 = pl.multiple_of(g * GROUP, GROUP)
        ld = ldb[pl.ds(r0, GROUP), :]
        tail = jnp.exp2(ld[GROUP - 1 : GROUP, :] - ld) * stepb[pl.ds(r0, GROUP), :]
        tail_e[...] = widen2(tail)

        def chunk(i, inner):
            q0 = i * ROWS
            r = pl.multiple_of(r0 + q0, ROWS)
            for j in range(2 * STATE // LANES):
                bconv[pl.ds(r, ROWS), j * LANES : (j + 1) * LANES] = conv(bcext, r, j, feat).astype(BF16)
            for j in range(tiles):
                c0 = j * LANES
                value = conv(xext, r, j, 0).astype(BF16)
                xconv[pl.ds(r, ROWS), c0 : c0 + LANES] = value
                weighted[pl.ds(q0, ROWS), c0 : c0 + LANES] = (
                    tail_e[pl.ds(q0, ROWS), c0 : c0 + LANES] * value.astype(F32)
                ).astype(BF16)
            return inner

        for i in range(GROUP // ROWS):
            chunk(i, 0)
        fresh[pl.ds(g, 1)] = dot(
            bconv[pl.ds(r0, GROUP), 0:STATE], weighted[...], ((0,), (0,))
        )[None]
        return carry

    for load in loads[:2]:
        load.wait()
    @pl.when(me > 0)
    def _():
        pl.semaphore_wait(barrier, 1 + pos + jnp.where(seg > 0, 1, 0) + n_head - 1)
        pl.semaphore_signal(ready_h, inc=1, device_id={"seq": me - 1}, device_id_type=MESH)

    for d in range(1, seg_len):

        @pl.when(pos >= d)
        def _():
            pl.semaphore_signal(ready_a.at[d - 1], inc=1, device_id={"seq": me - d}, device_id_type=MESH)

    @pl.when(seg > 0)
    def _():
        pl.semaphore_signal(ready_b, inc=1, device_id={"seq": me - seg_len}, device_id_type=MESH)

    def remote(src, dst, send, recv, where):
        return pltpu.make_async_remote_copy(
            src_ref=src, dst_ref=dst, send_sem=send, recv_sem=recv,
            device_id=where, device_id_type=MESH,
        )

    halos = [
        remote(xext.at[pl.ds(length, HALO)], xext.at[pl.ds(0, HALO)], halo_s.at[0], halo_r.at[0], {"seq": lax.rem(me + 1, n_seq)}),
        remote(bcext.at[pl.ds(length, HALO)], bcext.at[pl.ds(0, HALO)], halo_s.at[1], halo_r.at[1], {"seq": lax.rem(me + 1, n_seq)}),
    ]

    def states_and_halo(g, carry):
        @pl.when((g == min(2, groups - 1)) & (me + 1 < n_seq))
        def _():
            pl.semaphore_wait(ready_h, 1)
            for copy in halos:
                copy.start()

        return states(g, carry)

    lax.fori_loop(1, groups, states_and_halo, 0)

    def far_first(copies, wanted):
        for m in range(seg_len - 1, 0, -1):
            for inside_seg, to, d in ((pos + m < seg_len, pos + m, m), (pos >= m, pos - m, seg_len - m)):

                @pl.when(inside_seg & wanted(to))
                def _():
                    copies[d - 1].start()

    def seg_peer(d):
        return {"seq": seg * seg_len + lax.rem(pos + d, seg_len)}

    for d in range(1, seg_len):

        @pl.when(pos + d < seg_len)
        def _():
            pl.semaphore_wait(ready_a.at[d - 1], 1)

    ld_copies = []
    for d in range(1, seg_len):
        ld_copies.append(
            remote(ld_mine, ld_recv.at[pl.ds(pos, 1)], al_s.at[d - 1], al_r.at[d - 1], seg_peer(d))
        )
    for copy in ld_copies:
        copy.start()
    ld_recv[pl.ds(pos, 1)] = ld_mine[...]

    @pl.when(me > 0)
    def _():
        for copy in halos:
            copy.wait_recv()

    @pl.when(me == 0)
    def _():
        xext[0:HALO, :] = jnp.zeros((HALO, feat), BF16)
        bcext[0:HALO, :] = jnp.zeros((HALO, 2 * STATE), BF16)

    states(0, 0)

    group_decay = jnp.exp2(widen3(dec[...]))
    run = fresh[0]
    entry[0] = jnp.zeros((STATE, feat), F32)
    entry[1] = run
    for g in range(1, groups):
        run = group_decay[g : g + 1, :] * run + fresh[g]
        if g + 1 < groups:
            entry[g + 1] = run
    s_send[...] = run.astype(BF16).reshape(seg_len, piece, feat)

    a_copies = []
    for d in range(1, seg_len):
        to = lax.rem(pos + d, seg_len)
        a_copies.append(
            remote(s_send.at[pl.ds(to, 1)], a_recv.at[pl.ds(pos, 1)], a_s.at[d - 1], a_r.at[d - 1], seg_peer(d))
        )
    far_first(a_copies, lambda to: True)
    a_recv[pl.ds(pos, 1)] = s_send[pl.ds(pos, 1)]

    skip_e = widen3(par[...])[2:3, :]

    def inside(g, carry):
        r0 = pl.multiple_of(g * GROUP, GROUP)
        scale[pl.ds(r0, GROUP), :] = widen2(jnp.exp2(ldb[pl.ds(r0, GROUP), :]))
        lane = lax.broadcasted_iota(jnp.int32, (ROWS, LANES), 1)
        for tb in range(GROUP // ROWS):
            cols = -(-(tb + 1) * ROWS // LANES) * LANES
            rt = pl.multiple_of(r0 + tb * ROWS, ROWS)
            inter = dot(
                bconv[pl.ds(rt, ROWS), STATE:], bconv[pl.ds(r0, cols), 0:STATE], ((1,), (1,))
            )
            t_i = tb * ROWS + lax.broadcasted_iota(jnp.int32, (ROWS, cols), 0)
            s_i = lax.broadcasted_iota(jnp.int32, (ROWS, cols), 1)
            keep = t_i >= s_i
            for j in range(tiles):
                c0 = j * LANES
                xs = xconv[pl.ds(r0, cols), c0 : c0 + LANES]
                halves = []
                for h in (2 * j, 2 * j + 1):
                    diff = ldb[pl.ds(rt, ROWS), h : h + 1] - ldt[g, h : h + 1, 0:cols]
                    kern = jnp.exp2(jnp.where(keep, diff, -jnp.inf))
                    mix = (inter * kern * stept[g, h : h + 1, 0:cols]).astype(BF16)
                    halves.append(dot(mix, xs))
                intra = jnp.where(lane < HEADDIM, halves[0], halves[1])
                x_t = xconv[pl.ds(rt, ROWS), c0 : c0 + LANES].astype(F32)
                gate = silu_of_half(0.5 * gbuf[pl.ds(rt, ROWS), c0 : c0 + LANES].astype(F32))
                base[pl.ds(rt, ROWS), c0 : c0 + LANES] = (intra + skip_e[:, c0 : c0 + LANES] * x_t) * gate
                scale[pl.ds(rt, ROWS), c0 : c0 + LANES] = scale[pl.ds(rt, ROWS), c0 : c0 + LANES] * gate
        return carry

    loads[2].wait()
    first_part = jnp.where(seg == 0, groups // 4, groups)
    lax.fori_loop(0, first_part, inside, 0)

    blocks = GROUP // 8
    lane8 = lax.broadcasted_iota(jnp.int32, (blocks, 8, LANES), 2)
    block_i = lax.broadcasted_iota(jnp.int32, (blocks, 8, LANES), 0)
    gdec[0:groups, :] = group_decay[0:groups, :]

    def finish(g, so_far):
        run_d, ss = so_far
        r0 = pl.multiple_of(g * GROUP, GROUP)
        state = entry[g] + run_d * inc[...].reshape(STATE, feat)
        high, low = two_parts(state)
        c_rows = bconv[pl.ds(r0, GROUP), STATE:]
        c_rows = jnp.concatenate([c_rows, c_rows], axis=1)
        both = jnp.concatenate([high, low], axis=0)
        squares = jnp.zeros((GROUP, LANES), F32)
        for j in range(tiles):
            c0 = j * LANES
            carried = dot(c_rows, both[:, c0 : c0 + LANES])
            gated = base[pl.ds(r0, GROUP), c0 : c0 + LANES] + scale[pl.ds(r0, GROUP), c0 : c0 + LANES] * carried
            base[pl.ds(r0, GROUP), c0 : c0 + LANES] = gated
            squares = squares + gated * gated
        total = jnp.broadcast_to(jnp.sum(squares, axis=1, keepdims=True), (GROUP, LANES))
        total = total.reshape(blocks, 8, LANES)
        ss = ss + jnp.sum(jnp.where(lane8 == block_i + g * blocks, total, 0.0), axis=0)
        return run_d * gdec[pl.ds(g, 1), :], ss

    nothing = (jnp.ones((1, feat), F32), jnp.zeros((8, LANES), F32))

    for copy in ld_copies:
        copy.wait()
    for copy in a_copies:
        copy.wait()
    lds = jnp.concatenate([ld_recv[q] for q in range(seg_len)], axis=0)
    dec_e = jnp.exp2(widen3(lds))
    run = jnp.zeros((piece, feat), F32)
    run_d = jnp.ones((1, feat), F32)
    before = []
    for q in range(seg_len):
        loc[q] = run
        before.append(run_d)
        run = dec_e[q : q + 1, :] * run + a_recv[q].astype(F32)
        run_d = run_d * dec_e[q : q + 1, :]

    after = {"seq": lax.rem(me + seg_len, n_seq)}
    rows = piece // SUB
    onward = [
        remote(t_send.at[pl.ds(u, 1)], b_recv.at[pl.ds(u, 1)], b_s.at[u], b_r.at[u], after)
        for u in range(SUB)
    ]

    @pl.when(seg + 1 < segs)
    def _():
        pl.semaphore_wait(ready_b, 1)

    for u in range(SUB):

        @pl.when(seg > 0)
        def _():
            onward[u].wait_recv()

        t_send[u] = run[u * rows : (u + 1) * rows] + run_d * b_recv[u]

        @pl.when(seg + 1 < segs)
        def _():
            onward[u].start()

    carry = b_recv[...].reshape(piece, feat)
    for q in range(seg_len):
        c_send[q] = loc[q] + before[q] * carry

    c_copies = []
    for d in range(1, seg_len):
        to = lax.rem(pos + d, seg_len)
        copy = remote(c_send.at[pl.ds(to, 1)], inc.at[pl.ds(pos, 1)], c_s.at[d - 1], c_r.at[d - 1], seg_peer(d))
        c_copies.append((seg + to > 0, copy))
    far_first([copy for _, copy in c_copies], lambda to: seg + to > 0)
    inc[pl.ds(pos, 1)] = c_send[pl.ds(pos, 1)]
    lax.fori_loop(first_part, groups, inside, 0)

    @pl.when(me > 0)
    def _():
        for _, copy in c_copies:
            copy.wait_recv()

    _, ss = lax.fori_loop(0, groups, finish, nothing)
    ss_mine[...] = ss[None]

    @pl.when(me == 0)
    def _():
        pl.semaphore_wait(barrier, n_head - 1)

    x_copies = []
    for d in range(1, n_head):
        x_copies.append(
            remote(ss_mine, ss_recv.at[pl.ds(mine_h, 1)], x_s.at[d - 1], x_r.at[d - 1], {"head": lax.rem(mine_h + d, n_head)})
        )
    for copy in x_copies:
        copy.start()
    ss_recv[pl.ds(mine_h, 1)] = ss_mine[...]
    for copy in x_copies:
        copy.wait()
    ss = ss_recv[0]
    for h in range(1, n_head):
        ss = ss + ss_recv[h]
    inv = lax.rsqrt(ss * (1.0 / di) + norm_eps)
    for g in range(groups):
        spread = jnp.where(lane8 == block_i + g * blocks, jnp.broadcast_to(inv[None], (blocks, 8, LANES)), 0.0)
        row_inv = jnp.sum(spread.reshape(GROUP, LANES), axis=1, keepdims=True)
        r0 = g * GROUP
        for j in range(tiles):
            c0 = j * LANES
            base[r0 : r0 + GROUP, c0 : c0 + LANES] = base[r0 : r0 + GROUP, c0 : c0 + LANES] * row_inv

    @pl.when(me + 1 < n_seq)
    def _():
        for copy in halos:
            copy.wait_send()

    @pl.when(seg + 1 < segs)
    def _():
        for copy in onward:
            copy.wait_send()

    for wanted, copy in c_copies:

        @pl.when(wanted)
        def _():
            copy.wait_send()


def on_device(n_seq, n_head, *args):
    (x_raw, bc_raw, gate_in, step_raw, cxw, cxb, cbw, cbb, dt_bias, a_log, d_skip, gain) = args
    length, feat = x_raw.shape[1], x_raw.shape[2]
    heads = dt_bias.shape[0]
    seg_len = SEG if n_seq % SEG == 0 else n_seq
    piece = STATE // seg_len
    groups = length // GROUP
    vmem = pl.BlockSpec(memory_space=pltpu.VMEM)
    hbm = pl.BlockSpec(memory_space=pltpu.HBM)
    dma = pltpu.SemaphoreType.DMA
    regular = pltpu.SemaphoreType.REGULAR
    scratch = [
        pltpu.VMEM((heads, 1, length), F32),
        pltpu.VMEM((CONV, feat), BF16),
        pltpu.VMEM((feat,), BF16),
        pltpu.VMEM((CONV, 2 * STATE), BF16),
        pltpu.VMEM((2 * STATE,), BF16),
        pltpu.VMEM((1, heads), F32),
        pltpu.VMEM((1, heads), F32),
        pltpu.VMEM((1, heads), F32),
        pltpu.VMEM((HALO + length, feat), BF16),
        pltpu.VMEM((HALO + length, 2 * STATE), BF16),
        pltpu.VMEM((length, feat), BF16),
        pltpu.VMEM((length, feat), BF16),
        pltpu.VMEM((length, 2 * STATE), BF16),
        pltpu.VMEM((16, length), F32),
        pltpu.VMEM((feat // LANES + 2, ROWS + HALO, LANES), F32),
        pltpu.VMEM((length, LANES), F32),
        pltpu.VMEM((length, LANES), F32),
        pltpu.VMEM((groups, 16, GROUP), F32),
        pltpu.VMEM((groups, 16, GROUP), F32),
        pltpu.VMEM((8, LANES), F32),
        pltpu.VMEM((8, feat + 2 * STATE), F32),
        pltpu.VMEM((2 * LANES, feat), BF16),
        pltpu.VMEM((GROUP, GROUP), BF16),
        pltpu.VMEM((GROUP, feat), F32),
        pltpu.VMEM((GROUP, feat), BF16),
        pltpu.VMEM((groups, STATE, feat), F32),
        pltpu.VMEM((groups, STATE, feat), F32),
        pltpu.VMEM((length, feat), F32),
        pltpu.VMEM((8, LANES), F32),
        pltpu.VMEM((8, feat), F32),
        pltpu.VMEM((seg_len, piece, feat), BF16),
        pltpu.VMEM((seg_len, piece, feat), BF16),
        pltpu.VMEM((1, 1, LANES), F32),
        pltpu.VMEM((seg_len, 1, LANES), F32),
        pltpu.VMEM((seg_len, piece, feat), F32),
        pltpu.VMEM((SUB, piece // SUB, feat), F32),
        pltpu.VMEM((SUB, piece // SUB, feat), F32),
        pltpu.VMEM((seg_len, piece, feat), F32),
        pltpu.VMEM((seg_len, piece, feat), F32),
        pltpu.VMEM((1, 8, LANES), F32),
        pltpu.VMEM((n_head, 8, LANES), F32),
        regular, regular((seg_len,)), regular,
        dma((11,)),
        dma((2,)), dma((2,)),
        dma((seg_len,)), dma((seg_len,)),
        dma((seg_len,)), dma((seg_len,)),
        dma((SUB,)), dma((SUB,)),
        dma((seg_len,)), dma((seg_len,)),
        dma((n_head,)), dma((n_head,)),
    ]
    sizes = (n_seq, n_head, seg_len, length, feat, heads)
    keep = lambda v: pltpu.with_memory_space_constraint(v, pltpu.HBM)
    out = pl.pallas_call(
        functools.partial(kernel, sizes),
        out_shape=jax.ShapeDtypeStruct((length, feat), F32),
        in_specs=[hbm] * 11,
        out_specs=vmem,
        scratch_shapes=scratch,
        compiler_params=pltpu.CompilerParams(
            collective_id=0, has_side_effects=True, vmem_limit_bytes=VMEM_LIMIT
        ),
        name="ssd_layer",
    )(
        *map(keep, (
            x_raw[0], bc_raw[0], gate_in[0], jnp.transpose(step_raw, (2, 0, 1)), cxw, cxb, cbw, cbb,
            dt_bias[None], a_log[None], d_skip[None],
        ))
    )
    return (out * gain).astype(BF16)[None]


def solution(mesh):
    in_specs = (
        P(("member", "rep"), "seq", "head"),
        P(("member", "rep"), "seq", None),
        P(("member", "rep"), "seq", "head"),
        P(("member", "rep"), "seq", "head"),
        P("member", "head"),
        P(("member", "head")),
        P("member", None),
        P("member"),
        P(("member", "head")),
        P(("member", "head")),
        P(("member", "head")),
        P(("member", "head")),
    )
    out_specs = P(("member", "rep"), "seq", "head")
    return jax.shard_map(
        functools.partial(on_device, mesh.shape["seq"], mesh.shape["head"]),
        mesh=mesh, in_specs=in_specs, out_specs=out_specs, check_vma=False,
    )
```
